256 devices in a mesh: ba: 64 (over z_hi, x, y, core), wa: 4 (over z_lo).
Axes of the slice: x: 4, y: 4, z: 8 (z_hi: 2, z_lo: 4; z = z_hi * 4 + z_lo), core: 2. Of those that a mesh axis runs over, the one named last changes fastest.
Arguments:
- sky_model: float32 [2, 2048, 2048], P(None, None, 'wa'), may hold values from -6 to 6
- plane_w: float32 [64], P('ba'), may hold values from -60 to 60
- kernel: float32 [16, 8], replicated, may hold values from -2 to 2
- tile_ids: int32 [4096], P(('ba', 'wa')), may hold values from 0 to 255, as said below
- plane_ids: int32 [4096, 1], P(('ba', 'wa')), may hold values from 0 to 63; in each aligned block of 16 rows (0 to 15, 16 to 31, ...) at most 2 rows name the same one
- positions: int32 [4096, 2, 512], P(('ba', 'wa')), may hold values from 0 to 1935
- observed: float32 [4096, 2, 512], P(('ba', 'wa')), may hold values from -6 to 6
Outputs:
- residual_vis: float32 [4096, 2, 512], P(('ba', 'wa'))
The draws below stay inside these ranges and needn't reach their ends.
Inputs may be any that keep to these rules, and one draw needn't show every extreme that they name: `plane_ids`: among the 16 blocks of one device at most 2 name the same w-plane, and in every draw some device has a w-plane named by exactly 2 of its blocks. `tile_ids`: A tile id is row_tile * 16 + column_tile; the blocks held at index a of wa name column tiles a * 4 to (a + 1) * 4 - 1.
All inputs are finite; a program needn't handle non-finite values.
Results may differ from the reference program's by a relative error of at most 0.0003.
Values sent between devices are 32-bit elements; how exact they have to be, the bound alone decides.
No kernel may reach another device: no remote copies, remote signals or barrier semaphores. Data moves between devices by JAX's collectives and lax.ppermute only.
A program may use at most 128 MiB of HBM per device.

```python
import math
import jax
import jax.numpy as jnp
import numpy as np
from jax import lax

N = 2048
TILE = 128
SUPPORT = 8
OVER = 16
SAMPLES = 512
BLK_DEV = 16
PLANES = 64
CAP = 2
NT = 16
NT_DEV = 4
BLOCKS = 4096
N_BA = 64
N_WA = 4


def draw_tile_ids(key, part):
    row_key = jax.random.fold_in(key, 11)
    column_key = jax.random.fold_in(key, 12)
    row_tile = jax.random.randint(row_key, (BLOCKS,), 0, NT, dtype=jnp.int32)
    local_column = jax.random.randint(column_key, (BLOCKS,), 0, NT_DEV, dtype=jnp.int32)
    slab_index = jnp.arange(BLOCKS, dtype=jnp.int32) // BLK_DEV % N_WA
    return row_tile * NT + slab_index * NT_DEV + local_column


def with_ends(array, own_key, least, high):
    longest = array.shape.index(max(array.shape))
    spots = []
    for shift in (0, 1):
        where = [jax.random.randint(jax.random.fold_in(own_key, axis), (), 0, length) for axis, length in enumerate(array.shape)]
        where[longest] = (where[longest] + shift) % array.shape[longest]
        spots.append(tuple(where))
    return array.at[spots[0]].set(least).at[spots[1]].set(high)


def block_scale(stream_key, extent, pieces, low, largest):
    def one(dim, shards_of):
        steps = jax.random.uniform(jax.random.fold_in(jax.random.fold_in(stream_key, 6), dim), (shards_of,), jnp.float32, low / len(pieces), largest / len(pieces))
        return jnp.repeat(jnp.exp(steps), extent[dim] // shards_of).reshape((-1,) + (1,) * (len(extent) - dim - 1))

    level = one(*pieces[0])
    for cut in pieces[1:]:
        level = level * one(*cut)
    return level


def routed_block(own_key, own, number, rows, number_of, top, limit, lean):
    sequence = jax.random.permutation(own_key, number_of)
    heavy_load, ordinary = shares(number_of, rows * top, limit, lean, True), shares(number_of, rows * top, limit, lean, False)
    places = jnp.arange(number_of)

    def named(sizes, turn):
        used = int((sizes > 0).sum())
        fixed = max(1, used // 4)
        shifted = fixed + (places - fixed + turn * (used - fixed)) % max(1, number_of - fixed)
        return jnp.zeros((number_of,), jnp.int32).at[sequence[jnp.where(places < fixed, places, shifted)]].set(jnp.asarray(sizes, jnp.int32))

    sizes = jnp.where(number % 4 == 0, named(heavy_load, number // 4), named(ordinary, number - number // 4 - 1))
    mixed = jax.random.permutation(jax.random.fold_in(own, 3), number_of)
    source_of, taker = mixed[0:number_of // 2 * 2:2], mixed[1:number_of // 2 * 2:2]
    margin = jnp.minimum(sizes[source_of] - 1, limit - sizes[taker]) // 2
    margin = jnp.where((source_of == sequence[0]) | (taker == sequence[0]) | (sizes[taker] == 0), 0, jnp.maximum(margin, 0))
    shifted = jax.random.randint(jax.random.fold_in(own, 4), (number_of // 2,), 0, 1 << 20) % (margin + 1)
    sizes = sizes.at[source_of].add(-shifted).at[taker].add(shifted)
    items = jnp.searchsorted(jnp.cumsum(sizes), jnp.arange(rows * top), side="right").astype(jnp.int32)
    listing = items.reshape(top, rows).T
    listing = listing[jax.random.permutation(jax.random.fold_in(own, 1), rows)]
    turn = jax.random.randint(jax.random.fold_in(own, 2), (rows, 1), 0, top)
    return jnp.take_along_axis(listing, (jnp.arange(top)[None, :] + turn) % top, axis=1)


def shares(count, total, bound, lean, full):
    portions = [(1 << 20) // math.isqrt(rank ** lean) + 1 for rank in range(1, count + 1)]
    largest = bound if full else min(bound, max(-(-total // count), total * portions[0] // sum(portions)))
    least = 1 if total - largest >= count - 1 else 0
    holding, spare = [largest] + [least] * (count - 1), total - largest - least * (count - 1)
    while spare > 0:
        free = [i for i in range(1, count) if holding[i] < largest] or [i for i in range(1, count) if holding[i] < bound]
        pool, remaining = sum([portions[i] for i in free]), spare
        for i in free:
            extra = min(bound - holding[i], max(1, remaining * portions[i] // pool), spare)
            holding[i] = holding[i] + extra
            spare = spare - extra
    return np.array(holding)


def bell_draw(own_key, extent, spread, limit, split=(), held_as=jnp.bfloat16):
    factor_of = block_scale(own_key, extent, split, -0.22, 0.18) if split else 1.0
    values = jax.random.normal(own_key, extent, jnp.float32) * spread * factor_of
    return jnp.minimum(jnp.maximum(values, -limit), limit).astype(held_as)


def setup_inputs(seed: int = 0) -> dict:
    seeds = jax.random.split(jax.random.key(seed), 8)
    sky_model = bell_draw(seeds[0], (2, N, N), 1.0, 6.0, ((2, 4),), jnp.float32)
    plane_w = jnp.clip(jax.random.uniform(seeds[1], (PLANES,), jnp.float32, -60.0, 60.0) * block_scale(seeds[1], (PLANES,), ((0, 64),), -0.4, 0.0), -60.0, 60.0)
    kernel = bell_draw(seeds[2], (OVER, SUPPORT), 0.35, 2.0, (), jnp.float32)
    tile_ids = draw_tile_ids(jax.random.fold_in(seeds[7], 71), 0)
    plane_ids_keys = jax.random.split(jax.random.fold_in(seeds[4], 1), BLOCKS // BLK_DEV)
    plane_ids_turns = jax.random.permutation(jax.random.fold_in(seeds[4], 3), BLOCKS // BLK_DEV)
    plane_ids = jax.vmap(lambda own, number: routed_block(jax.random.fold_in(seeds[4], 2), own, number, BLK_DEV, PLANES, 1, CAP, 2))(plane_ids_keys, plane_ids_turns).reshape((BLOCKS, 1))
    positions = with_ends(jax.random.randint(seeds[5], (BLOCKS, 2, SAMPLES), 0, (TILE - SUPPORT + 1) * OVER), jax.random.fold_in(seeds[5], 1), 0, ((TILE - SUPPORT + 1) * OVER) - 1).astype(jnp.int32)
    observed = bell_draw(seeds[6], (BLOCKS, 2, SAMPLES), 1.0, 6.0, ((0, 256),), jnp.float32)
    return {"sky_model": sky_model, "plane_w": plane_w, "kernel": kernel, "tile_ids": tile_ids, "plane_ids": plane_ids, "positions": positions, "observed": observed}


FIELD_WIDTH = 0.7

def degrid_blocks(uv_grid, tile_list, fine_position, kernel):
    tiles_across = N // TILE
    row_tile = tile_list // tiles_across
    col_tile = tile_list % tiles_across
    cell_index = fine_position // OVER
    offset_index = fine_position % OVER
    kernel_taps = kernel[offset_index]
    tap_offsets = jnp.arange(SUPPORT, dtype=jnp.int32)
    row_cells = (row_tile * TILE)[:, None, None] + cell_index[:, 0, :, None] + tap_offsets
    col_cells = (col_tile * TILE)[:, None, None] + cell_index[:, 1, :, None] + tap_offsets
    patches = uv_grid[:, row_cells[:, :, :, None], col_cells[:, :, None, :]]
    return jnp.einsum('cmsij,msi,msj->mcs', patches, kernel_taps[:, 0], kernel_taps[:, 1])

def reference(sky_model, plane_w, kernel, tile_ids, plane_ids, positions, observed):
    coordinate = (jnp.arange(N, dtype=jnp.int32).astype(jnp.float32) - N / 2) * (FIELD_WIDTH / N)
    radius_sq = coordinate[:, None] ** 2 + coordinate[None, :] ** 2
    lowered = -radius_sq / (1.0 + jnp.sqrt(1.0 - radius_sq))
    target = plane_ids[:, 0]
    window = N_BA * N_WA * CAP
    sorted_blocks = jnp.argsort(target, stable=True).astype(jnp.int32)
    counts = lax.optimization_barrier(jnp.sum((target[None, :] == jnp.arange(PLANES, dtype=jnp.int32)[:, None]).astype(jnp.int32), axis=1))
    starts = (jnp.cumsum(counts) - counts).astype(jnp.int32)
    padded_order = jnp.concatenate([sorted_blocks, jnp.zeros((window,), jnp.int32)])

    def one_plane(predicted, plane_index):
        phase_angle = -2.0 * math.pi * plane_w[plane_index] * lowered
        cosine = jnp.cos(phase_angle)
        sine_part = jnp.sin(phase_angle)
        plane_image = lax.complex(sky_model[0] * cosine - sky_model[1] * sine_part, sky_model[0] * sine_part + sky_model[1] * cosine)
        spectrum = jnp.fft.fft2(plane_image).T / N
        uv_grid = jnp.stack([jnp.real(spectrum), jnp.imag(spectrum)])
        chosen = lax.dynamic_slice(padded_order, (starts[plane_index],), (window,))
        live_rows = jnp.arange(window, dtype=jnp.int32) < counts[plane_index]
        values_out = degrid_blocks(uv_grid, tile_ids[chosen], positions[chosen], kernel)
        predicted = predicted.at[chosen].add(jnp.where(live_rows[:, None, None], values_out, 0.0))
        return (predicted, None)
    predicted = lax.scan(one_plane, jnp.zeros(observed.shape, jnp.float32), jnp.arange(PLANES, dtype=jnp.int32))[0]
    return observed - predicted
```

```python
import functools
import math

import jax
import jax.numpy as jnp
from jax import lax
from jax.experimental import pallas as pl
from jax.experimental.pallas import tpu as pltpu
from jax.sharding import Mesh
from jax.sharding import PartitionSpec as P


N = 2048
SP = 0.7 / N
AROWS = 24
CROWS = 64
F32 = jnp.float32
BF16 = jnp.bfloat16

SIN_C = (3.14159264, -5.16771009, 2.55007766, -0.59829216, 0.07765941)
COS_C = (1.0, -4.93480214, 4.05870916, -1.33521206, 0.23493756, -0.02439672)
G_C = (0.5, 0.12500105, 0.0624521, 0.03985648, 0.0215331, 0.03890036)
MAGIC = 12582912.0


def horner(z, coefs):
    acc = jnp.full_like(z, coefs[-1])
    for c in coefs[-2::-1]:
        acc = acc * z + c
    return acc


def cis_turns(t):
    r = t - ((t + MAGIC) - MAGIC)
    z = r * r
    s = r * horner(z, SIN_C)
    c = horner(z, COS_C)
    s2 = s + s
    return 1.0 - s2 * s, s2 * c


def split(x):
    hi = x.astype(BF16)
    return hi, (x - hi.astype(F32)).astype(BF16)


def bdot(a, b):
    return jnp.dot(a, b, preferred_element_type=F32)


def tables_kernel(e1h, e1l, e2h, e2l):
    k0 = pl.program_id(0)
    row = lax.broadcasted_iota(jnp.int32, (128, 128), 0)
    col = lax.broadcasted_iota(jnp.int32, (128, 128), 1)

    def cs(freq, pos):
        k = (freq * (16 * pos + k0)) & (N - 1)
        return cis_turns(k.astype(F32) * (1.0 / N))

    def put(h, l, r, c, v):
        a, b = split(v)
        h[0, 128 * r : 128 * r + 128, 128 * c : 128 * c + 128] = a
        l[0, 128 * r : 128 * r + 128, 128 * c : 128 * c + 128] = b

    c, s = cs(col, row)
    put(e1h, e1l, 0, 0, c)
    put(e1h, e1l, 1, 1, c)
    put(e1h, e1l, 0, 1, -s)
    put(e1h, e1l, 1, 0, s)
    c, s = cs(row, col)
    c, s = c * (1.0 / N), s * (1.0 / N)
    put(e2h, e2l, 0, 0, c)
    put(e2h, e2l, 1, 1, c)
    put(e2h, e2l, 0, 1, s)
    put(e2h, e2l, 1, 0, -s)


def tables():
    sds = jax.ShapeDtypeStruct((16, 256, 256), BF16)
    spec = pl.BlockSpec((1, 256, 256), lambda i: (i, 0, 0))
    return pl.pallas_call(
        tables_kernel,
        grid=(16,),
        out_shape=[sds] * 4,
        out_specs=[spec] * 4,
        cost_estimate=pl.CostEstimate(flops=60 * 16 * 2 * 16384, bytes_accessed=8 << 20, transcendentals=0),
        name="tables",
    )()


def turn_kernel(core, x_ref, o_ref, tmp):
    for y0 in range(16):
        t = tmp.at[y0 % 2]
        t[...] = x_ref[0, pl.ds(y0, 128, stride=16), :].T
        for j0 in range(16):
            o_ref[y0, j0, 0] = t[pl.ds(j0, 8, stride=16), :]


def turn(core, sky):
    out = pl.pallas_call(
        turn_kernel,
        grid_spec=pltpu.PrefetchScalarGridSpec(
            num_scalar_prefetch=1,
            grid=(2, 2),
            in_specs=[pl.BlockSpec((1, N, 128), lambda c, b, s: (c, 0, 2 * s[0] + b))],
            out_specs=pl.BlockSpec((16, 16, 1, 8, 128), lambda c, b, s: (0, 0, b, 0, c)),
            scratch_shapes=[pltpu.VMEM((2, 128, 128), F32)],
        ),
        out_shape=jax.ShapeDtypeStruct((16, 16, 2, 8, 256), F32),
        cost_estimate=pl.CostEstimate(flops=1 << 22, bytes_accessed=8 << 20, transcendentals=0),
        name="turn",
    )(core, sky)
    return out.reshape(16, 256, 256)


def along_y_kernel(plan, ints, floats, e1h, e1l, *rest):
    n_src = 1 + max(s for blk in plan for (s, _, _, _) in blk["src"])
    srcs = rest[:n_src]
    keep, send = rest[n_src : n_src + 2]
    xin, xh, xl, yb, gb, cx2, sem_in, sem_out = rest[n_src + 2 :]
    core = ints[0]
    lane = lax.broadcasted_iota(jnp.int32, (8, 128), 1)
    sub = lax.broadcasted_iota(jnp.int32, (8, 128), 0)

    def loads(b):
        blk, slot = plan[b], b % 2
        out = []
        for i, (s, rows0, d0, dn) in enumerate(blk["src"]):
            out.append(
                pltpu.make_async_copy(
                    srcs[s].at[:, pl.ds(rows0, blk["rows"]), :],
                    xin.at[slot, pl.ds(d0, dn), pl.ds(0, blk["rows"]), :],
                    sem_in.at[slot, i],
                )
            )
        return out

    def stores(b):
        blk, slot = plan[b], b % 2
        rows = pl.ds(0, blk["rows"])
        dst = pl.ds(blk["off"], blk["rows"])
        return [
            pltpu.make_async_copy(gb.at[slot, core, :, :, rows, :], keep.at[:, :, dst, :], sem_out.at[slot, 0]),
            pltpu.make_async_copy(gb.at[slot, 1 - core, :, :, rows, :], send.at[:, :, dst, :], sem_out.at[slot, 1]),
        ]

    for c in loads(0):
        c.start()
    w = [floats[0], floats[1]]
    for b, blk in enumerate(plan):
        slot, R = b % 2, blk["rows"]
        U = R // 8
        u0 = blk["off"] // 8
        base = ints[1 + b]
        tw = [[(floats[2 + 32 * b + 8 * j + 2 * q], floats[2 + 32 * b + 8 * j + 2 * q + 1]) for q in range(4)] for j in range(4)]
        if b + 1 < len(plan):
            for c in loads(b + 1):
                c.start()
        for g in range(U):
            x = (ints[1 + len(plan) + u0 + g] + 16 * sub).astype(F32)
            cx = (x - N / 2) * SP
            cx2[g] = cx * cx
        for c in loads(b):
            c.wait()
        if b >= 2:
            for c in stores(b - 2):
                c.wait()

        def step(q, carry, slot=slot, R=R, U=U, base=base, b=b):
            for p in range(4):
                y0 = 4 * ((base + p) & 3) + q
                cy = ((16 * lane + y0).astype(F32) - N / 2) * SP
                cy2 = cy * cy
                for g in range(U):
                    s = cx2[g] + cy2
                    t = s * horner(s, G_C)
                    sr = xin[slot, 4 * p + q, 8 * g : 8 * g + 8, 0:128]
                    si = xin[slot, 4 * p + q, 8 * g : 8 * g + 8, 128:256]
                    re, im = [], []
                    for pi in range(2):
                        c, sn = cis_turns(t * w[pi])
                        re.append(sr * c - si * sn)
                        im.append(sr * sn + si * c)
                    h, l = split(jnp.concatenate(re, axis=0))
                    xh[p, 16 * g : 16 * g + 16, 0:128] = h
                    xl[p, 16 * g : 16 * g + 16, 0:128] = l
                    h, l = split(jnp.concatenate(im, axis=0))
                    xh[p, 16 * g : 16 * g + 16, 128:256] = h
                    xl[p, 16 * g : 16 * g + 16, 128:256] = l
                eh = e1h[y0]
                a = xh[p, 0 : 2 * R, :]
                yb[p, 0 : 2 * R, :] = bdot(a, eh) + bdot(xl[p, 0 : 2 * R, :], eh) + bdot(a, e1l[y0])
            fr = [floats[2 + 32 * b + 8 * j + 2 * q] for j in range(4)]
            fi = [floats[2 + 32 * b + 8 * j + 2 * q + 1] for j in range(4)]
            for g in range(U):
                for pi in range(2):
                    r0 = 16 * g + 8 * pi
                    yr = [yb[p, r0 : r0 + 8, 0:128] for p in range(4)]
                    yi = [yb[p, r0 : r0 + 8, 128:256] for p in range(4)]
                    ar, ai = yr[0] + yr[2], yi[0] + yi[2]
                    br, bi = yr[0] - yr[2], yi[0] - yi[2]
                    cr, ci = yr[1] + yr[3], yi[1] + yi[3]
                    dr, di = yr[1] - yr[3], yi[1] - yi[3]
                    outs = ((ar + cr, ai + ci), (br + di, bi - dr), (ar - cr, ai - ci), (br - di, bi + dr))
                    for j, (o_r, o_i) in enumerate(outs):
                        vr = o_r * fr[j] - o_i * fi[j]
                        vi = o_r * fi[j] + o_i * fr[j]
                        hh, jj = j // 2, 128 * (j % 2)
                        rr = slice(8 * g, 8 * g + 8)
                        cc = slice(jj, jj + 128)
                        first = q == 0
                        gb[slot, hh, pi, 0, rr, cc] = jnp.where(first, 0.0, gb[slot, hh, pi, 0, rr, cc]) + vr
                        gb[slot, hh, pi, 1, rr, cc] = jnp.where(first, 0.0, gb[slot, hh, pi, 1, rr, cc]) + vi
            return carry

        del tw
        lax.fori_loop(0, 4, step, 0)
        for c in stores(b):
            c.start()
    for b in range(max(0, len(plan) - 2), len(plan)):
        for c in stores(b):
            c.wait()


def along_y(name, plan, ints, floats, e1, srcs):
    total = sum(b["rows"] for b in plan)
    rmax = max(b["rows"] for b in plan)
    out = jax.ShapeDtypeStruct((2, 2, total, 256), F32)
    smem = pl.BlockSpec(memory_space=pltpu.SMEM)
    vmem = pl.BlockSpec(memory_space=pltpu.VMEM)
    anys = pl.BlockSpec(memory_space=pl.ANY)
    return pl.pallas_call(
        functools.partial(along_y_kernel, plan),
        out_shape=[out, out],
        in_specs=[smem, smem, vmem, vmem] + [anys] * len(srcs),
        out_specs=[anys, anys],
        scratch_shapes=[
            pltpu.VMEM((2, 16, rmax, 256), F32),
            pltpu.VMEM((4, 2 * rmax, 256), BF16),
            pltpu.VMEM((4, 2 * rmax, 256), BF16),
            pltpu.VMEM((4, 2 * rmax, 256), F32),
            pltpu.VMEM((2, 2, 2, 2, rmax, 256), F32),
            pltpu.VMEM((rmax // 8, 8, 128), F32),
            pltpu.SemaphoreType.DMA((2, 2)),
            pltpu.SemaphoreType.DMA((2, 2)),
        ],
        compiler_params=pltpu.CompilerParams(vmem_limit_bytes=40 << 20),
        cost_estimate=pl.CostEstimate(
            flops=total * 2 * 16 * 3 * 256 * 256 * 2, bytes_accessed=total * 24 * 1024, transcendentals=0
        ),
        name=name,
    )(ints, floats, *e1, *srcs)


def butterfly4(v):
    (r0, i0), (r1, i1), (r2, i2), (r3, i3) = v
    ar, ai, br, bi = r0 + r2, i0 + i2, r0 - r2, i0 - i2
    cr, ci, dr, di = r1 + r3, i1 + i3, r1 - r3, i1 - i3
    return [(ar + cr, ai + ci), (br + di, bi - dr), (ar - cr, ai - ci), (br - di, bi + dr)]


def dft16(v):
    out = [None] * 16
    inner = [butterfly4([v[4 * p + q] for p in range(4)]) for q in range(4)]
    for t0 in range(4):
        col = []
        for q in range(4):
            r, i = inner[q][t0]
            k = (t0 * q) % 16
            if k == 4:
                r, i = i, -r
            elif k:
                c, s = math.cos(2 * math.pi * k / 16), -math.sin(2 * math.pi * k / 16)
                r, i = r * c - i * s, r * s + i * c
            col.append((r, i))
        for t1, val in enumerate(butterfly4(col)):
            out[t0 + 4 * t1] = val
    return out


def along_x_kernel(n_units, ints, tiles, e2h, e2l, k2, pos_a, pos_b, *rest):
    n = len(n_units)
    parts = rest[: 2 * n]
    out = rest[2 * n]
    d, f, grid, wh, wl, lst, sem = rest[2 * n + 1 :]
    core = ints[0]
    u = 0
    for part, cnt in enumerate(n_units):
        def issue(i, carry, part=part, u=u):
            dst = ints[1 + u + i]
            flip = dst + jnp.where((dst >> 4) & 1 == 1, -16, 16)
            for ref, row in ((parts[2 * part], dst), (parts[2 * part + 1], flip)):
                pltpu.make_async_copy(
                    ref.at[:, :, pl.ds(pl.multiple_of(8 * i, 8), 8), :],
                    d.at[:, :, pl.ds(pl.multiple_of(row, 8), 8), :],
                    sem,
                ).start()
            return carry

        lax.fori_loop(0, cnt, issue, 0)
        u += cnt

    def scan(s, cnt):
        t = tiles[s]
        lst[cnt] = s
        mine = jnp.logical_and(t > 0, (((t - 1) >> 1) & 1) == core)
        return cnt + mine.astype(jnp.int32)

    count = lax.fori_loop(0, 256, scan, jnp.int32(0))
    pltpu.make_async_copy(d, d, sem).wait()

    for pi in range(2):
        def first(x0, carry, pi=pi):
            rows = pl.ds(pl.multiple_of(128 * x0, 128), 128)
            x = jnp.concatenate([d[pi, 0, rows, :], d[pi, 1, rows, :]], axis=0)
            h, l = split(x)
            eh = e2h[x0]
            f[x0] = bdot(eh, h) + bdot(e2l[x0], h) + bdot(eh, l)
            return carry

        lax.fori_loop(0, 16, first, 0)

        def second(m, carry, pi=pi):
            rr = pl.ds(pl.multiple_of(8 * m, 8), 8)
            ri = pl.ds(pl.multiple_of(128 + 8 * m, 8), 8)
            for jj in range(2):
                cc = slice(128 * jj, 128 * jj + 128)
                v = dft16([(f[x0, rr, cc], f[x0, ri, cc]) for x0 in range(16)])
                for t in range(16):
                    grid[(pi * 2 + jj) * 16 + t, rr, :] = v[t][0]
                    grid[(pi * 2 + jj) * 16 + t, ri, :] = v[t][1]
            return carry

        lax.fori_loop(0, 16, second, 0)

    sub = lax.broadcasted_iota(jnp.int32, (8, 128), 0)
    table = k2[...]

    def taps(row):
        off = row & 15
        cell = row >> 4
        cl = cell & 7
        idx = off * 8 + ((sub - cl) & 7)
        return jnp.take_along_axis(table, idx, axis=1), (cell >> 3) + (sub < cl).astype(jnp.int32)

    def degrid(sid, z):
        t = tiles[sid] - 1
        pi = (sid >> 1) & 1
        gi = (pi * 2 + (t & 1)) * 16 + (t >> 4)
        half = sid >> 7
        ps = sid & 127
        pos = jnp.where(half == 0, pos_a[ps], pos_b[ps])
        for j in range(4):
            r, h = taps(jnp.broadcast_to(pos[4 + j : 5 + j, :], (8, 128)))
            rh = r.astype(BF16).astype(F32)
            rl = r - rh
            for k in range(8):
                m0, m1 = h == 2 * k, h == 2 * k + 1
                dst = (z, slice(16 * k, 16 * k + 16), slice(128 * j, 128 * j + 128))
                wh[dst] = jnp.concatenate([jnp.where(m0, rh, 0.0), jnp.where(m1, rh, 0.0)], axis=0).astype(BF16)
                wl[dst] = jnp.concatenate([jnp.where(m0, rl, 0.0), jnp.where(m1, rl, 0.0)], axis=0).astype(BF16)
        th, tl = split(grid[gi])
        w = wh[z]
        part = bdot(th, w) + bdot(tl, w) + bdot(th, wl[z])
        rows = []
        for j in range(4):
            r, h = taps(jnp.broadcast_to(pos[j : j + 1, :], (8, 128)))
            for c in range(2):
                acc = jnp.zeros((8, 128), F32)
                for i in range(16):
                    acc = jnp.where(h == i, part[128 * c + 8 * i : 128 * c + 8 * i + 8, 128 * j : 128 * j + 128], acc)
                rows.append(jnp.sum(r * acc, axis=0, keepdims=True))
        out[sid] = jnp.concatenate(rows[0::2] + rows[1::2], axis=0)

    def pair(i, carry):
        degrid(lst[2 * i], 0)
        degrid(lst[jnp.minimum(2 * i + 1, count - 1)], 1)
        return carry

    lax.fori_loop(0, (count + 1) >> 1, pair, 0)


def along_x(n_units, ints, tiles, e2, k2, pos_a, pos_b, parts):
    smem = pl.BlockSpec(memory_space=pltpu.SMEM)
    vmem = pl.BlockSpec(memory_space=pltpu.VMEM)
    anys = pl.BlockSpec(memory_space=pl.ANY)
    return pl.pallas_call(
        functools.partial(along_x_kernel, n_units),
        out_shape=jax.ShapeDtypeStruct((256, 8, 128), F32),
        in_specs=[smem, smem, vmem, vmem, vmem, vmem, vmem] + [anys] * len(parts),
        out_specs=vmem,
        scratch_shapes=[
            pltpu.VMEM((2, 2, N, 256), F32),
            pltpu.VMEM((16, 256, 256), F32),
            pltpu.VMEM((64, 256, 128), F32),
            pltpu.VMEM((2, 128, 512), BF16),
            pltpu.VMEM((2, 128, 512), BF16),
            pltpu.SMEM((264,), jnp.int32),
            pltpu.SemaphoreType.DMA,
        ],
        compiler_params=pltpu.CompilerParams(vmem_limit_bytes=50 << 20),
        cost_estimate=pl.CostEstimate(flops=60_000_000_000, bytes_accessed=16 << 20, transcendentals=0),
        name="along_x",
    )(ints, tiles, *e2, k2, pos_a, pos_b, *parts)


def shift(x, axes, size, by):
    return lax.ppermute(x, axes, [(i, (i + by) % size) for i in range(size)])


def shards(sky, plane_w, kernel, tile_ids, plane_ids, positions, observed):
    i32 = jnp.int32
    xc, yc = lax.axis_index("x"), lax.axis_index("y")
    core, a = lax.axis_index("core"), lax.axis_index("wa")
    z_axes, c_axes = ("zh", "wa"), ("zh", "x", "y")
    swap = [(0, 1), (1, 0)]

    target = plane_ids[:, 0]
    same = (target[:, None] == target[None, :]).astype(i32)
    rank = jnp.sum(jnp.tril(same, -1), axis=1)
    slot = target * 2 + rank
    pos = positions.reshape(16, 8, 128)
    slot_pos = jnp.zeros((128, 8, 128), i32).at[slot].set(pos, unique_indices=True)
    slot_tile = jnp.zeros((128,), i32).at[slot].set(tile_ids + 1, unique_indices=True)
    tile_row = jnp.pad(slot_tile.reshape(32, 1, 4), ((0, 0), (0, 7), (0, 124)))
    payload = jnp.concatenate([slot_pos.reshape(32, 32, 128), tile_row], axis=1)
    asked = lax.all_to_all(payload, c_axes, split_axis=0, concat_axis=0, tiled=True)
    asked_b = lax.ppermute(asked, "core", swap)
    other_w = lax.ppermute(plane_w, "core", swap)
    w0 = jnp.where(core == 0, plane_w[0], other_w[0])
    w1 = jnp.where(core == 0, other_w[0], plane_w[0])

    own = turn(jnp.reshape(core, (1,)), sky)
    e1h, e1l, e2h, e2l = tables()
    R = AROWS
    piece_a = lax.dynamic_slice(own, (4 * xc, R * yc, 0), (4, R, 256))
    piece_b = lax.dynamic_slice(own, (4 * yc, 4 * R + R * xc, 0), (4, R, 256))
    piece_c = own[:, 8 * R :, :]
    piece = jnp.concatenate([piece_a, piece_b], axis=0)
    zl = shift(piece, z_axes, 8, 1)
    zr = shift(piece, z_axes, 8, -1)
    za = shift(zl[:4], z_axes, 8, 1)
    zb = shift(zr[4:], z_axes, 8, -1)
    cl = shift(piece_c, z_axes, 8, 1)
    cr = shift(piece_c, z_axes, 8, -1)
    cfl = shift(cl[:8], z_axes, 8, 1)
    cfr = shift(cr[8:], z_axes, 8, -1)

    def planar(mine, first, second):
        l = shift(mine, first, 4, 1)
        r = shift(mine, first, 4, -1)
        lo = shift(l[:2], first, 4, 1)
        hi = shift(r[2:], first, 4, -1)
        whole = jnp.concatenate([mine, r, lo, hi, l], axis=0)
        nl = shift(whole, second, 4, 1)
        nr = shift(whole, second, 4, -1)
        nlo = shift(nl[:8], second, 4, 1)
        nhi = shift(nr[8:], second, 4, -1)
        return whole, nl, nr, nlo, nhi

    mine_a = jnp.concatenate([zl[:4], zr[:4], za], axis=1)
    mine_b = jnp.concatenate([zl[4:], zr[4:], zb], axis=1)
    a0, al, ar, alo, ahi = planar(mine_a, "x", "y")
    b0, bl, br, blo, bhi = planar(mine_b, "y", "x")

    sl = (a + 3) & 3, (a + 1) & 3, (a + 2) & 3
    sevens = jnp.arange(0, 4096, 8, dtype=i32)

    def rows_x(slab, row):
        j0, jh = row >> 4, (row >> 3) & 1
        return 512 * slab + 256 * core + 128 * jh + j0, 128 * j0 + 32 * slab + 16 * core + 8 * jh

    def run(slab, start, rows):
        r = start + sevens[: rows // 8]
        return rows_x(slab, r)

    def block_ab(start):
        parts = [run(s, start, R) for s in sl]
        return [jnp.concatenate(v) for v in zip(*parts)]

    def call(name, blocks, srcs):
        plan, bases, xs, ds, off = [], [], [], [], 0
        for rows, src, base, (x, dst) in blocks:
            plan.append(dict(rows=rows, src=src, off=off))
            off += rows
            bases.append(base)
            xs.append(x)
            ds.append(dst)
        bases = jnp.stack([jnp.asarray(v, i32) for v in bases])
        xs, ds = jnp.concatenate(xs), jnp.concatenate(ds)
        j = jnp.arange(4, dtype=i32)[None, :, None]
        q = jnp.arange(4, dtype=i32)[None, None, :]
        k = ((4 * a + j) * q + 4 * j * bases[:, None, None]) & 15
        ang = k.astype(F32) * (2.0 * math.pi / 16)
        tw = jnp.stack([jnp.cos(ang), -jnp.sin(ang)], axis=-1).reshape(-1)
        floats = jnp.concatenate([jnp.stack([w0, w1]), tw])
        ints = jnp.concatenate([core[None].astype(i32), bases, xs])
        keep, send = along_y(name, plan, ints, floats, (e1h, e1l), srcs)
        return keep, lax.ppermute(send, "core", swap), ds

    one = lambda s: [(s, 0, 0, 16)]
    two = lambda s: [(s, 0, 0, 8), (s + 1, 0, 8, 8)]
    calls = [
        call("along_y_own", [(64, [(0, 64 * k, 0, 16)], 0, run(a, 64 * k, 64)) for k in range(4)], [own]),
        call(
            "along_y_near",
            [
                (CROWS, one(0), 0, run(sl[0], 8 * R, CROWS)),
                (CROWS, one(1), 0, run(sl[1], 8 * R, CROWS)),
                (CROWS, two(2), 0, run(sl[2], 8 * R, CROWS)),
                (3 * R, one(4), xc, block_ab(R * yc)),
                (3 * R, one(5), yc, block_ab(4 * R + R * xc)),
            ],
            [cl, cr, cfl, cfr, a0, b0],
        ),
        call(
            "along_y_beside",
            [
                (3 * R, one(0), xc, block_ab(R * ((yc + 3) & 3))),
                (3 * R, one(1), xc, block_ab(R * ((yc + 1) & 3))),
                (3 * R, one(2), yc, block_ab(4 * R + R * ((xc + 3) & 3))),
                (3 * R, one(3), yc, block_ab(4 * R + R * ((xc + 1) & 3))),
            ],
            [al, ar, bl, br],
        ),
        call(
            "along_y_far",
            [
                (3 * R, two(0), xc, block_ab(R * ((yc + 2) & 3))),
                (3 * R, two(2), yc, block_ab(4 * R + R * ((xc + 2) & 3))),
            ],
            [alo, ahi, blo, bhi],
        ),
    ]

    parts, dests = [], []
    for keep, got, ds in calls:
        parts += [keep, got]
        dests.append(ds)
    ints = jnp.concatenate([core[None].astype(i32)] + dests)
    tiles_a = asked[:, 32, :4].reshape(128)
    tiles_b = asked_b[:, 32, :4].reshape(128)
    k2 = jnp.broadcast_to(kernel.reshape(1, 128), (8, 128))
    values = along_x(
        tuple(d.shape[0] for d in dests),
        ints,
        jnp.concatenate([tiles_a, tiles_b]),
        (e2h, e2l),
        k2,
        asked[:, :32].reshape(128, 8, 128),
        asked_b[:, :32].reshape(128, 8, 128),
        parts,
    )
    from_b = lax.ppermute(values[128:], "core", swap)
    here = (((tiles_a - 1) >> 1) & 1) == core
    merged = jnp.where(here[:, None, None], values[:128], from_b)
    answers = lax.all_to_all(merged.reshape(32, 32, 128), c_axes, split_axis=0, concat_axis=0, tiled=True)
    predicted = answers.reshape(128, 8, 128)[slot]
    return observed - predicted.reshape(16, 2, 512)


def solution(mesh):
    fine = Mesh(mesh.devices.reshape(2, 4, 4, 2, 4), ("zh", "x", "y", "core", "wa"))
    ba = ("zh", "x", "y", "core")
    rows = ba + ("wa",)
    return jax.shard_map(
        shards,
        mesh=fine,
        in_specs=(
            P(None, None, "wa"),
            P(ba),
            P(),
            P(rows),
            P(rows, None),
            P(rows, None, None),
            P(rows, None, None),
        ),
        out_specs=P(rows, None, None),
        check_vma=False,
    )
```

```python
import functools

import jax
import jax.numpy as jnp
from jax import lax
from jax.experimental import pallas as pl
from jax.experimental.pallas import tpu as pltpu
from jax.sharding import Mesh
from jax.sharding import PartitionSpec as P


N = 2048
SP = 0.7 / N
R = 16
CR = 128
SMEM = pl.BlockSpec(memory_space=pltpu.SMEM)
VMEM = pl.BlockSpec(memory_space=pltpu.VMEM)
HBM = pl.BlockSpec(memory_space=pltpu.HBM)
F32 = jnp.float32
BF16 = jnp.bfloat16

SIN_C = (3.14159264, -5.16771009, 2.55007766, -0.59829216, 0.07765941)
COS_C = (1.0, -4.93480214, 4.05870916, -1.33521206, 0.23493756, -0.02439672)
G_C = (0.5, 0.12500105, 0.0624521, 0.03985648, 0.0215331, 0.03890036)
MAGIC = 12582912.0


def horner(z, coefs):
    acc = jnp.full_like(z, coefs[-1])
    for c in coefs[-2::-1]:
        acc = acc * z + c
    return acc


def cis_turns(t):
    r = t - ((t + MAGIC) - MAGIC)
    z = r * r
    s = r * horner(z, SIN_C)
    c = horner(z, COS_C)
    s2 = s + s
    return 1.0 - s2 * s, s2 * c


def split(x):
    hi = x.astype(BF16)
    return hi, (x - hi.astype(F32)).astype(BF16)


def bdot(a, b):
    return jnp.dot(a, b, preferred_element_type=F32)


def tables_kernel(ids, e1h, e1l, e2h, e2l, tw1, tw2):
    row = lax.broadcasted_iota(jnp.int32, (128, 128), 0)
    col = lax.broadcasted_iota(jnp.int32, (128, 128), 1)
    lane = lax.broadcasted_iota(jnp.int32, (8, 128), 1)

    def cs(k):
        return cis_turns((k & (N - 1)).astype(F32) * (1.0 / N))

    def put(h, l, i, r, c, v):
        a, b = v
        h[i, 128 * r : 128 * r + 128, 128 * c : 128 * c + 128] = a
        l[i, 128 * r : 128 * r + 128, 128 * c : 128 * c + 128] = b

    for p in range(4):
        y = 16 * (127 - row if p > 1 else row) + 4 * p
        c, s = cs(col * y)
        ch, sh = split(c), split(s)
        put(e1h, e1l, p, 0, 0, ch)
        put(e1h, e1l, p, 1, 1, ch)
        put(e1h, e1l, p, 0, 1, (-sh[0], -sh[1]))
        put(e1h, e1l, p, 1, 0, sh)
        c, s = cs(row * (16 * col + 4 * p))
        ch, sh = split(c * (1.0 / N)), split(s * (1.0 / N))
        put(e2h, e2l, p, 0, 0, ch)
        put(e2h, e2l, p, 1, 1, ch)
        put(e2h, e2l, p, 0, 1, sh)
        put(e2h, e2l, p, 1, 0, (-sh[0], -sh[1]))
    for q in range(1, 4):
        for j in range(4):
            k = 4 * (q - 1) + j
            c, s = cs((512 * ids[1] + 128 * j + lane) * q)
            tw1[2 * k] = c
            tw1[2 * k + 1] = -s
            c, s = cs((128 * j + row) * q)
            tw2[0, k] = c
            tw2[1, k] = -s


def tables(ids):
    sds = jax.ShapeDtypeStruct
    shapes = [sds((4, 256, 256), BF16)] * 4 + [sds((24, 8, 128), F32), sds((2, 12, 128, 128), F32)]
    return pl.pallas_call(
        tables_kernel,
        out_shape=shapes,
        in_specs=[SMEM],
        out_specs=[VMEM] * 6,
        cost_estimate=pl.CostEstimate(flops=60 * 16 * 2 * 16384, bytes_accessed=4 << 20, transcendentals=0),
        name="tables",
    )(ids)


def turn_kernel(b, ids, sky, own, *rest):
    outs, (xin, t, tmp, sem_in, sem_out) = rest[:-5], rest[-5:]
    core, xc, yc = ids[0], ids[2], ids[3]
    loads = []
    for c in range(2):
        col = pl.multiple_of(256 * core + 128 * b, 128)
        loads.append(pltpu.make_async_copy(sky.at[c, :, pl.ds(col, 128)], xin.at[c], sem_in.at[c]))
        loads[c].start()
    moves = []

    def move(src, dst):
        moves.append(pltpu.make_async_copy(src, dst, sem_out.at[len(moves)]))
        moves[-1].start()

    rev = 127 - lax.broadcasted_iota(jnp.int32, (128, 128), 1)
    for y0 in range(16):
        for c in range(2):
            if y0 == 0:
                loads[c].wait()
            v = xin[c, pl.ds(y0, 128, stride=16), :].T
            if y0 > 7:
                v = jnp.take_along_axis(v, rev, axis=1)
            z = 2 * (y0 % 2) + c
            tmp[z] = v
            for j0 in range(16):
                t[y0, 8 * j0 : 8 * j0 + 8, 128 * c : 128 * c + 128] = tmp[z, pl.ds(j0, 8, stride=16), :]
        if y0 % 4 == 3 and y0 < 15:
            move(t.at[pl.ds(y0 - 3, 4)], own.at[pl.ds(y0 - 3, 4)])
    if outs:
        a_src = t.at[pl.ds(4 * xc, 4), pl.ds(pl.multiple_of(R * yc, 8), R), :]
        b_src = t.at[pl.ds(4 * yc, 4), pl.ds(pl.multiple_of(4 * R + R * xc, 8), R), :]
        ab, pa, pb = outs
        move(a_src, ab.at[0])
        move(b_src, ab.at[1])
        move(a_src, pa)
        move(b_src, pb)
    move(t.at[pl.ds(12, 4)], own.at[pl.ds(12, 4)])
    for m in moves:
        m.wait()


def turn(b, ids, sky):
    sds = lambda *d: jax.ShapeDtypeStruct(d, F32)
    outs = [sds(16, 128, 256)] + [sds(2, 4, R, 256), sds(4, R, 256), sds(4, R, 256)] * (1 - b)
    return pl.pallas_call(
        functools.partial(turn_kernel, b),
        in_specs=[SMEM, HBM],
        out_specs=[HBM] * len(outs),
        out_shape=outs,
        scratch_shapes=[
            pltpu.VMEM((2, N, 128), F32),
            pltpu.VMEM((16, 128, 256), F32),
            pltpu.VMEM((4, 128, 128), F32),
            pltpu.SemaphoreType.DMA((2,)),
            pltpu.SemaphoreType.DMA((8,)),
        ],
        cost_estimate=pl.CostEstimate(flops=1 << 22, bytes_accessed=4 << 20, transcendentals=0),
    )(ids, sky)


def gather3_kernel(zl, zr, za, zb, oa, ob):
    for k, (o, far) in enumerate(((oa, za), (ob, zb))):
        o[:, 0:R, :] = zl[k]
        o[:, R : 2 * R, :] = zr[k]
        o[:, 2 * R : 3 * R, :] = far[...]


def gather3(*z):
    return pl.pallas_call(
        gather3_kernel,
        out_shape=[jax.ShapeDtypeStruct((4, 3 * R, 256), F32)] * 2,
        in_specs=[VMEM] * 4,
        out_specs=[VMEM] * 2,
        compiler_params=pltpu.CompilerParams(vmem_limit_bytes=8 << 20),
        cost_estimate=pl.CostEstimate(flops=1 << 20, bytes_accessed=1 << 20, transcendentals=0),
        name="gather3",
    )(*z)


def join_kernel(ids, *refs):
    for k in range(4):
        for base, ref, o in ((ids[2], refs[k], refs[8]), (ids[3], refs[4 + k], refs[9])):
            o[pl.ds(4 * ((base + k) & 3), 4)] = ref[...]


def join(ids, a, b):
    return pl.pallas_call(
        join_kernel,
        out_shape=[jax.ShapeDtypeStruct((16, 3 * R, 256), F32)] * 2,
        in_specs=[SMEM] + [VMEM] * 8,
        out_specs=[VMEM] * 2,
        compiler_params=pltpu.CompilerParams(vmem_limit_bytes=16 << 20),
        cost_estimate=pl.CostEstimate(flops=1 << 20, bytes_accessed=3 << 20, transcendentals=0),
        name="join",
    )(ids, *a, *b)


def slab_of(kind, k, ids):
    a = ids[1]
    return (a + (0 if kind == "own" else (3, 1, 2)[k])) & 3


def block_rows(blk, ids):
    kind, d, n = blk["kind"], blk["d"], blk["rows"]
    if kind == "own":
        return [(slab_of(kind, 0, ids), d, n // 8)]
    if kind == "c":
        return [(slab_of(kind, d, ids), 128, n // 8)]
    first = R * ((ids[3] + d) & 3) if kind == "a" else 4 * R + R * ((ids[2] + d) & 3)
    return [(slab_of(kind, k, ids), first, R // 8) for k in range(3)]


def along_y_kernel(plan, n_src, ids, ws, e1h, e1l, tw1, *rest):
    srcs = rest[:n_src]
    keep, send = rest[n_src : n_src + 2]
    eh, el, tw, xin, xh0, xl0, yb0, xh1, xl1, yb1, gb, cs, tab, where, sem_e, sem_in, sem_out = rest[n_src + 2 :]
    core = ids[0]
    lane = lax.broadcasted_iota(jnp.int32, (8, 128), 1)
    sub = lax.broadcasted_iota(jnp.int32, (8, 128), 0)
    w = [ws[0], ws[1]]
    n_pairs = sum(blk["rows"] for blk in plan) // 16
    steps = n_pairs // 2

    e_copies = [
        pltpu.make_async_copy(src, dst, sem_e.at[i]) for i, (src, dst) in enumerate(((e1h, eh), (e1l, el), (tw1, tw)))
    ]
    for c in e_copies:
        c.start()
    kinds, k = [], 0
    for blk in plan:
        if blk["src"] not in kinds:
            kinds.append(blk["src"])
        for i in range(blk["rows"] // 16):
            where[2 * k] = kinds.index(blk["src"])
            where[2 * k + 1] = blk["row"] + 16 * i
            k += 1
    k = 0
    for blk in plan:
        for slab, first, n in block_rows(blk, ids):
            for i in range(n):
                row = first + 8 * i
                tab[k] = 512 * slab + 256 * core + 128 * (row >> 7) + ((row >> 3) & 15)
                k += 1

    def load(pair, slot, a):
        kind, row = where[2 * pair], pl.ds(pl.multiple_of(where[2 * pair + 1], 16), 16)
        for i, src in enumerate(kinds):
            @pl.when(kind == i)
            def _(src=src):
                h = 16 // len(src)
                for j, s in enumerate(src):
                    pltpu.make_async_copy(
                        srcs[s].at[:, row, :], xin.at[slot, a, pl.ds(h * j, h)], sem_in.at[slot, a]
                    ).start()

    def stores(k, slot):
        out = []
        for a in range(2):
            dst = pl.ds(pl.multiple_of(32 * k + 16 * a, 16), 16)
            out.append(pltpu.make_async_copy(gb.at[slot, a, core], keep.at[:, :, dst, :], sem_out.at[slot, a, 0]))
            out.append(pltpu.make_async_copy(gb.at[slot, a, 1 - core], send.at[:, :, dst, :], sem_out.at[slot, a, 1]))
        return out

    for k in range(min(2, steps)):
        for a in range(2):
            load(2 * k + a, k, a)
    for c in e_copies:
        c.wait()

    def image(pair, slot, s, xh, xl):
        for a in range(2):
            cx = ((tab[2 * pair + a] + 16 * sub).astype(F32) - N / 2) * SP
            cx2 = cx * cx
            for y0 in range(16):
                p, q = y0 // 4, y0 % 4
                kap = min(y0, 16 - y0)
                if y0 <= 8:
                    cy = ((16 * lane + kap).astype(F32) - N / 2) * SP
                    r2 = cx2 + cy * cy
                    t = r2 * horner(r2, G_C)
                    pairs = [cis_turns(t * w[pi]) for pi in range(2)]
                    if 0 < y0 < 8:
                        for pi in range(2):
                            cs[s, a, kap, pi, 0] = pairs[pi][0]
                            cs[s, a, kap, pi, 1] = pairs[pi][1]
                else:
                    pairs = [(cs[s, a, kap, pi, 0], cs[s, a, kap, pi, 1]) for pi in range(2)]
                sr = xin[slot, s, y0, 8 * a : 8 * a + 8, 0:128]
                si = xin[slot, s, y0, 8 * a : 8 * a + 8, 128:256]
                dst = slice(64 * a + 16 * q, 64 * a + 16 * q + 16)
                h, l = split(jnp.concatenate([sr * c - si * n for c, n in pairs], axis=0))
                xh[p, dst, 0:128] = h
                xl[p, dst, 0:128] = l
                h, l = split(jnp.concatenate([sr * n + si * c for c, n in pairs], axis=0))
                xh[p, dst, 128:256] = h
                xl[p, dst, 128:256] = l

    def long_part(xh, xl, yb):
        for p in range(4):
            x = xh[p]
            yb[p] = bdot(x, eh[p]) + bdot(xl[p], eh[p]) + bdot(x, el[p])

    def short_part(slot, s, yb):
        for a in range(2):
            for pi in range(2):
                sums = None
                for q in range(4):
                    r0 = 64 * a + 16 * q + 8 * pi
                    v = butterfly4([(yb[p, r0 : r0 + 8, 0:128], yb[p, r0 : r0 + 8, 128:256]) for p in range(4)])
                    if q:
                        out = []
                        for j, (r, i) in enumerate(v):
                            k = 8 * (q - 1) + 2 * j
                            out.append((r * tw[k] - i * tw[k + 1], r * tw[k + 1] + i * tw[k]))
                        v = out
                    sums = v if sums is None else [(x + u, y + z) for (x, y), (u, z) in zip(sums, v)]
                for j, (vr, vi) in enumerate(sums):
                    cc = slice(128 * (j % 2), 128 * (j % 2) + 128)
                    gb[slot, s, j // 2, pi, 0, 8 * a : 8 * a + 8, cc] = vr
                    gb[slot, s, j // 2, pi, 1, 8 * a : 8 * a + 8, cc] = vi

    def step(k, slot3):
        @pl.when(k >= 2)
        def _():
            for c in stores(k - 2, k & 1):
                c.start()

        @pl.when(k >= 3)
        def _():
            for c in stores(k - 3, 1 - (k & 1)):
                c.wait()

        ahead = jnp.where(slot3 == 0, 2, slot3 - 1)

        @pl.when(k + 2 < steps)
        def _():
            for a in range(2):
                load(2 * k + 4 + a, ahead, a)

        for a in range(2):
            pltpu.make_async_copy(xin.at[slot3, a], xin.at[slot3, a], sem_in.at[slot3, a]).wait()
        done = 1 - (k & 1)
        long_part(xh1, xl1, yb1)
        short_part(done, 0, yb0)
        image(2 * k, slot3, 0, xh0, xl0)
        long_part(xh0, xl0, yb0)
        short_part(done, 1, yb1)
        image(2 * k + 1, slot3, 1, xh1, xl1)
        return jnp.where(slot3 == 2, 0, slot3 + 1)

    lax.fori_loop(0, steps, step, jnp.int32(0))
    last = (steps - 1) % 2
    if steps >= 2:
        for c in stores(steps - 2, steps % 2):
            c.start()
    if steps >= 3:
        for c in stores(steps - 3, last):
            c.wait()
    long_part(xh1, xl1, yb1)
    short_part(last, 0, yb0)
    short_part(last, 1, yb1)
    for c in stores(steps - 1, last):
        c.start()
    if steps >= 2:
        for c in stores(steps - 2, steps % 2):
            c.wait()
    for c in stores(steps - 1, last):
        c.wait()


def along_y(plan, ids, ws, e1, srcs):
    total = sum(blk["rows"] for blk in plan)
    out = jax.ShapeDtypeStruct((2, 2, total, 256), F32)
    stage = [pltpu.VMEM((4, 128, 256), BF16), pltpu.VMEM((4, 128, 256), BF16), pltpu.VMEM((4, 128, 256), F32)]
    return pl.pallas_call(
        functools.partial(along_y_kernel, plan, len(srcs)),
        out_shape=[out, out],
        in_specs=[SMEM, SMEM] + [HBM] * (3 + len(srcs)),
        out_specs=[HBM, HBM],
        scratch_shapes=[
            pltpu.VMEM((4, 256, 256), BF16),
            pltpu.VMEM((4, 256, 256), BF16),
            pltpu.VMEM((24, 8, 128), F32),
            pltpu.VMEM((3, 2, 16, 16, 256), F32),
            *stage,
            *stage,
            pltpu.VMEM((2, 2, 2, 2, 2, 16, 256), F32),
            pltpu.VMEM((2, 2, 8, 2, 2, 8, 128), F32),
            pltpu.SMEM((total // 8,), jnp.int32),
            pltpu.SMEM((total // 8,), jnp.int32),
            pltpu.SemaphoreType.DMA((3,)),
            pltpu.SemaphoreType.DMA((3, 2)),
            pltpu.SemaphoreType.DMA((2, 2, 2)),
        ],
        cost_estimate=pl.CostEstimate(
            flops=total * 2 * 16 * 3 * 256 * 256 * 2, bytes_accessed=total * 24 * 1024, transcendentals=0
        ),
    )(ids, ws, *e1, *srcs)


def butterfly4(v):
    (r0, i0), (r1, i1), (r2, i2), (r3, i3) = v
    ar, ai, br, bi = r0 + r2, i0 + i2, r0 - r2, i0 - i2
    cr, ci, dr, di = r1 + r3, i1 + i3, r1 - r3, i1 - i3
    return [(ar + cr, ai + ci), (br + di, bi - dr), (ar - cr, ai - ci), (br - di, bi + dr)]


def dft16(v, tw):
    out = [None] * 16
    inner = [butterfly4([v[4 * p + q] for p in range(4)]) for q in range(4)]
    for t0 in range(4):
        cols = [inner[0][t0]]
        for q in range(1, 4):
            (r, i), (c, s) = inner[q][t0], tw(4 * (q - 1) + t0)
            cols.append((r * c - i * s, r * s + i * c))
        for t1, val in enumerate(butterfly4(cols)):
            out[t0 + 4 * t1] = val
    return out


def along_x_kernel(plans, ids, tiles, eh, el, tw, k2, pos_a, pos_b, *rest):
    n = len(plans)
    parts = rest[: 2 * n]
    out_a, out_b = rest[2 * n : 2 * n + 2]
    d, f, grid, ww, wl, ru, hu, res, lst, sem, sem_o = rest[2 * n + 2 :]
    core = ids[0]
    for i, plan in enumerate(plans):
        off = 0
        for blk in plan:
            for slab, first, cnt in block_rows(blk, ids):
                def issue(k, carry, i=i, slab=slab, first=first, off=off):
                    row = first + 8 * k
                    base = 128 * ((row >> 3) & 15) + 32 * slab + 8 * (row >> 7)
                    src = pl.ds(pl.multiple_of(off + 8 * k, 8), 8)
                    for ref, dst in ((parts[2 * i], base + 16 * core), (parts[2 * i + 1], base + 16 * (1 - core))):
                        pltpu.make_async_copy(
                            ref.at[:, :, src, :], d.at[:, :, pl.ds(pl.multiple_of(dst, 8), 8), :], sem
                        ).start()
                    return carry

                lax.fori_loop(0, cnt, issue, 0)
                off += 8 * cnt

    def scan(s, cnt):
        t = tiles[s]
        lst[cnt] = s
        mine = jnp.logical_and(t > 0, (((t - 1) >> 1) & 1) == core)
        return cnt + mine.astype(jnp.int32)

    lst[0] = 0
    count = lax.fori_loop(0, 256, scan, jnp.int32(0))
    last = jnp.where(count > 0, lst[jnp.maximum(count - 1, 0)], 0)
    for k in range(4):
        lst[count + k] = last
    pltpu.make_async_copy(d, d, sem).wait()

    for pi in range(2):
        def first(k, carry, pi=pi):
            for q in range(4):
                x0 = 4 * k + q
                rows = pl.ds(pl.multiple_of(128 * x0, 128), 128)
                h, l = split(jnp.concatenate([d[pi, 0, rows, :], d[pi, 1, rows, :]], axis=0))
                f[x0] = bdot(eh[k], h) + bdot(el[k], h) + bdot(eh[k], l)
            return carry

        lax.fori_loop(0, 4, first, 0)

        def second(m, carry, pi=pi):
            rr = pl.ds(pl.multiple_of(8 * m, 8), 8)
            ri = pl.ds(pl.multiple_of(128 + 8 * m, 8), 8)
            for jj in range(2):
                cc = slice(128 * jj, 128 * jj + 128)
                v = dft16([(f[x0, rr, cc], f[x0, ri, cc]) for x0 in range(16)], lambda k: (tw[0, k, rr, :], tw[1, k, rr, :]))
                for t in range(16):
                    grid[(pi * 2 + jj) * 16 + t, rr, :] = v[t][0]
                    grid[(pi * 2 + jj) * 16 + t, ri, :] = v[t][1]
            return carry

        lax.fori_loop(0, 16, second, 0)

    sub = lax.broadcasted_iota(jnp.int32, (8, 128), 0)
    table = k2[...]

    def taps(row):
        off = row & 15
        cell = row >> 4
        cl = cell & 7
        idx = off * 8 + ((sub - cl) & 7)
        return jnp.take_along_axis(table, idx, axis=1), (cell >> 3) + (sub < cl).astype(jnp.int32)

    def build(sid, z):
        who, rr = (sid & 127) >> 2, pl.ds(pl.multiple_of(8 * (sid & 3), 8), 8)
        pos = jnp.where(sid < 128, pos_a[who, rr, :], pos_b[who, rr, :])
        for j in range(4):
            r, h = taps(jnp.broadcast_to(pos[4 + j : 5 + j, :], (8, 128)))
            rh = r.astype(BF16).astype(F32)
            rl = r - rh
            cc = slice(128 * j, 128 * j + 128)
            for k in range(8):
                m0, m1 = h == 2 * k, h == 2 * k + 1
                wh = jnp.concatenate([jnp.where(m0, rh, 0.0), jnp.where(m1, rh, 0.0)], axis=0).astype(BF16)
                ww[z, 16 * k : 16 * k + 16, cc] = wh
                ww[z, 128 + 16 * k : 144 + 16 * k, cc] = wh
                wl[z, 16 * k : 16 * k + 16, cc] = jnp.concatenate(
                    [jnp.where(m0, rl, 0.0), jnp.where(m1, rl, 0.0)], axis=0
                ).astype(BF16)
            r, h = taps(jnp.broadcast_to(pos[j : j + 1, :], (8, 128)))
            ru[z, j] = r
            hu[z, j] = h

    def finish(sid, z):
        t = jnp.maximum(tiles[sid] - 1, 0)
        gi = (((sid >> 1) & 1) * 2 + (t & 1)) * 16 + (t >> 4)
        th, tl = split(grid[gi])
        part = bdot(jnp.concatenate([th, tl], axis=1), ww[z]) + bdot(th, wl[z])
        rows = []
        for j in range(4):
            r, h = ru[z, j], hu[z, j]
            for c in range(2):
                acc = jnp.zeros((8, 128), F32)
                for i in range(16):
                    acc = jnp.where(h == i, part[128 * c + 8 * i : 128 * c + 8 * i + 8, 128 * j : 128 * j + 128], acc)
                rows.append(jnp.sum(r * acc, axis=0, keepdims=True))
        res[sid] = jnp.concatenate(rows[0::2] + rows[1::2], axis=0)

    build(lst[0], 0)
    build(lst[1], 1)

    def pair(i, carry):
        z = 2 * (i & 1)
        for k in range(2):
            finish(lst[2 * i + k], z + k)
            build(lst[2 * i + 2 + k], 2 - z + k)
        return carry

    lax.fori_loop(0, (count + 1) >> 1, pair, 0)
    moves = [
        pltpu.make_async_copy(res.at[pl.ds(0, 128)], out_a, sem_o.at[0]),
        pltpu.make_async_copy(res.at[pl.ds(128, 128)], out_b, sem_o.at[1]),
    ]
    for m in moves:
        m.start()
    for m in moves:
        m.wait()


def along_x(plans, ids, tiles, e2, k2, pos_a, pos_b, parts):
    return pl.pallas_call(
        functools.partial(along_x_kernel, plans),
        out_shape=[jax.ShapeDtypeStruct((128, 8, 128), F32)] * 2,
        in_specs=[SMEM, SMEM] + [VMEM] * 6 + [HBM] * len(parts),
        out_specs=[HBM, HBM],
        scratch_shapes=[
            pltpu.VMEM((2, 2, N, 256), F32),
            pltpu.VMEM((16, 256, 256), F32),
            pltpu.VMEM((64, 256, 128), F32),
            pltpu.VMEM((4, 256, 512), BF16),
            pltpu.VMEM((4, 128, 512), BF16),
            pltpu.VMEM((4, 4, 8, 128), F32),
            pltpu.VMEM((4, 4, 8, 128), jnp.int32),
            pltpu.VMEM((256, 8, 128), F32),
            pltpu.SMEM((264,), jnp.int32),
            pltpu.SemaphoreType.DMA,
            pltpu.SemaphoreType.DMA((2,)),
        ],
        cost_estimate=pl.CostEstimate(flops=60_000_000_000, bytes_accessed=16 << 20, transcendentals=0),
        name="along_x",
    )(ids, tiles, *e2, k2, pos_a, pos_b, *parts)


def shift(x, axes, size, by):
    return lax.ppermute(x, axes, [(i, (i + by) % size) for i in range(size)])


def shards(sky, plane_w, kernel, tile_ids, plane_ids, positions, observed):
    i32 = jnp.int32
    core = lax.axis_index("core")
    ids = jnp.stack([core, lax.axis_index("wa"), lax.axis_index("x"), lax.axis_index("y")]).astype(i32)
    z_axes, c_axes = ("zh", "wa"), ("zh", "x", "y")
    swap = [(0, 1), (1, 0)]

    own0, ab, pa, pb = turn(0, ids, sky)
    zl = shift(ab, z_axes, 8, 1)
    zr = shift(ab, z_axes, 8, -1)
    za = shift(pa, z_axes, 8, 2)
    zb = shift(pb, z_axes, 8, -2)
    (own1,) = turn(1, ids, sky)
    cl = shift(own1, z_axes, 8, 1)
    cr = shift(own1, z_axes, 8, -1)
    cf_lo = shift(cl[:8], z_axes, 8, 1)
    cf_hi = shift(cr[8:], z_axes, 8, -1)

    mine_a, mine_b = gather3(zl, zr, za, zb)

    def three(x, axis):
        l = shift(x, axis, 4, 1)
        r = shift(x, axis, 4, -1)
        return r, shift(x, axis, 4, 2), l

    ax, bx = three(mine_a, "x"), three(mine_b, "y")
    a0, b0 = join(ids, (mine_a,) + ax, (mine_b,) + bx)
    ar, af, al = three(a0, "y")
    br, bf, bl = three(b0, "x")

    target = plane_ids[:, 0]
    same = (target[:, None] == target[None, :]).astype(i32)
    rank = jnp.sum(jnp.tril(same, -1), axis=1)
    slot = target * 2 + rank
    pos = positions.reshape(16, 8, 128)
    slot_pos = jnp.zeros((128, 8, 128), i32).at[slot].set(pos, unique_indices=True)
    slot_tile = jnp.zeros((128,), i32).at[slot].set(tile_ids + 1, unique_indices=True)
    tile_row = jnp.pad(slot_tile.reshape(32, 1, 4), ((0, 0), (0, 7), (0, 124)))
    payload = jnp.concatenate([slot_pos.reshape(32, 32, 128), tile_row], axis=1)
    asked = lax.all_to_all(payload, c_axes, split_axis=0, concat_axis=0, tiled=True)
    asked_b = lax.ppermute(asked, "core", swap)
    other_w = lax.ppermute(plane_w, "core", swap)
    ws = jnp.where(core == 0, jnp.concatenate([plane_w, other_w]), jnp.concatenate([other_w, plane_w]))
    tiles_a = asked[:, 32, :4].reshape(128)
    tiles_b = asked_b[:, 32, :4].reshape(128)
    tiles = jnp.concatenate([tiles_a, tiles_b])

    *e1, tw1, tw2 = tables(ids)
    e1, e2 = e1[:2] + [tw1], e1[2:] + [tw2]
    plans, parts = [], []

    def call(plan, srcs):
        keep, send = along_y(plan, ids, ws, e1, srcs)
        plans.append(plan)
        parts.extend([keep, lax.ppermute(send, "core", swap)])

    def blk(kind, d, rows, row, *src):
        return dict(kind=kind, d=d, rows=rows, row=row, src=src)

    call([blk("own", 0, 128, 0, 0)], [own0])
    call([blk("own", 128, 128, 0, 0), blk("a", 0, 3 * R, 0, 1), blk("b", 0, 3 * R, 0, 2)], [own1, a0, b0])
    call(
        [
            blk("a", 3, 3 * R, 0, 2),
            blk("a", 1, 3 * R, 0, 3),
            blk("b", 3, 3 * R, 0, 4),
            blk("b", 1, 3 * R, 0, 5),
            blk("c", 0, CR, 0, 0),
            blk("c", 1, CR, 0, 1),
        ],
        [cl, cr, al, ar, bl, br],
    )
    call([blk("a", 2, 3 * R, 0, 2), blk("b", 2, 3 * R, 0, 3), blk("c", 2, CR, 0, 0, 1)], [cf_lo, cf_hi, af, bf])

    k2 = jnp.broadcast_to(kernel.reshape(1, 128), (8, 128))
    out_a, out_b = along_x(plans, ids, tiles, e2, k2, asked, asked_b, parts)
    from_b = lax.ppermute(out_b, "core", swap)
    here = (((tiles_a - 1) >> 1) & 1) == core
    merged = jnp.where(here[:, None, None], out_a, from_b)
    answers = lax.all_to_all(merged.reshape(32, 32, 128), c_axes, split_axis=0, concat_axis=0, tiled=True)
    predicted = answers.reshape(128, 8, 128)[slot]
    return observed - predicted.reshape(16, 2, 512)


def solution(mesh):
    fine = Mesh(mesh.devices.reshape(2, 4, 4, 2, 4), ("zh", "x", "y", "core", "wa"))
    ba = ("zh", "x", "y", "core")
    rows = ba + ("wa",)
    return jax.shard_map(
        shards,
        mesh=fine,
        in_specs=(
            P(None, None, "wa"),
            P(ba),
            P(),
            P(rows),
            P(rows, None),
            P(rows, None, None),
            P(rows, None, None),
        ),
        out_specs=P(rows, None, None),
        check_vma=False,
    )
```

```python
import functools

import jax
import jax.numpy as jnp
from jax import lax
from jax.experimental import pallas as pl
from jax.experimental.pallas import tpu as pltpu
from jax.sharding import Mesh
from jax.sharding import PartitionSpec as P


N = 2048
SP = 0.7 / N
R = 16
CR = 128
SMEM = pl.BlockSpec(memory_space=pltpu.SMEM)
VMEM = pl.BlockSpec(memory_space=pltpu.VMEM)
HBM = pl.BlockSpec(memory_space=pltpu.HBM)
F32 = jnp.float32
BF16 = jnp.bfloat16

SIN_C = (3.14159264, -5.16771009, 2.55007766, -0.59829216, 0.07765941)
COS_C = (0.99999995, -4.93479286, 4.05841191, -1.33188016, 0.21969679)
G_C = (0.5, 0.12500105, 0.0624521, 0.03985648, 0.0215331, 0.03890036)
MAGIC = 12582912.0


def horner(z, coefs):
    acc = jnp.full_like(z, coefs[-1])
    for c in coefs[-2::-1]:
        acc = acc * z + c
    return acc


def cis_turns(t):
    r = t - ((t + MAGIC) - MAGIC)
    z = r * r
    s = r * horner(z, SIN_C)
    c = horner(z, COS_C)
    s2 = s + s
    return 1.0 - s2 * s, s2 * c


def split(x):
    hi = x.astype(BF16)
    return hi, (x - hi.astype(F32)).astype(BF16)


def bdot(a, b):
    return jnp.dot(a, b, preferred_element_type=F32)


def tables_kernel(ids, e1h, e1l, e2h, e2l, tw1, tw2):
    row = lax.broadcasted_iota(jnp.int32, (128, 128), 0)
    col = lax.broadcasted_iota(jnp.int32, (128, 128), 1)
    lane = lax.broadcasted_iota(jnp.int32, (8, 128), 1)

    def cs(k):
        return cis_turns((k & (N - 1)).astype(F32) * (1.0 / N))

    def put(h, l, i, r, c, v):
        a, b = v
        h[i, 128 * r : 128 * r + 128, 128 * c : 128 * c + 128] = a
        l[i, 128 * r : 128 * r + 128, 128 * c : 128 * c + 128] = b

    for p in range(4):
        y = 16 * (127 - row if p > 1 else row) + 4 * p
        c, s = cs(col * y)
        ch, sh = split(c), split(s)
        put(e1h, e1l, p, 0, 0, ch)
        put(e1h, e1l, p, 1, 1, ch)
        put(e1h, e1l, p, 0, 1, (-sh[0], -sh[1]))
        put(e1h, e1l, p, 1, 0, sh)
        c, s = cs(row * (16 * col + 4 * p))
        ch, sh = split(c * (1.0 / N)), split(s * (1.0 / N))
        put(e2h, e2l, p, 0, 0, ch)
        put(e2h, e2l, p, 1, 1, ch)
        put(e2h, e2l, p, 0, 1, sh)
        put(e2h, e2l, p, 1, 0, (-sh[0], -sh[1]))
    for q in range(1, 4):
        for j in range(4):
            k = 4 * (q - 1) + j
            c, s = cs((512 * ids[1] + 128 * j + lane) * q)
            tw1[2 * k] = c
            tw1[2 * k + 1] = -s
            c, s = cs((128 * j + row) * q)
            tw2[0, k] = c
            tw2[1, k] = -s


def tables(ids):
    sds = jax.ShapeDtypeStruct
    shapes = [sds((4, 256, 256), BF16)] * 4 + [sds((24, 8, 128), F32), sds((2, 12, 128, 128), F32)]
    return pl.pallas_call(
        tables_kernel,
        out_shape=shapes,
        in_specs=[SMEM],
        out_specs=[VMEM] * 6,
        cost_estimate=pl.CostEstimate(flops=60 * 16 * 2 * 16384, bytes_accessed=4 << 20, transcendentals=0),
        name="tables",
    )(ids)


def turn_kernel(b, ids, sky, own, *rest):
    outs, (xin, t, tmp, sem_in, sem_out) = rest[:-5], rest[-5:]
    core, xc, yc = ids[0], ids[2], ids[3]
    loads = []
    for c in range(2):
        col = pl.multiple_of(256 * core + 128 * b, 128)
        loads.append(pltpu.make_async_copy(sky.at[c, :, pl.ds(col, 128)], xin.at[c], sem_in.at[c]))
        loads[c].start()
    moves = []

    def move(src, dst):
        moves.append(pltpu.make_async_copy(src, dst, sem_out.at[len(moves)]))
        moves[-1].start()

    rev = 127 - lax.broadcasted_iota(jnp.int32, (128, 128), 1)
    for y0 in range(16):
        for c in range(2):
            if y0 == 0:
                loads[c].wait()
            v = xin[c, pl.ds(y0, 128, stride=16), :].T
            if y0 > 7:
                v = jnp.take_along_axis(v, rev, axis=1)
            z = 2 * (y0 % 2) + c
            tmp[z] = v
            for j0 in range(16):
                t[y0, 8 * j0 : 8 * j0 + 8, 128 * c : 128 * c + 128] = tmp[z, pl.ds(j0, 8, stride=16), :]
        if y0 % 4 == 3 and y0 < 15:
            move(t.at[pl.ds(y0 - 3, 4)], own.at[pl.ds(y0 - 3, 4)])
    if outs:
        a_src = t.at[pl.ds(4 * xc, 4), pl.ds(pl.multiple_of(R * yc, 8), R), :]
        b_src = t.at[pl.ds(4 * yc, 4), pl.ds(pl.multiple_of(4 * R + R * xc, 8), R), :]
        ab, pa, pb = outs
        move(a_src, ab.at[0])
        move(b_src, ab.at[1])
        move(a_src, pa)
        move(b_src, pb)
    move(t.at[pl.ds(12, 4)], own.at[pl.ds(12, 4)])
    for m in moves:
        m.wait()


def turn(b, ids, sky):
    sds = lambda *d: jax.ShapeDtypeStruct(d, F32)
    outs = [sds(16, 128, 256)] + [sds(2, 4, R, 256), sds(4, R, 256), sds(4, R, 256)] * (1 - b)
    return pl.pallas_call(
        functools.partial(turn_kernel, b),
        in_specs=[SMEM, HBM],
        out_specs=[HBM] * len(outs),
        out_shape=outs,
        scratch_shapes=[
            pltpu.VMEM((2, N, 128), F32),
            pltpu.VMEM((16, 128, 256), F32),
            pltpu.VMEM((4, 128, 128), F32),
            pltpu.SemaphoreType.DMA((2,)),
            pltpu.SemaphoreType.DMA((8,)),
        ],
        cost_estimate=pl.CostEstimate(flops=1 << 22, bytes_accessed=4 << 20, transcendentals=0),
    )(ids, sky)


def gather3_kernel(zl, zr, za, zb, oa, ob):
    for k, (o, far) in enumerate(((oa, za), (ob, zb))):
        o[:, 0:R, :] = zl[k]
        o[:, R : 2 * R, :] = zr[k]
        o[:, 2 * R : 3 * R, :] = far[...]


def gather3(*z):
    return pl.pallas_call(
        gather3_kernel,
        out_shape=[jax.ShapeDtypeStruct((4, 3 * R, 256), F32)] * 2,
        in_specs=[VMEM] * 4,
        out_specs=[VMEM] * 2,
        compiler_params=pltpu.CompilerParams(vmem_limit_bytes=8 << 20),
        cost_estimate=pl.CostEstimate(flops=1 << 20, bytes_accessed=1 << 20, transcendentals=0),
        name="gather3",
    )(*z)


def join_kernel(ids, *refs):
    for k in range(4):
        for base, ref, o in ((ids[2], refs[k], refs[8]), (ids[3], refs[4 + k], refs[9])):
            o[pl.ds(4 * ((base + k) & 3), 4)] = ref[...]


def join(ids, a, b):
    return pl.pallas_call(
        join_kernel,
        out_shape=[jax.ShapeDtypeStruct((16, 3 * R, 256), F32)] * 2,
        in_specs=[SMEM] + [VMEM] * 8,
        out_specs=[VMEM] * 2,
        compiler_params=pltpu.CompilerParams(vmem_limit_bytes=16 << 20),
        cost_estimate=pl.CostEstimate(flops=1 << 20, bytes_accessed=3 << 20, transcendentals=0),
        name="join",
    )(ids, *a, *b)


def slab_of(kind, k, ids):
    a = ids[1]
    return (a + (0 if kind == "own" else (3, 1, 2)[k])) & 3


def block_rows(blk, ids):
    kind, d, n = blk["kind"], blk["d"], blk["rows"]
    if kind == "own":
        return [(slab_of(kind, 0, ids), d, n // 8)]
    if kind == "c":
        return [(slab_of(kind, d, ids), 128, n // 8)]
    first = R * ((ids[3] + d) & 3) if kind == "a" else 4 * R + R * ((ids[2] + d) & 3)
    return [(slab_of(kind, k, ids), first, R // 8) for k in range(3)]


def along_y_kernel(plan, n_src, ids, ws, e1h, e1l, tw1, *rest):
    srcs = rest[:n_src]
    keep, send = rest[n_src : n_src + 2]
    eh, el, tw, xin, xh0, xl0, yb0, xh1, xl1, yb1, gb, cs, tab, where, sem_e, sem_in, sem_out = rest[n_src + 2 :]
    core = ids[0]
    lane = lax.broadcasted_iota(jnp.int32, (8, 128), 1)
    sub = lax.broadcasted_iota(jnp.int32, (8, 128), 0)
    w = [ws[core], ws[1 - core]]
    n_pairs = sum(blk["rows"] for blk in plan) // 16
    steps = n_pairs // 2

    e_copies = [
        pltpu.make_async_copy(src, dst, sem_e.at[i]) for i, (src, dst) in enumerate(((e1h, eh), (e1l, el), (tw1, tw)))
    ]
    for c in e_copies:
        c.start()
    kinds, k = [], 0
    for blk in plan:
        if blk["src"] not in kinds:
            kinds.append(blk["src"])
        for i in range(blk["rows"] // 16):
            where[2 * k] = kinds.index(blk["src"])
            where[2 * k + 1] = blk["row"] + 16 * i
            k += 1
    k = 0
    for blk in plan:
        for slab, first, n in block_rows(blk, ids):
            for i in range(n):
                row = first + 8 * i
                tab[k] = 512 * slab + 256 * core + 128 * (row >> 7) + ((row >> 3) & 15)
                k += 1

    def load(pair, slot, a):
        kind, row = where[2 * pair], pl.ds(pl.multiple_of(where[2 * pair + 1], 16), 16)
        for i, src in enumerate(kinds):
            @pl.when(kind == i)
            def _(src=src):
                h = 16 // len(src)
                for j, s in enumerate(src):
                    pltpu.make_async_copy(
                        srcs[s].at[:, row, :], xin.at[slot, a, pl.ds(h * j, h)], sem_in.at[slot, a]
                    ).start()

    def stores(k, slot):
        out = []
        for a in range(2):
            dst = pl.ds(4 * k + 2 * a, 2)
            out.append(pltpu.make_async_copy(gb.at[slot, a, core], keep.at[:, :, dst], sem_out.at[slot, a, 0]))
            out.append(pltpu.make_async_copy(gb.at[slot, a, 1 - core], send.at[:, :, dst], sem_out.at[slot, a, 1]))
        return out

    for k in range(min(2, steps)):
        for a in range(2):
            load(2 * k + a, k, a)
    for c in e_copies:
        c.wait()

    def image(pair, slot, s, xh, xl):
        for a in range(2):
            cx = ((tab[2 * pair + a] + 16 * sub).astype(F32) - N / 2) * SP
            cx2 = cx * cx
            for y0 in range(16):
                p, q = y0 // 4, y0 % 4
                kap = min(y0, 16 - y0)
                if y0 <= 8:
                    cy = ((16 * lane + kap).astype(F32) - N / 2) * SP
                    r2 = cx2 + cy * cy
                    t = r2 * horner(r2, G_C)
                    pairs = [cis_turns(t * w[pi]) for pi in range(2)]
                    if 0 < y0 < 8:
                        for pi in range(2):
                            cs[s, a, kap, pi, 0] = pairs[pi][0]
                            cs[s, a, kap, pi, 1] = pairs[pi][1]
                else:
                    pairs = [(cs[s, a, kap, pi, 0], cs[s, a, kap, pi, 1]) for pi in range(2)]
                sr = xin[slot, s, y0, 8 * a : 8 * a + 8, 0:128]
                si = xin[slot, s, y0, 8 * a : 8 * a + 8, 128:256]
                for pi, (c, n) in enumerate(pairs):
                    r0 = 64 * a + 16 * q + 8 * pi
                    h, l = split(jnp.concatenate([sr * c - si * n, sr * n + si * c], axis=1))
                    xh[p, r0 : r0 + 8, :] = h
                    xl[p, r0 : r0 + 8, :] = l

    def long_part(xh, xl, yb):
        for p in range(4):
            x = xh[p]
            yb[p] = bdot(x, eh[p]) + bdot(xl[p], eh[p]) + bdot(x, el[p])

    def short_part(slot, s, yb):
        for a in range(2):
            for pi in range(2):
                sums = None
                for q in range(4):
                    r0 = 64 * a + 16 * q + 8 * pi
                    v = butterfly4([(yb[p, r0 : r0 + 8, 0:128], yb[p, r0 : r0 + 8, 128:256]) for p in range(4)])
                    if q:
                        out = []
                        for j, (r, i) in enumerate(v):
                            k = 8 * (q - 1) + 2 * j
                            out.append((r * tw[k] - i * tw[k + 1], r * tw[k + 1] + i * tw[k]))
                        v = out
                    sums = v if sums is None else [(x + u, y + z) for (x, y), (u, z) in zip(sums, v)]
                for j, (vr, vi) in enumerate(sums):
                    cc = slice(128 * (j % 2), 128 * (j % 2) + 128)
                    gb[slot, s, j // 2, pi, 0, a, :, cc] = vr
                    gb[slot, s, j // 2, pi, 1, a, :, cc] = vi

    def step(k, slot3):
        @pl.when(k >= 2)
        def _():
            for c in stores(k - 2, k & 1):
                c.start()

        @pl.when(k >= 3)
        def _():
            for c in stores(k - 3, 1 - (k & 1)):
                c.wait()

        ahead = jnp.where(slot3 == 0, 2, slot3 - 1)

        @pl.when(k + 2 < steps)
        def _():
            for a in range(2):
                load(2 * k + 4 + a, ahead, a)

        for a in range(2):
            pltpu.make_async_copy(xin.at[slot3, a], xin.at[slot3, a], sem_in.at[slot3, a]).wait()
        done = 1 - (k & 1)
        long_part(xh1, xl1, yb1)
        short_part(done, 0, yb0)
        image(2 * k, slot3, 0, xh0, xl0)
        long_part(xh0, xl0, yb0)
        short_part(done, 1, yb1)
        image(2 * k + 1, slot3, 1, xh1, xl1)
        return jnp.where(slot3 == 2, 0, slot3 + 1)

    lax.fori_loop(0, steps, step, jnp.int32(0))
    last = (steps - 1) % 2
    if steps >= 2:
        for c in stores(steps - 2, steps % 2):
            c.start()
    if steps >= 3:
        for c in stores(steps - 3, last):
            c.wait()
    long_part(xh1, xl1, yb1)
    short_part(last, 0, yb0)
    short_part(last, 1, yb1)
    for c in stores(steps - 1, last):
        c.start()
    if steps >= 2:
        for c in stores(steps - 2, steps % 2):
            c.wait()
    for c in stores(steps - 1, last):
        c.wait()


def along_y(plan, ids, ws, e1, srcs):
    total = sum(blk["rows"] for blk in plan)
    out = jax.ShapeDtypeStruct((2, 2, total // 8, 8, 256), F32)
    stage = [pltpu.VMEM((4, 128, 256), BF16), pltpu.VMEM((4, 128, 256), BF16), pltpu.VMEM((4, 128, 256), F32)]
    return pl.pallas_call(
        functools.partial(along_y_kernel, plan, len(srcs)),
        out_shape=[out, out],
        in_specs=[SMEM] * 2 + [HBM] * (3 + len(srcs)),
        out_specs=[HBM, HBM],
        scratch_shapes=[
            pltpu.VMEM((4, 256, 256), BF16),
            pltpu.VMEM((4, 256, 256), BF16),
            pltpu.VMEM((24, 8, 128), F32),
            pltpu.VMEM((3, 2, 16, 16, 256), F32),
            *stage,
            *stage,
            pltpu.VMEM((2, 2, 2, 2, 2, 2, 8, 256), F32),
            pltpu.VMEM((2, 2, 8, 2, 2, 8, 128), F32),
            pltpu.SMEM((total // 8,), jnp.int32),
            pltpu.SMEM((total // 8,), jnp.int32),
            pltpu.SemaphoreType.DMA((3,)),
            pltpu.SemaphoreType.DMA((3, 2)),
            pltpu.SemaphoreType.DMA((2, 2, 2)),
        ],
        cost_estimate=pl.CostEstimate(
            flops=total * 2 * 16 * 3 * 256 * 256 * 2, bytes_accessed=total * 24 * 1024, transcendentals=0
        ),
    )(ids, ws, *e1, *srcs)


def butterfly4(v):
    (r0, i0), (r1, i1), (r2, i2), (r3, i3) = v
    ar, ai, br, bi = r0 + r2, i0 + i2, r0 - r2, i0 - i2
    cr, ci, dr, di = r1 + r3, i1 + i3, r1 - r3, i1 - i3
    return [(ar + cr, ai + ci), (br + di, bi - dr), (ar - cr, ai - ci), (br - di, bi + dr)]


def dft16(v, tw):
    out = [None] * 16
    inner = [butterfly4([v[4 * p + q] for p in range(4)]) for q in range(4)]
    for t0 in range(4):
        cols = [inner[0][t0]]
        for q in range(1, 4):
            (r, i), (c, s) = inner[q][t0], tw(4 * (q - 1) + t0)
            cols.append((r * c - i * s, r * s + i * c))
        for t1, val in enumerate(butterfly4(cols)):
            out[t0 + 4 * t1] = val
    return out


def along_x_kernel(plans, ids, k1, e2h, e2l, tw2, pos_a, pos_b, *rest):
    n = len(plans)
    parts = rest[: 2 * n]
    out_a, out_b = rest[2 * n : 2 * n + 2]
    eh, el, tw, pv, d, f0, f1, grid = rest[2 * n + 2 : 2 * n + 10]
    bufs = [rest[2 * n + 10 + 4 * k : 2 * n + 14 + 4 * k] for k in range(4)]
    res, lst, notes, sem, sem_e, sem_o = rest[2 * n + 26 :]
    f = (f0, f1)
    core = ids[0]
    for i, plan in enumerate(plans):
        off = 0
        for blk in plan:
            for slab, first, cnt in block_rows(blk, ids):
                base = 32 * slab + 8 * (first >> 7)
                for ref, side in ((parts[2 * i], core), (parts[2 * i + 1], 1 - core)):
                    at = pl.ds(pl.multiple_of(base + 16 * side, 8), 8)
                    dst = d.at[:, :, pl.ds((first >> 3) & 15, cnt), at, :]
                    pltpu.make_async_copy(ref.at[:, :, pl.ds(off, cnt)], dst, sem).start()
                off += cnt
    last8 = pl.ds(64, 8)
    notice = [
        pltpu.make_async_copy(src.at[:, last8, :], notes.at[i], sem_o.at[i]) for i, src in enumerate((pos_a, pos_b))
    ]
    for c in notice:
        c.start()
    small = [(e2h, eh), (e2l, el), (tw2, tw), (pos_a, pv.at[0]), (pos_b, pv.at[1])]
    small = [pltpu.make_async_copy(s, t, sem_e.at[i]) for i, (s, t) in enumerate(small)]
    for c in small:
        c.start()
    res[...] = jnp.zeros_like(res)
    for c in notice:
        c.wait()

    def tile_of(sid):
        return notes[sid >> 7, (sid & 127) >> 3, 0, sid & 7]

    def scan(s, cnt):
        for k in range(8):
            t = notes[s >> 4, s & 15, 0, k]
            lst[cnt] = 8 * s + k
            mine = jnp.logical_and(t > 0, (((t - 1) >> 1) & 1) == core)
            cnt = cnt + mine.astype(jnp.int32)
        return cnt

    lst[0] = 0
    count = lax.fori_loop(0, 32, scan, jnp.int32(0))
    last = jnp.where(count > 0, lst[jnp.maximum(count - 1, 0)], 0)
    for k in range(8):
        lst[count + k] = last
    for c in small:
        c.wait()
    pltpu.make_async_copy(d, d, sem).wait()

    def first(pi, k, qs=range(4)):
        for q in qs:
            x0 = 4 * k + q
            h, l = split(jnp.concatenate([d[pi, 0, x0], d[pi, 1, x0]], axis=0))
            f[pi][x0] = bdot(eh[k], h) + bdot(el[k], h) + bdot(eh[k], l)

    def second(pi, m):
        rr = pl.ds(pl.multiple_of(8 * m, 8), 8)
        ri = pl.ds(pl.multiple_of(128 + 8 * m, 8), 8)
        for jj in range(2):
            cc = slice(128 * jj, 128 * jj + 128)
            v = [(f[pi][x0, rr, cc], f[pi][x0, ri, cc]) for x0 in range(16)]
            v = dft16(v, lambda k: (tw[0, k, rr, :], tw[1, k, rr, :]))
            for t in range(16):
                grid[(pi * 2 + jj) * 16 + t, rr, :] = v[t][0]
                grid[(pi * 2 + jj) * 16 + t, ri, :] = v[t][1]

    def stage0(k, carry):
        first(0, k)
        return carry

    def stage1(k, carry):
        for m in range(4):
            first(1, k, (m,))
            second(0, 4 * k + m)
        return carry

    def stage2(k, carry):
        second(1, 2 * k)
        second(1, 2 * k + 1)
        return carry

    lax.fori_loop(0, 4, stage0, 0)
    lax.fori_loop(0, 4, stage1, 0)
    lax.fori_loop(0, 8, stage2, 0)

    sub = lax.broadcasted_iota(jnp.int32, (8, 128), 0)
    table = jnp.broadcast_to(k1[...], (8, 128))

    def taps(row):
        row = jnp.broadcast_to(row, (8, 128))
        off = row & 15
        cell = row >> 4
        cl = cell & 7
        idx = off * 8 + ((sub - cl) & 7)
        return jnp.take_along_axis(table, idx, axis=1), (cell >> 3) + (sub < cl).astype(jnp.int32)

    def build(sid, buf):
        ww, wl, ru, hu = buf
        pos = pv[sid >> 7, (sid & 127) >> 3, pl.ds(pl.multiple_of(8 * (sid & 7), 8), 8), :]
        for jp in range(2):
            th = []
            for j in (2 * jp, 2 * jp + 1):
                r, h = taps(pos[4 + j : 5 + j, :])
                rh = r.astype(BF16).astype(F32)
                th.append((rh, r - rh, h))
                ru[j], hu[j] = taps(pos[j : j + 1, :])
            cc = slice(256 * jp, 256 * jp + 256)
            for i in range(16):
                masks = [h == i for _, _, h in th]
                wh = jnp.concatenate([jnp.where(m, v[0], 0.0) for m, v in zip(masks, th)], axis=1).astype(BF16)
                ww[8 * i : 8 * i + 8, cc] = wh
                ww[128 + 8 * i : 136 + 8 * i, cc] = wh
                wl[8 * i : 8 * i + 8, cc] = jnp.concatenate(
                    [jnp.where(m, v[1], 0.0) for m, v in zip(masks, th)], axis=1
                ).astype(BF16)

    def finish(sid, buf):
        ww, wl, ru, hu = buf
        t = jnp.maximum(tile_of(sid) - 1, 0)
        x = grid[(((sid >> 1) & 1) * 2 + (t & 1)) * 16 + (t >> 4)]
        h = x.astype(BF16)
        hf = h.astype(F32)
        part = bdot(jnp.concatenate([hf, x - hf], axis=1).astype(BF16), ww[...]) + bdot(h, wl[...])
        rows = []
        for j in range(4):
            r, h = ru[j], hu[j]
            for c in range(2):
                acc = jnp.zeros((8, 128), F32)
                for i in range(16):
                    acc = jnp.where(h == i, part[128 * c + 8 * i : 128 * c + 8 * i + 8, 128 * j : 128 * j + 128], acc)
                rows.append(jnp.sum(r * acc, axis=0, keepdims=True))
        res[sid] = jnp.concatenate(rows[0::2] + rows[1::2], axis=0)

    build(lst[0], bufs[0])
    build(lst[1], bufs[1])

    def four(i, carry):
        for k in range(4):
            finish(lst[4 * i + k], bufs[k])
            build(lst[4 * i + 2 + k], bufs[(k + 2) % 4])
        return carry

    lax.fori_loop(0, (count + 3) >> 2, four, 0)
    moves = [
        pltpu.make_async_copy(res.at[pl.ds(0, 128)], out_a, sem_o.at[0]),
        pltpu.make_async_copy(res.at[pl.ds(128, 128)], out_b, sem_o.at[1]),
    ]
    for m in moves:
        m.start()
    for m in moves:
        m.wait()


def along_x(plans, ids, k1, e2, pos_a, pos_b, parts):
    buf = [
        pltpu.VMEM((256, 512), BF16),
        pltpu.VMEM((128, 512), BF16),
        pltpu.VMEM((4, 8, 128), F32),
        pltpu.VMEM((4, 8, 128), jnp.int32),
    ]
    return pl.pallas_call(
        functools.partial(along_x_kernel, plans),
        out_shape=[jax.ShapeDtypeStruct((128, 8, 128), F32)] * 2,
        in_specs=[SMEM, VMEM] + [HBM] * (5 + len(parts)),
        out_specs=[HBM, HBM],
        scratch_shapes=[
            pltpu.VMEM((4, 256, 256), BF16),
            pltpu.VMEM((4, 256, 256), BF16),
            pltpu.VMEM((2, 12, 128, 128), F32),
            pltpu.VMEM((2, 16, 72, 128), jnp.int32),
            pltpu.VMEM((2, 2, 16, 128, 256), F32),
            pltpu.VMEM((16, 256, 256), F32),
            pltpu.VMEM((16, 256, 256), F32),
            pltpu.VMEM((64, 256, 128), F32),
            *buf,
            *buf,
            *buf,
            *buf,
            pltpu.VMEM((256, 8, 128), F32),
            pltpu.SMEM((272,), jnp.int32),
            pltpu.SMEM((2, 16, 8, 128), jnp.int32),
            pltpu.SemaphoreType.DMA,
            pltpu.SemaphoreType.DMA((5,)),
            pltpu.SemaphoreType.DMA((2,)),
        ],
        cost_estimate=pl.CostEstimate(flops=60_000_000_000, bytes_accessed=16 << 20, transcendentals=0),
        name="along_x",
    )(ids, k1, *e2, pos_a, pos_b, *parts)


def pick_kernel(here, there, answers, observed, rest, other):
    for b in range(16):
        i, j = here[b], there[b]
        v = answers[jnp.maximum(i, 0)]
        rest[b] = observed[b] - jnp.where(i >= 0, v, 0.0)
        v = answers[jnp.maximum(j, 0)]
        other[b] = jnp.where(j >= 0, v, 0.0)


def pick(here, there, answers, observed):
    return pl.pallas_call(
        pick_kernel,
        out_shape=[jax.ShapeDtypeStruct((16, 8, 128), F32)] * 2,
        in_specs=[SMEM, SMEM, VMEM, VMEM],
        out_specs=[VMEM, VMEM],
        compiler_params=pltpu.CompilerParams(vmem_limit_bytes=8 << 20),
        name="pick",
    )(here, there, answers, observed)


def shift(x, axes, size, by):
    return lax.ppermute(x, axes, [(i, (i + by) % size) for i in range(size)])


def shards(sky, plane_w, kernel, tile_ids, plane_ids, positions, observed):
    i32 = jnp.int32
    core = lax.axis_index("core")
    ids = jnp.stack([core, lax.axis_index("wa"), lax.axis_index("x"), lax.axis_index("y")]).astype(i32)
    z_axes = ("zh", "wa")
    swap = [(0, 1), (1, 0)]
    zh = lax.axis_index("zh")

    target = plane_ids[:, 0]
    same = (target[:, None] == target[None, :]).astype(i32)
    slot = target * 2 + jnp.sum(jnp.tril(same, -1), axis=1)
    notes = jnp.pad(jnp.stack([slot, tile_ids + 1]), ((0, 6), (0, 112)))
    mine0 = jnp.concatenate([positions.reshape(16, 8, 128), notes[None]], axis=0)
    got0 = lax.ppermute(mine0, "zh", swap)

    own0, ab, pa, pb = turn(0, ids, sky)
    zl = shift(ab, z_axes, 8, 1)
    zr = shift(ab, z_axes, 8, -1)
    za = shift(pa, z_axes, 8, 2)
    zb = shift(pb, z_axes, 8, -2)
    (own1,) = turn(1, ids, sky)
    cl = shift(own1, z_axes, 8, 1)
    cr = shift(own1, z_axes, 8, -1)
    cf_lo = shift(cl[:8], z_axes, 8, 1)
    cf_hi = shift(cr[8:], z_axes, 8, -1)

    mine_a, mine_b = gather3(zl, zr, za, zb)

    def three(x, axis):
        l = shift(x, axis, 4, 1)
        r = shift(x, axis, 4, -1)
        return r, shift(x, axis, 4, 2), l

    ax, bx = three(mine_a, "x"), three(mine_b, "y")
    a0, b0 = join(ids, (mine_a,) + ax, (mine_b,) + bx)
    ar, af, al = three(a0, "y")
    br, bf, bl = three(b0, "x")

    def place(sl, home):
        return jnp.where((sl >> 6) == zh, (((sl >> 2) & 15) * 2 + home) * 4 + (sl & 3), -1)

    here, there = place(slot, zh), place(got0[16, 0, :16], 1 - zh)
    dst = jnp.concatenate([here, there])
    dst = jnp.where(dst < 0, 128 + jnp.arange(32, dtype=i32), dst)
    pos = jnp.concatenate([mine0[:16], got0[:16]])
    tile = jnp.concatenate([tile_ids + 1, got0[16, 1, :16]])
    slot_pos = jnp.zeros((128, 8, 128), i32).at[dst].set(pos, unique_indices=True, mode="drop")
    slot_tile = jnp.zeros((128,), i32).at[dst].set(tile, unique_indices=True, mode="drop")
    tile_row = jnp.pad(slot_tile.reshape(16, 1, 8), ((0, 0), (0, 7), (0, 120)))
    payload = jnp.concatenate([slot_pos.reshape(16, 64, 128), tile_row], axis=1)
    asked = lax.all_to_all(payload, ("x", "y"), split_axis=0, concat_axis=0, tiled=True)
    asked_b = lax.ppermute(asked, "core", swap)
    other_w = lax.ppermute(plane_w, "core", swap)
    ws = jnp.concatenate([plane_w, other_w])
    *e1, tw1, tw2 = tables(ids)
    e1, e2 = e1[:2] + [tw1], e1[2:] + [tw2]
    plans, parts = [], []

    def call(plan, srcs):
        keep, send = along_y(plan, ids, ws, e1, srcs)
        plans.append(plan)
        parts.extend([keep, lax.ppermute(send, "core", swap)])

    def blk(kind, d, rows, row, *src):
        return dict(kind=kind, d=d, rows=rows, row=row, src=src)

    call([blk("own", 0, 128, 0, 0)], [own0])
    call([blk("own", 128, 128, 0, 0), blk("a", 0, 3 * R, 0, 1), blk("b", 0, 3 * R, 0, 2)], [own1, a0, b0])
    call(
        [
            blk("a", 3, 3 * R, 0, 2),
            blk("a", 1, 3 * R, 0, 3),
            blk("b", 3, 3 * R, 0, 4),
            blk("b", 1, 3 * R, 0, 5),
            blk("c", 0, CR, 0, 0),
            blk("c", 1, CR, 0, 1),
        ],
        [cl, cr, al, ar, bl, br],
    )
    call([blk("a", 2, 3 * R, 0, 2), blk("b", 2, 3 * R, 0, 3), blk("c", 2, CR, 0, 0, 1)], [cf_lo, cf_hi, af, bf])

    k1 = kernel.reshape(1, 128)
    out_a, out_b = along_x(plans, ids, k1, e2, asked, asked_b, parts)
    from_b = lax.ppermute(out_b, "core", swap)
    merged = out_a + from_b
    answers = lax.all_to_all(merged.reshape(16, 64, 128), ("x", "y"), split_axis=0, concat_axis=0, tiled=True)
    rest, other = pick(here, there, answers.reshape(128, 8, 128), observed.reshape(16, 8, 128))
    got = lax.ppermute(other, "zh", swap)
    return (rest - got).reshape(16, 2, 512)


def solution(mesh):
    fine = Mesh(mesh.devices.reshape(2, 4, 4, 2, 4), ("zh", "x", "y", "core", "wa"))
    ba = ("zh", "x", "y", "core")
    rows = ba + ("wa",)
    return jax.shard_map(
        shards,
        mesh=fine,
        in_specs=(
            P(None, None, "wa"),
            P(ba),
            P(),
            P(rows),
            P(rows, None),
            P(rows, None, None),
            P(rows, None, None),
        ),
        out_specs=P(rows, None, None),
        check_vma=False,
    )
```

```python
import functools

import jax
import jax.numpy as jnp
from jax import lax
from jax.experimental import pallas as pl
from jax.experimental.pallas import tpu as pltpu
from jax.sharding import Mesh
from jax.sharding import PartitionSpec as P


N = 2048
SP = 0.7 / N
R = 16
CR = 128
SMEM = pl.BlockSpec(memory_space=pltpu.SMEM)
VMEM = pl.BlockSpec(memory_space=pltpu.VMEM)
HBM = pl.BlockSpec(memory_space=pltpu.HBM)
F32 = jnp.float32
BF16 = jnp.bfloat16

SIN_C = (3.14159264, -5.16771009, 2.55007766, -0.59829216, 0.07765941)
COS_C = (0.99999995, -4.93479286, 4.05841191, -1.33188016, 0.21969679)
G_C = (0.5, 0.12500105, 0.0624521, 0.03985648, 0.0215331, 0.03890036)
MAGIC = 12582912.0


def place_ids():
    return tuple(lax.axis_index(n) for n in ("core", "wa", "x", "y"))


def horner(z, coefs):
    acc = jnp.full_like(z, coefs[-1])
    for c in coefs[-2::-1]:
        acc = acc * z + c
    return acc


def cis_turns(t):
    r = t - ((t + MAGIC) - MAGIC)
    z = r * r
    s = r * horner(z, SIN_C)
    c = horner(z, COS_C)
    s2 = s + s
    return 1.0 - s2 * s, s2 * c


def split(x):
    hi = x.astype(BF16)
    return hi, (x - hi.astype(F32)).astype(BF16)


def bdot(a, b):
    return jnp.dot(a, b, preferred_element_type=F32)


def tables_kernel(e1h, e1l, e2h, e2l, tw1, tw2):
    row = lax.broadcasted_iota(jnp.int32, (128, 128), 0)
    col = lax.broadcasted_iota(jnp.int32, (128, 128), 1)
    lane = lax.broadcasted_iota(jnp.int32, (8, 128), 1)

    ids = place_ids()

    def cs(k):
        return cis_turns((k & (N - 1)).astype(F32) * (1.0 / N))

    def put(h, l, i, r, c, v):
        a, b = v
        h[i, 128 * r : 128 * r + 128, 128 * c : 128 * c + 128] = a
        l[i, 128 * r : 128 * r + 128, 128 * c : 128 * c + 128] = b

    def matrices(p, carry):
        y = 16 * jnp.where(p > 1, 127 - row, row) + 4 * p
        c, s = cs(col * y)
        ch, sh = split(c), split(s)
        put(e1h, e1l, p, 0, 0, ch)
        put(e1h, e1l, p, 1, 1, ch)
        put(e1h, e1l, p, 0, 1, (-sh[0], -sh[1]))
        put(e1h, e1l, p, 1, 0, sh)
        c, s = cs(row * (16 * col + 4 * p))
        ch, sh = split(c * (1.0 / N)), split(s * (1.0 / N))
        put(e2h, e2l, p, 0, 0, ch)
        put(e2h, e2l, p, 1, 1, ch)
        put(e2h, e2l, p, 0, 1, sh)
        put(e2h, e2l, p, 1, 0, (-sh[0], -sh[1]))
        return carry

    def factors(k, carry):
        q, j = 1 + (k >> 2), k & 3
        c, s = cs((512 * ids[1] + 128 * j + lane) * q)
        tw1[2 * k] = c
        tw1[2 * k + 1] = -s
        c, s = cs((128 * j + row) * q)
        tw2[0, k] = c
        tw2[1, k] = -s
        return carry

    lax.fori_loop(0, 4, matrices, 0)
    lax.fori_loop(0, 12, factors, 0)


def tables():
    sds = jax.ShapeDtypeStruct
    shapes = [sds((4, 256, 256), BF16)] * 4 + [sds((24, 8, 128), F32), sds((2, 12, 128, 128), F32)]
    return pl.pallas_call(
        tables_kernel,
        out_shape=shapes,
        out_specs=[VMEM] * 6,
        cost_estimate=pl.CostEstimate(flops=60 * 16 * 2 * 16384, bytes_accessed=4 << 20, transcendentals=0),
        name="tables",
    )()


def turn_kernel(b, sky, own, *rest):
    core, _, xc, yc = place_ids()
    outs, (xin, t, tmp, sem_in, sem_out) = rest[:-5], rest[-5:]
    own, outs = ((own,), outs) if b == 0 else ((own, outs[0]), ())
    loads = []
    for c in range(2):
        col = pl.multiple_of(256 * core + 128 * b, 128)
        loads.append(pltpu.make_async_copy(sky.at[c, :, pl.ds(col, 128)], xin.at[c], sem_in.at[c]))
        loads[c].start()
    moves = []

    def move(src, dst):
        moves.append(pltpu.make_async_copy(src, dst, sem_out.at[len(moves)]))
        moves[-1].start()

    def part(y4):
        return own[0].at[pl.ds(4 * y4, 4)] if b == 0 else own[y4 // 2].at[pl.ds(4 * (y4 % 2), 4)]

    rev = 127 - lax.broadcasted_iota(jnp.int32, (128, 128), 1)
    for c in range(2):
        loads[c].wait()
    for y4 in range(4):
        def group(i, carry, y4=y4):
            for e in range(2):
                y0 = 4 * y4 + 2 * i + e
                for c in range(2):
                    v = xin[c, pl.ds(y0, 128, stride=16), :].T
                    if y4 > 1:
                        v = jnp.take_along_axis(v, rev, axis=1)
                    z = 2 * e + c
                    tmp[z] = v
                    for j0 in range(16):
                        t[y0, 8 * j0 : 8 * j0 + 8, 128 * c : 128 * c + 128] = tmp[z, pl.ds(j0, 8, stride=16), :]
            return carry

        lax.fori_loop(0, 2, group, 0)
        if y4 < 3:
            move(t.at[pl.ds(4 * y4, 4)], part(y4))
    if outs:
        a_src = t.at[pl.ds(4 * xc, 4), pl.ds(pl.multiple_of(R * yc, 8), R), :]
        b_src = t.at[pl.ds(4 * yc, 4), pl.ds(pl.multiple_of(4 * R + R * xc, 8), R), :]
        ab, pa, pb = outs
        move(a_src, ab.at[0])
        move(b_src, ab.at[1])
        move(a_src, pa)
        move(b_src, pb)
    move(t.at[pl.ds(12, 4)], part(3))
    for m in moves:
        m.wait()


def turn(b, sky):
    sds = lambda *d: jax.ShapeDtypeStruct(d, F32)
    outs = [sds(8, 128, 256)] * 2 if b else [sds(16, 128, 256), sds(2, 4, R, 256), sds(4, R, 256), sds(4, R, 256)]
    return pl.pallas_call(
        functools.partial(turn_kernel, b),
        in_specs=[HBM],
        out_specs=[HBM] * len(outs),
        out_shape=outs,
        scratch_shapes=[
            pltpu.VMEM((2, N, 128), F32),
            pltpu.VMEM((16, 128, 256), F32),
            pltpu.VMEM((4, 128, 128), F32),
            pltpu.SemaphoreType.DMA((2,)),
            pltpu.SemaphoreType.DMA((8,)),
        ],
        cost_estimate=pl.CostEstimate(flops=1 << 22, bytes_accessed=4 << 20, transcendentals=0),
    )(sky)


def gather3_kernel(zl, zr, za, zb, oa, ob):
    for k, (o, far) in enumerate(((oa, za), (ob, zb))):
        o[:, 0:R, :] = zl[k]
        o[:, R : 2 * R, :] = zr[k]
        o[:, 2 * R : 3 * R, :] = far[...]


def gather3(*z):
    return pl.pallas_call(
        gather3_kernel,
        out_shape=[jax.ShapeDtypeStruct((4, 3 * R, 256), F32)] * 2,
        in_specs=[VMEM] * 4,
        out_specs=[VMEM] * 2,
        compiler_params=pltpu.CompilerParams(vmem_limit_bytes=8 << 20),
        cost_estimate=pl.CostEstimate(flops=1 << 20, bytes_accessed=1 << 20, transcendentals=0),
        name="gather3",
    )(*z)


def join_kernel(*refs):
    ids = place_ids()
    for k in range(4):
        for base, ref, o in ((ids[2], refs[k], refs[8]), (ids[3], refs[4 + k], refs[9])):
            o[pl.ds(4 * ((base + k) & 3), 4)] = ref[...]


def join(a, b):
    return pl.pallas_call(
        join_kernel,
        out_shape=[jax.ShapeDtypeStruct((16, 3 * R, 256), F32)] * 2,
        in_specs=[VMEM] * 8,
        out_specs=[VMEM] * 2,
        compiler_params=pltpu.CompilerParams(vmem_limit_bytes=16 << 20),
        cost_estimate=pl.CostEstimate(flops=1 << 20, bytes_accessed=3 << 20, transcendentals=0),
        name="join",
    )(*a, *b)


def slab_of(kind, k, ids):
    a = ids[1]
    return (a + (0 if kind == "own" else (3, 1, 2)[k])) & 3


def block_rows(blk, ids):
    kind, d, n = blk["kind"], blk["d"], blk["rows"]
    if kind == "own":
        return [(slab_of(kind, 0, ids), d, n // 8)]
    if kind == "c":
        return [(slab_of(kind, d, ids), 128, n // 8)]
    first = R * ((ids[3] + d) & 3) if kind == "a" else 4 * R + R * ((ids[2] + d) & 3)
    return [(slab_of(kind, k, ids), first, R // 8) for k in range(3)]


def along_y_kernel(plan, n_src, w_own, w_other, e1h, e1l, tw1, *rest):
    ids = place_ids()
    srcs = rest[:n_src]
    keep, send = rest[n_src : n_src + 2]
    eh, el, tw, xin, xh0, xl0, yb0, xh1, xl1, yb1, gb, cs, tab, where, sem_e, sem_in, sem_out = rest[n_src + 2 :]
    core = ids[0]
    lane = lax.broadcasted_iota(jnp.int32, (8, 128), 1)
    sub = lax.broadcasted_iota(jnp.int32, (8, 128), 0)
    w = [jnp.where(core == pi, w_own[0], w_other[0]) for pi in range(2)]
    n_pairs = sum(blk["rows"] for blk in plan) // 16
    steps = n_pairs // 2

    kinds, k = [], 0
    for blk in plan:
        if blk["src"] not in kinds:
            kinds.append(blk["src"])
        for i in range(blk["rows"] // 16):
            where[2 * k] = kinds.index(blk["src"])
            where[2 * k + 1] = blk["row"] + 16 * i
            k += 1
    k = 0
    for blk in plan:
        for slab, first, n in block_rows(blk, ids):
            for i in range(n):
                row = first + 8 * i
                tab[k] = 512 * slab + 256 * core + 128 * (row >> 7) + ((row >> 3) & 15)
                k += 1

    def load(pair, slot, a):
        kind, row = where[2 * pair], pl.ds(pl.multiple_of(where[2 * pair + 1], 16), 16)
        for i, src in enumerate(kinds):
            @pl.when(kind == i)
            def _(src=src):
                h = 16 // len(src)
                for j, s in enumerate(src):
                    pltpu.make_async_copy(
                        srcs[s].at[:, row, :], xin.at[slot, a, pl.ds(h * j, h)], sem_in.at[slot, a]
                    ).start()

    def stores(k, slot):
        out = []
        for a in range(2):
            dst = pl.ds(4 * k + 2 * a, 2)
            out.append(pltpu.make_async_copy(gb.at[slot, a, core], keep.at[:, :, dst], sem_out.at[slot, a, 0]))
            out.append(pltpu.make_async_copy(gb.at[slot, a, 1 - core], send.at[:, :, dst], sem_out.at[slot, a, 1]))
        return out

    for k in range(min(2, steps)):
        for a in range(2):
            load(2 * k + a, k, a)

    e_copies = [
        pltpu.make_async_copy(src, dst, sem_e.at[i]) for i, (src, dst) in enumerate(((e1h, eh), (e1l, el), (tw1, tw)))
    ]
    for c in e_copies:
        c.start()

    def image(pair, slot, s, xh, xl):
        for a in range(2):
            cx = ((tab[2 * pair + a] + 16 * sub).astype(F32) - N / 2) * SP
            cx2 = cx * cx
            for y0 in range(16):
                p, q = y0 // 4, y0 % 4
                kap = min(y0, 16 - y0)
                if y0 <= 8:
                    cy = ((16 * lane + kap).astype(F32) - N / 2) * SP
                    r2 = cx2 + cy * cy
                    t = r2 * horner(r2, G_C)
                    pairs = [cis_turns(t * w[pi]) for pi in range(2)]
                    if 0 < y0 < 8:
                        for pi in range(2):
                            cs[s, a, kap, pi, 0] = pairs[pi][0]
                            cs[s, a, kap, pi, 1] = pairs[pi][1]
                else:
                    pairs = [(cs[s, a, kap, pi, 0], cs[s, a, kap, pi, 1]) for pi in range(2)]
                sr = xin[slot, s, y0, 8 * a : 8 * a + 8, 0:128]
                si = xin[slot, s, y0, 8 * a : 8 * a + 8, 128:256]
                for pi, (c, n) in enumerate(pairs):
                    r0 = 64 * a + 16 * q + 8 * pi
                    h, l = split(jnp.concatenate([sr * c - si * n, sr * n + si * c], axis=1))
                    xh[p, r0 : r0 + 8, :] = h
                    xl[p, r0 : r0 + 8, :] = l

    def long_part(xh, xl, yb):
        for p in range(4):
            x = xh[p]
            yb[p] = bdot(x, eh[p]) + bdot(xl[p], eh[p]) + bdot(x, el[p])

    def short_one(slot, s, yb, a, pi):
        sums = None
        for q in range(4):
            r0 = 64 * a + 16 * q + 8 * pi
            rows = pl.ds(r0 if isinstance(r0, int) else pl.multiple_of(r0, 8), 8)
            v = butterfly4([(yb[p, rows, 0:128], yb[p, rows, 128:256]) for p in range(4)])
            if q:
                out = []
                for j, (r, i) in enumerate(v):
                    k = 8 * (q - 1) + 2 * j
                    out.append((r * tw[k] - i * tw[k + 1], r * tw[k + 1] + i * tw[k]))
                v = out
            sums = v if sums is None else [(x + u, y + z) for (x, y), (u, z) in zip(sums, v)]
        for j, (vr, vi) in enumerate(sums):
            cc = slice(128 * (j % 2), 128 * (j % 2) + 128)
            gb[slot, s, j // 2, pi, 0, a, :, cc] = vr
            gb[slot, s, j // 2, pi, 1, a, :, cc] = vi

    def short_part(slot, s, yb):
        for a in range(2):
            for pi in range(2):
                short_one(slot, s, yb, a, pi)

    def short_tail(i, carry):
        for s, yb in enumerate((yb0, yb1)):
            short_one((steps - 1) % 2, s, yb, i >> 1, i & 1)
        return carry

    def step(k, slot3):
        @pl.when(k >= 2)
        def _():
            for c in stores(k - 2, k & 1):
                c.start()

        @pl.when(k >= 3)
        def _():
            for c in stores(k - 3, 1 - (k & 1)):
                c.wait()

        ahead = jnp.where(slot3 == 0, 2, slot3 - 1)

        @pl.when(k + 2 < steps)
        def _():
            for a in range(2):
                load(2 * k + 4 + a, ahead, a)

        for a in range(2):
            pltpu.make_async_copy(xin.at[slot3, a], xin.at[slot3, a], sem_in.at[slot3, a]).wait()
        done = 1 - (k & 1)
        long_part(xh1, xl1, yb1)
        short_part(done, 0, yb0)
        image(2 * k, slot3, 0, xh0, xl0)
        long_part(xh0, xl0, yb0)
        short_part(done, 1, yb1)
        image(2 * k + 1, slot3, 1, xh1, xl1)
        return jnp.where(slot3 == 2, 0, slot3 + 1)

    def arrived(slot):
        for a in range(2):
            pltpu.make_async_copy(xin.at[slot, a], xin.at[slot, a], sem_in.at[slot, a]).wait()

    if steps > 2:
        for a in range(2):
            load(4 + a, 2, a)
    arrived(0)
    image(0, 0, 0, xh0, xl0)
    for c in e_copies:
        c.wait()
    long_part(xh0, xl0, yb0)
    image(1, 0, 1, xh1, xl1)
    lax.fori_loop(1, steps, step, jnp.int32(1))
    last = (steps - 1) % 2
    if steps >= 2:
        for c in stores(steps - 2, steps % 2):
            c.start()
    if steps >= 3:
        for c in stores(steps - 3, last):
            c.wait()
    long_part(xh1, xl1, yb1)
    lax.fori_loop(0, 4, short_tail, 0)
    for c in stores(steps - 1, last):
        c.start()
    if steps >= 2:
        for c in stores(steps - 2, steps % 2):
            c.wait()
    for c in stores(steps - 1, last):
        c.wait()


def along_y(plan, ws, e1, srcs):
    total = sum(blk["rows"] for blk in plan)
    out = jax.ShapeDtypeStruct((2, 2, total // 8, 8, 256), F32)
    stage = [pltpu.VMEM((4, 128, 256), BF16), pltpu.VMEM((4, 128, 256), BF16), pltpu.VMEM((4, 128, 256), F32)]
    return pl.pallas_call(
        functools.partial(along_y_kernel, plan, len(srcs)),
        out_shape=[out, out],
        in_specs=[SMEM] * 2 + [HBM] * (3 + len(srcs)),
        out_specs=[HBM, HBM],
        scratch_shapes=[
            pltpu.VMEM((4, 256, 256), BF16),
            pltpu.VMEM((4, 256, 256), BF16),
            pltpu.VMEM((24, 8, 128), F32),
            pltpu.VMEM((3, 2, 16, 16, 256), F32),
            *stage,
            *stage,
            pltpu.VMEM((2, 2, 2, 2, 2, 2, 8, 256), F32),
            pltpu.VMEM((2, 2, 8, 2, 2, 8, 128), F32),
            pltpu.SMEM((total // 8,), jnp.int32),
            pltpu.SMEM((total // 8,), jnp.int32),
            pltpu.SemaphoreType.DMA((3,)),
            pltpu.SemaphoreType.DMA((3, 2)),
            pltpu.SemaphoreType.DMA((2, 2, 2)),
        ],
        compiler_params=pltpu.CompilerParams(vmem_limit_bytes=67043328),
        cost_estimate=pl.CostEstimate(
            flops=total * 2 * 16 * 3 * 256 * 256 * 2, bytes_accessed=total * 24 * 1024, transcendentals=0
        ),
    )(*ws, *e1, *srcs)


def butterfly4(v):
    (r0, i0), (r1, i1), (r2, i2), (r3, i3) = v
    ar, ai, br, bi = r0 + r2, i0 + i2, r0 - r2, i0 - i2
    cr, ci, dr, di = r1 + r3, i1 + i3, r1 - r3, i1 - i3
    return [(ar + cr, ai + ci), (br + di, bi - dr), (ar - cr, ai - ci), (br - di, bi + dr)]


def dft16(v, tw):
    out = [None] * 16
    inner = [butterfly4([v[4 * p + q] for p in range(4)]) for q in range(4)]
    for t0 in range(4):
        cols = [inner[0][t0]]
        for q in range(1, 4):
            (r, i), (c, s) = inner[q][t0], tw(4 * (q - 1) + t0)
            cols.append((r * c - i * s, r * s + i * c))
        for t1, val in enumerate(butterfly4(cols)):
            out[t0 + 4 * t1] = val
    return out


def along_x_kernel(plans, kt, e2h, e2l, tw2, pos_a, pos_b, *rest):
    ids = place_ids()
    n = len(plans)
    parts = rest[: 2 * n]
    out_a, out_b = rest[2 * n : 2 * n + 2]
    eh, el, tw, pv, d, f0, f1, grid = rest[2 * n + 2 : 2 * n + 10]
    bufs = [rest[2 * n + 10 + 4 * k : 2 * n + 14 + 4 * k] for k in range(4)]
    res, wide, lst, notes, sem, sem_e, sem_o = rest[2 * n + 26 :]
    f = (f0, f1)
    core = ids[0]
    loads = []
    for i, plan in enumerate(plans):
        off = 0
        for blk in plan:
            for slab, first, cnt in block_rows(blk, ids):
                base = 32 * slab + 8 * (first >> 7)
                for ref, side in ((parts[2 * i], core), (parts[2 * i + 1], 1 - core)):
                    at = pl.ds(pl.multiple_of(base + 16 * side, 8), 8)
                    loads.append((ref, off, cnt, (first >> 3) & 15, at))
                off += cnt
    for pi in range(2):
        for ref, off, cnt, j0, at in loads:
            dst = d.at[pi, :, pl.ds(j0, cnt), at, :]
            pltpu.make_async_copy(ref.at[pi, :, pl.ds(off, cnt)], dst, sem.at[pi]).start()
    last8 = pl.ds(64, 8)
    notice = [
        pltpu.make_async_copy(src.at[:, last8, :], notes.at[i], sem_o.at[i]) for i, src in enumerate((pos_a, pos_b))
    ]
    for c in notice:
        c.start()
    small = [(e2h, eh), (e2l, el), (tw2, tw), (pos_a, pv.at[0]), (pos_b, pv.at[1])]
    small = [pltpu.make_async_copy(s, t, sem_e.at[i]) for i, (s, t) in enumerate(small)]
    for c in small:
        c.start()
    res[...] = jnp.zeros_like(res)
    for c in notice:
        c.wait()

    def tile_of(sid):
        return notes[sid >> 7, (sid & 127) >> 3, 0, sid & 7]

    def scan(s, cnt):
        for k in range(8):
            t = notes[s >> 4, s & 15, 0, k]
            lst[cnt] = 8 * s + k
            mine = jnp.logical_and(t > 0, (((t - 1) >> 1) & 1) == core)
            cnt = cnt + mine.astype(jnp.int32)
        return cnt

    lst[0] = 0
    count = lax.fori_loop(0, 32, scan, jnp.int32(0))
    last = jnp.where(count > 0, lst[jnp.maximum(count - 1, 0)], 0)
    for k in range(8):
        lst[count + k] = last
    for c in small:
        c.wait()
    pltpu.make_async_copy(d.at[0], d.at[0], sem.at[0]).wait()

    def first(pi, k, qs=range(4)):
        for q in qs:
            x0 = 4 * k + q
            h, l = split(jnp.concatenate([d[pi, 0, x0], d[pi, 1, x0]], axis=0))
            f[pi][x0] = bdot(eh[k], h) + bdot(el[k], h) + bdot(eh[k], l)

    def second(pi, m):
        rr = pl.ds(pl.multiple_of(8 * m, 8), 8)
        ri = pl.ds(pl.multiple_of(128 + 8 * m, 8), 8)
        for jj in range(2):
            cc = slice(128 * jj, 128 * jj + 128)
            v = [(f[pi][x0, rr, cc], f[pi][x0, ri, cc]) for x0 in range(16)]
            v = dft16(v, lambda k: (tw[0, k, rr, :], tw[1, k, rr, :]))
            for t in range(16):
                grid[(pi * 2 + jj) * 16 + t, rr, :] = v[t][0]
                grid[(pi * 2 + jj) * 16 + t, ri, :] = v[t][1]

    def stage0(k, carry):
        first(0, k)
        return carry

    def stage1(k, carry):
        for m in range(4):
            first(1, k, (m,))
            second(0, 4 * k + m)
        return carry

    def stage2(k, carry):
        second(1, k)
        return carry

    lax.fori_loop(0, 4, stage0, 0)
    pltpu.make_async_copy(d.at[1], d.at[1], sem.at[1]).wait()
    lax.fori_loop(0, 4, stage1, 0)
    lax.fori_loop(0, 16, stage2, 0)

    sub = lax.broadcasted_iota(jnp.int32, (8, 128), 0)
    lane = lax.broadcasted_iota(jnp.int32, (8, 128), 1)
    wide[...] = jnp.zeros_like(wide)
    wide[:, 0:16] = kt[...]
    spread = jnp.take_along_axis(wide[...], lane >> 3, axis=1)
    table = jnp.broadcast_to(jnp.sum(jnp.where(sub == (lane & 7), spread, 0.0), axis=0, keepdims=True), (8, 128))

    def taps(row):
        row = jnp.broadcast_to(row, (8, 128))
        off = row & 15
        cell = row >> 4
        cl = cell & 7
        idx = off * 8 + ((sub - cl) & 7)
        return jnp.take_along_axis(table, idx, axis=1), (cell >> 3) + (sub < cl).astype(jnp.int32)

    def build(sid, buf):
        ww, wl, ru, hu = buf
        pos = pv[sid >> 7, (sid & 127) >> 3, pl.ds(pl.multiple_of(8 * (sid & 7), 8), 8), :]
        for jp in range(2):
            th = []
            for j in (2 * jp, 2 * jp + 1):
                r, h = taps(pos[4 + j : 5 + j, :])
                rh = r.astype(BF16).astype(F32)
                th.append((rh, r - rh, h))
                ru[j], hu[j] = taps(pos[j : j + 1, :])
            cc = slice(256 * jp, 256 * jp + 256)
            for i in range(16):
                masks = [h == i for _, _, h in th]
                wh = jnp.concatenate([jnp.where(m, v[0], 0.0) for m, v in zip(masks, th)], axis=1).astype(BF16)
                ww[8 * i : 8 * i + 8, cc] = wh
                ww[128 + 8 * i : 136 + 8 * i, cc] = wh
                wl[8 * i : 8 * i + 8, cc] = jnp.concatenate(
                    [jnp.where(m, v[1], 0.0) for m, v in zip(masks, th)], axis=1
                ).astype(BF16)

    def finish(sid, buf):
        ww, wl, ru, hu = buf
        t = jnp.maximum(tile_of(sid) - 1, 0)
        x = grid[(((sid >> 1) & 1) * 2 + (t & 1)) * 16 + (t >> 4)]
        h = x.astype(BF16)
        hf = h.astype(F32)
        part = bdot(jnp.concatenate([hf, x - hf], axis=1).astype(BF16), ww[...]) + bdot(h, wl[...])
        rows = []
        for j in range(4):
            r, h = ru[j], hu[j]
            for c in range(2):
                acc = jnp.zeros((8, 128), F32)
                for i in range(16):
                    acc = jnp.where(h == i, part[128 * c + 8 * i : 128 * c + 8 * i + 8, 128 * j : 128 * j + 128], acc)
                rows.append(jnp.sum(r * acc, axis=0, keepdims=True))
        res[sid] = jnp.concatenate(rows[0::2] + rows[1::2], axis=0)

    build(lst[0], bufs[0])
    build(lst[1], bufs[1])

    def four(i, carry):
        for k in range(4):
            finish(lst[4 * i + k], bufs[k])
            build(lst[4 * i + 2 + k], bufs[(k + 2) % 4])
        return carry

    lax.fori_loop(0, (count + 3) >> 2, four, 0)
    moves = [
        pltpu.make_async_copy(res.at[pl.ds(0, 128)], out_a, sem_o.at[0]),
        pltpu.make_async_copy(res.at[pl.ds(128, 128)], out_b, sem_o.at[1]),
    ]
    for m in moves:
        m.start()
    for m in moves:
        m.wait()


def along_x(plans, kt, e2, pos_a, pos_b, parts):
    buf = [
        pltpu.VMEM((256, 512), BF16),
        pltpu.VMEM((128, 512), BF16),
        pltpu.VMEM((4, 8, 128), F32),
        pltpu.VMEM((4, 8, 128), jnp.int32),
    ]
    return pl.pallas_call(
        functools.partial(along_x_kernel, plans),
        out_shape=[jax.ShapeDtypeStruct((128, 8, 128), F32)] * 2,
        in_specs=[VMEM] + [HBM] * (5 + len(parts)),
        out_specs=[HBM, HBM],
        scratch_shapes=[
            pltpu.VMEM((4, 256, 256), BF16),
            pltpu.VMEM((4, 256, 256), BF16),
            pltpu.VMEM((2, 12, 128, 128), F32),
            pltpu.VMEM((2, 16, 72, 128), jnp.int32),
            pltpu.VMEM((2, 2, 16, 128, 256), F32),
            pltpu.VMEM((16, 256, 256), F32),
            pltpu.VMEM((16, 256, 256), F32),
            pltpu.VMEM((64, 256, 128), F32),
            *buf,
            *buf,
            *buf,
            *buf,
            pltpu.VMEM((256, 8, 128), F32),
            pltpu.VMEM((8, 128), F32),
            pltpu.SMEM((272,), jnp.int32),
            pltpu.SMEM((2, 16, 8, 128), jnp.int32),
            pltpu.SemaphoreType.DMA((2,)),
            pltpu.SemaphoreType.DMA((5,)),
            pltpu.SemaphoreType.DMA((2,)),
        ],
        compiler_params=pltpu.CompilerParams(vmem_limit_bytes=67043328),
        cost_estimate=pl.CostEstimate(flops=60_000_000_000, bytes_accessed=16 << 20, transcendentals=0),
        name="along_x",
    )(kt, *e2, pos_a, pos_b, *parts)


def arrange_kernel(mine, got, payload, here, there, blocks, notes, sem):
    zh = lax.axis_index("zh")
    copies = []
    for i, src in enumerate((mine, got)):
        copies.append(pltpu.make_async_copy(src.at[pl.ds(0, 16)], blocks.at[i], sem.at[2 * i]))
        copies.append(pltpu.make_async_copy(src.at[16], notes.at[i], sem.at[2 * i + 1]))
    for c in copies:
        c.start()
    for c in copies:
        c.wait()
    payload[:, 64:72, :] = jnp.zeros((16, 8, 128), jnp.int32)
    lane = lax.broadcasted_iota(jnp.int32, (8, 128), 1)
    for i, (out, home) in enumerate(((here, zh), (there, 1 - zh))):
        def one(b, carry, i=i, out=out, home=home):
            slot, tile = notes[i, 0, b], notes[i, 1, b]
            mine = (slot >> 6) == zh
            chip, k = (slot >> 2) & 15, 4 * home + (slot & 3)
            out[b] = jnp.where(mine, 8 * chip + k, -1)

            @pl.when(mine)
            def _():
                payload[chip, pl.ds(pl.multiple_of(8 * k, 8), 8), :] = blocks[i, b]
                payload[chip, 64:72, :] = jnp.where(lane == k, tile, payload[chip, 64:72, :])

            return carry

        lax.fori_loop(0, 16, one, 0)


def arrange(mine, got):
    i32 = jnp.int32
    return pl.pallas_call(
        arrange_kernel,
        out_shape=[jax.ShapeDtypeStruct((16, 72, 128), i32)] + [jax.ShapeDtypeStruct((16,), i32)] * 2,
        in_specs=[HBM, HBM],
        out_specs=[VMEM, SMEM, SMEM],
        scratch_shapes=[
            pltpu.VMEM((2, 16, 8, 128), i32),
            pltpu.SMEM((2, 8, 128), i32),
            pltpu.SemaphoreType.DMA((4,)),
        ],
        compiler_params=pltpu.CompilerParams(vmem_limit_bytes=8 << 20),
        cost_estimate=pl.CostEstimate(flops=1 << 20, bytes_accessed=1 << 20, transcendentals=0),
        name="arrange",
    )(mine, got)


def pick_kernel(here, there, answers, observed, rest, other):
    for b in range(16):
        i, j = here[b], there[b]
        v = answers[jnp.maximum(i, 0)]
        rest[b] = observed[b] - jnp.where(i >= 0, v, 0.0)
        v = answers[jnp.maximum(j, 0)]
        other[b] = jnp.where(j >= 0, v, 0.0)


def pick(here, there, answers, observed):
    return pl.pallas_call(
        pick_kernel,
        out_shape=[jax.ShapeDtypeStruct((16, 8, 128), F32)] * 2,
        in_specs=[SMEM, SMEM, VMEM, VMEM],
        out_specs=[VMEM, VMEM],
        compiler_params=pltpu.CompilerParams(vmem_limit_bytes=8 << 20),
        name="pick",
    )(here, there, answers, observed)


def shift(x, axes, size, by):
    return lax.ppermute(x, axes, [(i, (i + by) % size) for i in range(size)])


def shards(sky, plane_w, kernel, tile_ids, plane_ids, positions, observed):
    i32 = jnp.int32
    z_axes = ("zh", "wa")
    swap = [(0, 1), (1, 0)]

    target = plane_ids[:, 0]
    same = (target[:, None] == target[None, :]).astype(i32)
    slot = target * 2 + jnp.sum(jnp.tril(same, -1), axis=1)
    notes = jnp.pad(jnp.stack([slot, tile_ids + 1]), ((0, 6), (0, 112)))
    mine0 = jnp.concatenate([positions.reshape(16, 8, 128), notes[None]], axis=0)
    got0 = lax.ppermute(mine0, "zh", swap)

    own0, ab, pa, pb = turn(0, sky)
    zl = shift(ab, z_axes, 8, 1)
    zr = shift(ab, z_axes, 8, -1)
    za = shift(pa, z_axes, 8, 2)
    zb = shift(pb, z_axes, 8, -2)
    lo, hi = turn(1, sky)
    cl_lo = shift(lo, z_axes, 8, 1)
    cr_hi = shift(hi, z_axes, 8, -1)
    cl_hi = shift(hi, z_axes, 8, 1)
    cr_lo = shift(lo, z_axes, 8, -1)
    cf_lo = shift(cl_lo, z_axes, 8, 1)
    cf_hi = shift(cr_hi, z_axes, 8, -1)

    mine_a, mine_b = gather3(zl, zr, za, zb)

    def three(x, axis):
        l = shift(x, axis, 4, 1)
        r = shift(x, axis, 4, -1)
        return r, shift(x, axis, 4, 2), l

    ax, bx = three(mine_a, "x"), three(mine_b, "y")
    a0, b0 = join((mine_a,) + ax, (mine_b,) + bx)
    ar, af, al = three(a0, "y")
    br, bf, bl = three(b0, "x")

    payload, here, there = arrange(mine0, got0)
    asked = lax.all_to_all(payload, ("x", "y"), split_axis=0, concat_axis=0, tiled=True)
    asked_b = lax.ppermute(asked, "core", swap)
    other_w = lax.ppermute(plane_w, "core", swap)
    ws = plane_w, other_w
    *e1, tw1, tw2 = tables()
    e1, e2 = e1[:2] + [tw1], e1[2:] + [tw2]
    plans, parts = [], []

    def call(plan, srcs):
        keep, send = along_y(plan, ws, e1, srcs)
        plans.append(plan)
        parts.extend([keep, lax.ppermute(send, "core", swap)])

    def blk(kind, d, rows, row, *src):
        return dict(kind=kind, d=d, rows=rows, row=row, src=src)

    call([blk("own", 0, 128, 0, 0)], [own0])
    call([blk("own", 128, 128, 0, 0, 1), blk("a", 0, 3 * R, 0, 2), blk("b", 0, 3 * R, 0, 3)], [lo, hi, a0, b0])
    call(
        [
            blk("c", 0, CR, 0, 0, 1),
            blk("c", 1, CR, 0, 2, 3),
            blk("a", 3, 3 * R, 0, 4),
            blk("a", 1, 3 * R, 0, 5),
            blk("b", 3, 3 * R, 0, 6),
            blk("b", 1, 3 * R, 0, 7),
        ],
        [cl_lo, cl_hi, cr_lo, cr_hi, al, ar, bl, br],
    )
    call([blk("c", 2, CR, 0, 0, 1), blk("a", 2, 3 * R, 0, 2), blk("b", 2, 3 * R, 0, 3)], [cf_lo, cf_hi, af, bf])

    out_a, out_b = along_x(plans, kernel.T, e2, asked, asked_b, parts)
    from_b = lax.ppermute(out_b, "core", swap)
    merged = out_a + from_b
    answers = lax.all_to_all(merged.reshape(16, 64, 128), ("x", "y"), split_axis=0, concat_axis=0, tiled=True)
    rest, other = pick(here, there, answers.reshape(128, 8, 128), observed.reshape(16, 8, 128))
    got = lax.ppermute(other, "zh", swap)
    return (rest - got).reshape(16, 2, 512)


def solution(mesh):
    fine = Mesh(mesh.devices.reshape(2, 4, 4, 2, 4), ("zh", "x", "y", "core", "wa"))
    ba = ("zh", "x", "y", "core")
    rows = ba + ("wa",)
    return jax.shard_map(
        shards,
        mesh=fine,
        in_specs=(
            P(None, None, "wa"),
            P(ba),
            P(),
            P(rows),
            P(rows, None),
            P(rows, None, None),
            P(rows, None, None),
        ),
        out_specs=P(rows, None, None),
        check_vma=False,
    )
```

```python
import functools

import jax
import jax.numpy as jnp
from jax import lax
from jax.experimental import pallas as pl
from jax.experimental.pallas import tpu as pltpu
from jax.sharding import Mesh
from jax.sharding import PartitionSpec as P


N = 2048
SP = 0.7 / N
R = 16
CR = 128
SMEM = pl.BlockSpec(memory_space=pltpu.SMEM)
VMEM = pl.BlockSpec(memory_space=pltpu.VMEM)
HBM = pl.BlockSpec(memory_space=pltpu.HBM)
F32 = jnp.float32
BF16 = jnp.bfloat16

SIN_C = (3.14159264, -5.16771009, 2.55007766, -0.59829216, 0.07765941)
COS_C = (0.99999995, -4.93479286, 4.05841191, -1.33188016, 0.21969679)
G_C = (0.5, 0.12500105, 0.0624521, 0.03985648, 0.0215331, 0.03890036)
MAGIC = 12582912.0


def place_ids():
    return tuple(lax.axis_index(n) for n in ("core", "wa", "x", "y"))


def horner(z, coefs):
    acc = jnp.full_like(z, coefs[-1])
    for c in coefs[-2::-1]:
        acc = acc * z + c
    return acc


def cis_turns(t):
    r = t - ((t + MAGIC) - MAGIC)
    z = r * r
    s = r * horner(z, SIN_C)
    c = horner(z, COS_C)
    s2 = s + s
    return 1.0 - s2 * s, s2 * c


def split(x):
    hi = x.astype(BF16)
    return hi, (x - hi.astype(F32)).astype(BF16)


def bdot(a, b):
    return jnp.dot(a, b, preferred_element_type=F32)


def tables_kernel(e1h, e1l, e2h, e2l, tw1, tw2):
    row = lax.broadcasted_iota(jnp.int32, (128, 128), 0)
    col = lax.broadcasted_iota(jnp.int32, (128, 128), 1)
    lane = lax.broadcasted_iota(jnp.int32, (8, 128), 1)

    ids = place_ids()

    def cs(k):
        return cis_turns((k & (N - 1)).astype(F32) * (1.0 / N))

    def put(h, l, i, r, c, v):
        a, b = v
        h[i, 128 * r : 128 * r + 128, 128 * c : 128 * c + 128] = a
        l[i, 128 * r : 128 * r + 128, 128 * c : 128 * c + 128] = b

    def matrices(p, carry):
        y = 16 * jnp.where(p > 1, 127 - row, row) + 4 * p
        c, s = cs(col * y)
        ch, sh = split(c), split(s)
        put(e1h, e1l, p, 0, 0, ch)
        put(e1h, e1l, p, 1, 1, ch)
        put(e1h, e1l, p, 0, 1, (-sh[0], -sh[1]))
        put(e1h, e1l, p, 1, 0, sh)
        c, s = cs(row * (16 * col + 4 * p))
        ch, sh = split(c * (1.0 / N)), split(s * (1.0 / N))
        put(e2h, e2l, p, 0, 0, ch)
        put(e2h, e2l, p, 1, 1, ch)
        put(e2h, e2l, p, 0, 1, sh)
        put(e2h, e2l, p, 1, 0, (-sh[0], -sh[1]))
        return carry

    def factors(k, carry):
        q, j = 1 + (k >> 2), k & 3
        c, s = cs((512 * ids[1] + 128 * j + lane) * q)
        tw1[2 * k] = c
        tw1[2 * k + 1] = -s
        c, s = cs((128 * j + row) * q)
        tw2[0, k] = c
        tw2[1, k] = -s
        return carry

    lax.fori_loop(0, 4, matrices, 0)
    lax.fori_loop(0, 12, factors, 0)


def tables():
    sds = jax.ShapeDtypeStruct
    shapes = [sds((4, 256, 256), BF16)] * 4 + [sds((24, 8, 128), F32), sds((2, 12, 128, 128), F32)]
    return pl.pallas_call(
        tables_kernel,
        out_shape=shapes,
        out_specs=[VMEM] * 6,
        cost_estimate=pl.CostEstimate(flops=60 * 16 * 2 * 16384, bytes_accessed=4 << 20, transcendentals=0),
        name="tables",
    )()


def turn_kernel(b, sky, own, *rest):
    core, _, xc, yc = place_ids()
    outs, (xin, t, tmp, sem_in, sem_out) = rest[:-5], rest[-5:]
    own, outs = ((own,), outs) if b == 0 else ((own, outs[0]), ())
    loads = []
    for c in range(2):
        col = pl.multiple_of(256 * core + 128 * b, 128)
        loads.append(pltpu.make_async_copy(sky.at[c, :, pl.ds(col, 128)], xin.at[c], sem_in.at[c]))
        loads[c].start()
    moves = []

    def move(src, dst):
        moves.append(pltpu.make_async_copy(src, dst, sem_out.at[len(moves)]))
        moves[-1].start()

    def part(y4):
        return own[0].at[pl.ds(4 * y4, 4)] if b == 0 else own[y4 // 2].at[pl.ds(4 * (y4 % 2), 4)]

    rev = 127 - lax.broadcasted_iota(jnp.int32, (128, 128), 1)
    for c in range(2):
        loads[c].wait()
        for y4 in range(4):
            def group(i, carry, y4=y4, c=c):
                for e in range(2):
                    y0 = 4 * y4 + 2 * i + e
                    v = xin[c, pl.ds(y0, 128, stride=16), :].T
                    if y4 > 1:
                        v = jnp.take_along_axis(v, rev, axis=1)
                    tmp[e] = v
                    for j0 in range(16):
                        t[y0, 8 * j0 : 8 * j0 + 8, 128 * c : 128 * c + 128] = tmp[e, pl.ds(j0, 8, stride=16), :]
                return carry

            lax.fori_loop(0, 2, group, 0)
            if c == 1 and y4 < 3:
                move(t.at[pl.ds(4 * y4, 4)], part(y4))
    if outs:
        a_src = t.at[pl.ds(4 * xc, 4), pl.ds(pl.multiple_of(R * yc, 8), R), :]
        b_src = t.at[pl.ds(4 * yc, 4), pl.ds(pl.multiple_of(4 * R + R * xc, 8), R), :]
        (ab,) = outs
        move(a_src, ab.at[0])
        move(b_src, ab.at[1])
    move(t.at[pl.ds(12, 4)], part(3))
    for m in moves:
        m.wait()


def turn(b, sky):
    sds = lambda *d: jax.ShapeDtypeStruct(d, F32)
    outs = [sds(8, 128, 256)] * 2 if b else [sds(16, 128, 256), sds(2, 4, R, 256)]
    return pl.pallas_call(
        functools.partial(turn_kernel, b),
        in_specs=[HBM],
        out_specs=[HBM] * len(outs),
        out_shape=outs,
        scratch_shapes=[
            pltpu.VMEM((2, N, 128), F32),
            pltpu.VMEM((16, 128, 256), F32),
            pltpu.VMEM((4, 128, 128), F32),
            pltpu.SemaphoreType.DMA((2,)),
            pltpu.SemaphoreType.DMA((8,)),
        ],
        cost_estimate=pl.CostEstimate(flops=1 << 22, bytes_accessed=4 << 20, transcendentals=0),
    )(sky)


def gather3_kernel(zl, zr, zf, oa, ob):
    for k, o in enumerate((oa, ob)):
        for i, z in enumerate((zl, zr, zf)):
            o[:, R * i : R * i + R, :] = z[k]


def gather3(*z):
    return pl.pallas_call(
        gather3_kernel,
        out_shape=[jax.ShapeDtypeStruct((4, 3 * R, 256), F32)] * 2,
        in_specs=[VMEM] * 3,
        out_specs=[VMEM] * 2,
        compiler_params=pltpu.CompilerParams(vmem_limit_bytes=8 << 20),
        cost_estimate=pl.CostEstimate(flops=1 << 20, bytes_accessed=1 << 20, transcendentals=0),
        name="gather3",
    )(*z)


def join_kernel(*refs):
    ids = place_ids()
    for k in range(4):
        for base, ref, o in ((ids[2], refs[k], refs[8]), (ids[3], refs[4 + k], refs[9])):
            o[pl.ds(4 * ((base + k) & 3), 4)] = ref[...]


def join(a, b):
    return pl.pallas_call(
        join_kernel,
        out_shape=[jax.ShapeDtypeStruct((16, 3 * R, 256), F32)] * 2,
        in_specs=[VMEM] * 8,
        out_specs=[VMEM] * 2,
        compiler_params=pltpu.CompilerParams(vmem_limit_bytes=16 << 20),
        cost_estimate=pl.CostEstimate(flops=1 << 20, bytes_accessed=3 << 20, transcendentals=0),
        name="join",
    )(*a, *b)


def slab_of(kind, k, ids):
    a = ids[1]
    return (a + (0 if kind == "own" else (3, 1, 2)[k])) & 3


def block_rows(blk, ids):
    kind, d, n = blk["kind"], blk["d"], blk["rows"]
    if kind == "own":
        return [(slab_of(kind, 0, ids), d, n // 8)]
    if kind == "c":
        return [(slab_of(kind, d, ids), 128, n // 8)]
    first = R * ((ids[3] + d) & 3) if kind == "a" else 4 * R + R * ((ids[2] + d) & 3)
    return [(slab_of(kind, k, ids), first, R // 8) for k in range(3)]


def along_y_kernel(plan, n_src, w_own, w_other, e1h, e1l, tw1, *rest):
    ids = place_ids()
    srcs = rest[:n_src]
    keep, send = rest[n_src : n_src + 2]
    eh, el, tw, xin, xh0, xl0, yb0, xh1, xl1, yb1, gb, cs, tab, where, sem_e, sem_in, sem_out = rest[n_src + 2 :]
    core = ids[0]
    lane = lax.broadcasted_iota(jnp.int32, (8, 128), 1)
    sub = lax.broadcasted_iota(jnp.int32, (8, 128), 0)
    w = [jnp.where(core == pi, w_own[0], w_other[0]) for pi in range(2)]
    n_pairs = sum(blk["rows"] for blk in plan) // 16
    steps = n_pairs // 2

    kinds, k = [], 0
    for blk in plan:
        if blk["src"] not in kinds:
            kinds.append(blk["src"])
        for i in range(blk["rows"] // 16):
            where[2 * k] = kinds.index(blk["src"])
            where[2 * k + 1] = blk["row"] + 16 * i
            k += 1
    k = 0
    for blk in plan:
        for slab, first, n in block_rows(blk, ids):
            for i in range(n):
                row = first + 8 * i
                tab[k] = 512 * slab + 256 * core + 128 * (row >> 7) + ((row >> 3) & 15)
                k += 1

    def load(pair, slot, a):
        kind, row = where[2 * pair], pl.ds(pl.multiple_of(where[2 * pair + 1], 16), 16)
        for i, src in enumerate(kinds):
            @pl.when(kind == i)
            def _(src=src):
                h = 16 // len(src)
                for j, s in enumerate(src):
                    pltpu.make_async_copy(
                        srcs[s].at[:, row, :], xin.at[slot, a, pl.ds(h * j, h)], sem_in.at[slot, a]
                    ).start()

    def stores(k, slot):
        out = []
        for a in range(2):
            dst = pl.ds(4 * k + 2 * a, 2)
            out.append(pltpu.make_async_copy(gb.at[slot, a, core], keep.at[:, :, dst], sem_out.at[slot, a, 0]))
            out.append(pltpu.make_async_copy(gb.at[slot, a, 1 - core], send.at[:, :, dst], sem_out.at[slot, a, 1]))
        return out

    for k in range(min(2, steps)):
        for a in range(2):
            load(2 * k + a, k, a)

    e_copies = [
        pltpu.make_async_copy(src, dst, sem_e.at[i]) for i, (src, dst) in enumerate(((e1h, eh), (e1l, el), (tw1, tw)))
    ]
    for c in e_copies:
        c.start()

    def image(pair, slot, s, xh, xl):
        for a in range(2):
            cx = ((tab[2 * pair + a] + 16 * sub).astype(F32) - N / 2) * SP
            cx2 = cx * cx
            for y0 in range(16):
                p, q = y0 // 4, y0 % 4
                kap = min(y0, 16 - y0)
                if y0 <= 8:
                    cy = ((16 * lane + kap).astype(F32) - N / 2) * SP
                    r2 = cx2 + cy * cy
                    t = r2 * horner(r2, G_C)
                    pairs = [cis_turns(t * w[pi]) for pi in range(2)]
                    if 0 < y0 < 8:
                        for pi in range(2):
                            cs[s, a, kap, pi, 0] = pairs[pi][0]
                            cs[s, a, kap, pi, 1] = pairs[pi][1]
                else:
                    pairs = [(cs[s, a, kap, pi, 0], cs[s, a, kap, pi, 1]) for pi in range(2)]
                sr = xin[slot, s, y0, 8 * a : 8 * a + 8, 0:128]
                si = xin[slot, s, y0, 8 * a : 8 * a + 8, 128:256]
                for pi, (c, n) in enumerate(pairs):
                    r0 = 64 * a + 16 * q + 8 * pi
                    h, l = split(jnp.concatenate([sr * c - si * n, sr * n + si * c], axis=1))
                    xh[p, r0 : r0 + 8, :] = h
                    xl[p, r0 : r0 + 8, :] = l

    def long_part(xh, xl, yb):
        for p in range(4):
            x = xh[p]
            yb[p] = bdot(x, eh[p]) + bdot(xl[p], eh[p]) + bdot(x, el[p])

    def short_one(slot, s, yb, a, pi):
        sums = None
        for q in range(4):
            r0 = 64 * a + 16 * q + 8 * pi
            rows = pl.ds(r0 if isinstance(r0, int) else pl.multiple_of(r0, 8), 8)
            v = butterfly4([(yb[p, rows, 0:128], yb[p, rows, 128:256]) for p in range(4)])
            if q:
                out = []
                for j, (r, i) in enumerate(v):
                    k = 8 * (q - 1) + 2 * j
                    out.append((r * tw[k] - i * tw[k + 1], r * tw[k + 1] + i * tw[k]))
                v = out
            sums = v if sums is None else [(x + u, y + z) for (x, y), (u, z) in zip(sums, v)]
        for j, (vr, vi) in enumerate(sums):
            cc = slice(128 * (j % 2), 128 * (j % 2) + 128)
            gb[slot, s, j // 2, pi, 0, a, :, cc] = vr
            gb[slot, s, j // 2, pi, 1, a, :, cc] = vi

    def short_part(slot, s, yb):
        for a in range(2):
            for pi in range(2):
                short_one(slot, s, yb, a, pi)

    def short_tail(i, carry):
        for s, yb in enumerate((yb0, yb1)):
            short_one((steps - 1) % 2, s, yb, i >> 1, i & 1)
        return carry

    def step(k, slot3):
        @pl.when(k >= 2)
        def _():
            for c in stores(k - 2, k & 1):
                c.start()

        @pl.when(k >= 3)
        def _():
            for c in stores(k - 3, 1 - (k & 1)):
                c.wait()

        ahead = jnp.where(slot3 == 0, 2, slot3 - 1)

        @pl.when(k + 2 < steps)
        def _():
            for a in range(2):
                load(2 * k + 4 + a, ahead, a)

        for a in range(2):
            pltpu.make_async_copy(xin.at[slot3, a], xin.at[slot3, a], sem_in.at[slot3, a]).wait()
        done = 1 - (k & 1)
        long_part(xh1, xl1, yb1)
        short_part(done, 0, yb0)
        image(2 * k, slot3, 0, xh0, xl0)
        long_part(xh0, xl0, yb0)
        short_part(done, 1, yb1)
        image(2 * k + 1, slot3, 1, xh1, xl1)
        return jnp.where(slot3 == 2, 0, slot3 + 1)

    def arrived(slot):
        for a in range(2):
            pltpu.make_async_copy(xin.at[slot, a], xin.at[slot, a], sem_in.at[slot, a]).wait()

    if steps > 2:
        for a in range(2):
            load(4 + a, 2, a)
    arrived(0)
    image(0, 0, 0, xh0, xl0)
    for c in e_copies:
        c.wait()
    long_part(xh0, xl0, yb0)
    image(1, 0, 1, xh1, xl1)
    lax.fori_loop(1, steps, step, jnp.int32(1))
    last = (steps - 1) % 2
    if steps >= 2:
        for c in stores(steps - 2, steps % 2):
            c.start()
    if steps >= 3:
        for c in stores(steps - 3, last):
            c.wait()
    long_part(xh1, xl1, yb1)
    lax.fori_loop(0, 4, short_tail, 0)
    for c in stores(steps - 1, last):
        c.start()
    if steps >= 2:
        for c in stores(steps - 2, steps % 2):
            c.wait()
    for c in stores(steps - 1, last):
        c.wait()


def along_y(plan, ws, e1, srcs):
    total = sum(blk["rows"] for blk in plan)
    out = jax.ShapeDtypeStruct((2, 2, total // 8, 8, 256), F32)
    stage = [pltpu.VMEM((4, 128, 256), BF16), pltpu.VMEM((4, 128, 256), BF16), pltpu.VMEM((4, 128, 256), F32)]
    return pl.pallas_call(
        functools.partial(along_y_kernel, plan, len(srcs)),
        out_shape=[out, out],
        in_specs=[SMEM] * 2 + [HBM] * (3 + len(srcs)),
        out_specs=[HBM, HBM],
        scratch_shapes=[
            pltpu.VMEM((4, 256, 256), BF16),
            pltpu.VMEM((4, 256, 256), BF16),
            pltpu.VMEM((24, 8, 128), F32),
            pltpu.VMEM((3, 2, 16, 16, 256), F32),
            *stage,
            *stage,
            pltpu.VMEM((2, 2, 2, 2, 2, 2, 8, 256), F32),
            pltpu.VMEM((2, 2, 8, 2, 2, 8, 128), F32),
            pltpu.SMEM((total // 8,), jnp.int32),
            pltpu.SMEM((total // 8,), jnp.int32),
            pltpu.SemaphoreType.DMA((3,)),
            pltpu.SemaphoreType.DMA((3, 2)),
            pltpu.SemaphoreType.DMA((2, 2, 2)),
        ],
        compiler_params=pltpu.CompilerParams(vmem_limit_bytes=67043328),
        cost_estimate=pl.CostEstimate(
            flops=total * 2 * 16 * 3 * 256 * 256 * 2, bytes_accessed=total * 24 * 1024, transcendentals=0
        ),
    )(*ws, *e1, *srcs)


def butterfly4(v):
    (r0, i0), (r1, i1), (r2, i2), (r3, i3) = v
    ar, ai, br, bi = r0 + r2, i0 + i2, r0 - r2, i0 - i2
    cr, ci, dr, di = r1 + r3, i1 + i3, r1 - r3, i1 - i3
    return [(ar + cr, ai + ci), (br + di, bi - dr), (ar - cr, ai - ci), (br - di, bi + dr)]


def dft16(v, tw):
    out = [None] * 16
    inner = [butterfly4([v[4 * p + q] for p in range(4)]) for q in range(4)]
    for t0 in range(4):
        cols = [inner[0][t0]]
        for q in range(1, 4):
            (r, i), (c, s) = inner[q][t0], tw(4 * (q - 1) + t0)
            cols.append((r * c - i * s, r * s + i * c))
        for t1, val in enumerate(butterfly4(cols)):
            out[t0 + 4 * t1] = val
    return out


def along_x_kernel(plans, kt, e2h, e2l, tw2, pos_a, pos_b, *rest):
    ids = place_ids()
    n = len(plans)
    parts = rest[: 2 * n]
    out_a, out_b = rest[2 * n : 2 * n + 2]
    eh, el, tw, pv, d, f0, f1, grid = rest[2 * n + 2 : 2 * n + 10]
    bufs = [rest[2 * n + 10 + 4 * k : 2 * n + 14 + 4 * k] for k in range(4)]
    res, wide, lst, notes, sem, sem_e, sem_o = rest[2 * n + 26 :]
    f = (f0, f1)
    core = ids[0]
    loads = []
    for i, plan in enumerate(plans):
        off = 0
        for blk in plan:
            for slab, first, cnt in block_rows(blk, ids):
                base = 32 * slab + 8 * (first >> 7)
                for ref, side in ((parts[2 * i], core), (parts[2 * i + 1], 1 - core)):
                    at = pl.ds(pl.multiple_of(base + 16 * side, 8), 8)
                    loads.append((ref, off, cnt, (first >> 3) & 15, at))
                off += cnt
    for pi in range(2):
        for ref, off, cnt, j0, at in loads:
            dst = d.at[pi, :, pl.ds(j0, cnt), at, :]
            pltpu.make_async_copy(ref.at[pi, :, pl.ds(off, cnt)], dst, sem.at[pi]).start()
    last8 = pl.ds(64, 1)
    notice = [
        pltpu.make_async_copy(src.at[:, last8, :], notes.at[i], sem_o.at[i]) for i, src in enumerate((pos_a, pos_b))
    ]
    for c in notice:
        c.start()
    small = [(e2h, eh), (e2l, el), (tw2, tw), (pos_a, pv.at[0]), (pos_b, pv.at[1])]
    small = [pltpu.make_async_copy(s, t, sem_e.at[i]) for i, (s, t) in enumerate(small)]
    for c in small:
        c.start()
    res[...] = jnp.zeros_like(res)
    for c in notice:
        c.wait()

    def tile_of(sid):
        return notes[sid >> 7, (sid & 127) >> 3, 0, sid & 7]

    def scan(g, cnt):
        def one(i, cnt):
            lst[cnt] = 8 * g + notes[g >> 4, g & 15, 0, 16 + 8 * core + i]
            return cnt + 1

        return lax.fori_loop(0, notes[g >> 4, g & 15, 0, 8 + core], one, cnt)

    lst[0] = 0
    count = lax.fori_loop(0, 32, scan, jnp.int32(0))
    last = jnp.where(count > 0, lst[jnp.maximum(count - 1, 0)], 0)
    for k in range(8):
        lst[count + k] = last
    for c in small:
        c.wait()
    pltpu.make_async_copy(d.at[0], d.at[0], sem.at[0]).wait()

    def first(pi, k, qs=range(4)):
        for q in qs:
            x0 = 4 * k + q
            h, l = split(jnp.concatenate([d[pi, 0, x0], d[pi, 1, x0]], axis=0))
            f[pi][x0] = bdot(eh[k], h) + bdot(el[k], h) + bdot(eh[k], l)

    def second(pi, m):
        rr = pl.ds(pl.multiple_of(8 * m, 8), 8)
        ri = pl.ds(pl.multiple_of(128 + 8 * m, 8), 8)
        for jj in range(2):
            cc = slice(128 * jj, 128 * jj + 128)
            v = [(f[pi][x0, rr, cc], f[pi][x0, ri, cc]) for x0 in range(16)]
            v = dft16(v, lambda k: (tw[0, k, rr, :], tw[1, k, rr, :]))
            for t in range(16):
                grid[(pi * 2 + jj) * 16 + t, rr, :] = v[t][0]
                grid[(pi * 2 + jj) * 16 + t, ri, :] = v[t][1]

    def stage0(k, carry):
        first(0, k)
        return carry

    def stage1(k, carry):
        for m in range(4):
            first(1, k, (m,))
            second(0, 4 * k + m)
        return carry

    def stage2(k, carry):
        second(1, k)
        return carry

    lax.fori_loop(0, 4, stage0, 0)
    pltpu.make_async_copy(d.at[1], d.at[1], sem.at[1]).wait()
    lax.fori_loop(0, 4, stage1, 0)
    lax.fori_loop(0, 16, stage2, 0)

    sub = lax.broadcasted_iota(jnp.int32, (8, 128), 0)
    lane = lax.broadcasted_iota(jnp.int32, (8, 128), 1)
    wide[...] = jnp.zeros_like(wide)
    wide[:, 0:16] = kt[...]
    spread = jnp.take_along_axis(wide[...], lane >> 3, axis=1)
    table = jnp.broadcast_to(jnp.sum(jnp.where(sub == (lane & 7), spread, 0.0), axis=0, keepdims=True), (8, 128))

    def taps(row):
        row = jnp.broadcast_to(row, (8, 128))
        off = row & 15
        cell = row >> 4
        cl = cell & 7
        idx = off * 8 + ((sub - cl) & 7)
        return jnp.take_along_axis(table, idx, axis=1), (cell >> 3) + (sub < cl).astype(jnp.int32)

    def build(sid, buf):
        ww, wl, ru, hu = buf
        pos = pv[sid >> 7, (sid & 127) >> 3, pl.ds(pl.multiple_of(8 * (sid & 7), 8), 8), :]
        for jp in range(2):
            th = []
            for j in (2 * jp, 2 * jp + 1):
                r, h = taps(pos[4 + j : 5 + j, :])
                rh = r.astype(BF16).astype(F32)
                th.append((rh, r - rh, h))
                ru[j], hu[j] = taps(pos[j : j + 1, :])
            cc = slice(256 * jp, 256 * jp + 256)
            for i in range(16):
                masks = [h == i for _, _, h in th]
                wh = jnp.concatenate([jnp.where(m, v[0], 0.0) for m, v in zip(masks, th)], axis=1).astype(BF16)
                ww[8 * i : 8 * i + 8, cc] = wh
                ww[128 + 8 * i : 136 + 8 * i, cc] = wh
                wl[8 * i : 8 * i + 8, cc] = jnp.concatenate(
                    [jnp.where(m, v[1], 0.0) for m, v in zip(masks, th)], axis=1
                ).astype(BF16)

    def finish(sid, buf):
        ww, wl, ru, hu = buf
        t = jnp.maximum(tile_of(sid) - 1, 0)
        x = grid[(((sid >> 1) & 1) * 2 + (t & 1)) * 16 + (t >> 4)]
        h = x.astype(BF16)
        hf = h.astype(F32)
        part = bdot(jnp.concatenate([hf, x - hf], axis=1).astype(BF16), ww[...]) + bdot(h, wl[...])
        rows = []
        for j in range(4):
            r, h = ru[j], hu[j]
            for c in range(2):
                acc = jnp.zeros((8, 128), F32)
                for i in range(16):
                    acc = jnp.where(h == i, part[128 * c + 8 * i : 128 * c + 8 * i + 8, 128 * j : 128 * j + 128], acc)
                rows.append(jnp.sum(r * acc, axis=0, keepdims=True))
        res[sid] = jnp.concatenate(rows[0::2] + rows[1::2], axis=0)

    build(lst[0], bufs[0])
    build(lst[1], bufs[1])

    def four(i, carry):
        for k in range(4):
            finish(lst[4 * i + k], bufs[k])
            build(lst[4 * i + 2 + k], bufs[(k + 2) % 4])
        return carry

    lax.fori_loop(0, (count + 3) >> 2, four, 0)

    def hand_over(i, carry):
        r8 = pl.ds(pl.multiple_of(8 * i, 8), 8)
        out_a[r8] = res[r8]
        out_b[r8] = res[pl.ds(pl.multiple_of(128 + 8 * i, 8), 8)]
        return carry

    lax.fori_loop(0, 16, hand_over, 0)


def along_x(plans, kt, e2, pos_a, pos_b, parts):
    buf = [
        pltpu.VMEM((256, 512), BF16),
        pltpu.VMEM((128, 512), BF16),
        pltpu.VMEM((4, 8, 128), F32),
        pltpu.VMEM((4, 8, 128), jnp.int32),
    ]
    return pl.pallas_call(
        functools.partial(along_x_kernel, plans),
        out_shape=[jax.ShapeDtypeStruct((128, 8, 128), F32)] * 2,
        in_specs=[VMEM] + [HBM] * (5 + len(parts)),
        out_specs=[VMEM, VMEM],
        scratch_shapes=[
            pltpu.VMEM((4, 256, 256), BF16),
            pltpu.VMEM((4, 256, 256), BF16),
            pltpu.VMEM((2, 12, 128, 128), F32),
            pltpu.VMEM((2, 16, 72, 128), jnp.int32),
            pltpu.VMEM((2, 2, 16, 128, 256), F32),
            pltpu.VMEM((16, 256, 256), F32),
            pltpu.VMEM((16, 256, 256), F32),
            pltpu.VMEM((64, 256, 128), F32),
            *buf,
            *buf,
            *buf,
            *buf,
            pltpu.VMEM((256, 8, 128), F32),
            pltpu.VMEM((8, 128), F32),
            pltpu.SMEM((272,), jnp.int32),
            pltpu.SMEM((2, 16, 1, 128), jnp.int32),
            pltpu.SemaphoreType.DMA((2,)),
            pltpu.SemaphoreType.DMA((5,)),
            pltpu.SemaphoreType.DMA((2,)),
        ],
        compiler_params=pltpu.CompilerParams(vmem_limit_bytes=67043328),
        cost_estimate=pl.CostEstimate(flops=60_000_000_000, bytes_accessed=16 << 20, transcendentals=0),
        name="along_x",
    )(kt, *e2, pos_a, pos_b, *parts)


def arrange_kernel(mine, got, payload, blocks, notes, counts, sem):
    zh = lax.axis_index("zh")
    copies = []
    for i, src in enumerate((mine, got)):
        copies.append(pltpu.make_async_copy(src.at[pl.ds(0, 16)], blocks.at[i], sem.at[2 * i]))
        copies.append(pltpu.make_async_copy(src.at[16], notes.at[i], sem.at[2 * i + 1]))
    for c in copies:
        c.start()
    for c in copies:
        c.wait()
    payload[:, 64:72, :] = jnp.zeros((16, 8, 128), jnp.int32)
    for i in range(32):
        counts[i] = 0
    lane = lax.broadcasted_iota(jnp.int32, (8, 128), 1)
    for i, home in enumerate((zh, 1 - zh)):
        def one(b, carry, i=i, home=home):
            slot, tile = notes[i, 0, b], notes[i, 1, b]
            mine = (slot >> 6) == zh
            chip, k = (slot >> 2) & 15, 4 * home + (slot & 3)

            @pl.when(mine)
            def _():
                payload[chip, pl.ds(pl.multiple_of(8 * k, 8), 8), :] = blocks[i, b]
                side = ((tile - 1) >> 1) & 1
                n = counts[2 * chip + side]
                counts[2 * chip + side] = n + 1
                row = jnp.where(lane == k, tile, payload[chip, 64:72, :])
                row = jnp.where(lane == 8 + side, n + 1, row)
                payload[chip, 64:72, :] = jnp.where(lane == 16 + 8 * side + n, k, row)

            return carry

        lax.fori_loop(0, 16, one, 0)


def arrange(mine, got):
    i32 = jnp.int32
    return pl.pallas_call(
        arrange_kernel,
        out_shape=jax.ShapeDtypeStruct((16, 72, 128), i32),
        in_specs=[HBM, HBM],
        out_specs=VMEM,
        scratch_shapes=[
            pltpu.VMEM((2, 16, 8, 128), i32),
            pltpu.SMEM((2, 8, 128), i32),
            pltpu.SMEM((32,), i32),
            pltpu.SemaphoreType.DMA((4,)),
        ],
        compiler_params=pltpu.CompilerParams(vmem_limit_bytes=8 << 20),
        cost_estimate=pl.CostEstimate(flops=1 << 20, bytes_accessed=1 << 20, transcendentals=0),
        name="arrange",
    )(mine, got)


def pick_kernel(here, there, answers, observed, rest, other):
    for b in range(16):
        i, j = here[b], there[b]
        v = answers[jnp.maximum(i, 0)]
        rest[b] = observed[b] - jnp.where(i >= 0, v, 0.0)
        v = answers[jnp.maximum(j, 0)]
        other[b] = jnp.where(j >= 0, v, 0.0)


def pick(here, there, answers, observed):
    return pl.pallas_call(
        pick_kernel,
        out_shape=[jax.ShapeDtypeStruct((16, 8, 128), F32)] * 2,
        in_specs=[SMEM, SMEM, VMEM, VMEM],
        out_specs=[VMEM, VMEM],
        compiler_params=pltpu.CompilerParams(vmem_limit_bytes=8 << 20),
        name="pick",
    )(here, there, answers, observed)


def shift(x, axes, size, by):
    return lax.ppermute(x, axes, [(i, (i + by) % size) for i in range(size)])


def shards(sky, plane_w, kernel, tile_ids, plane_ids, positions, observed):
    i32 = jnp.int32
    z_axes = ("zh", "wa")
    swap = [(0, 1), (1, 0)]

    target = plane_ids[:, 0]
    same = (target[:, None] == target[None, :]).astype(i32)
    slot = target * 2 + jnp.sum(jnp.tril(same, -1), axis=1)
    notes = jnp.pad(jnp.stack([slot, tile_ids + 1]), ((0, 6), (0, 112)))
    mine0 = jnp.concatenate([positions.reshape(16, 8, 128), notes[None]], axis=0)
    got0 = lax.ppermute(mine0, "zh", swap)

    own0, ab = turn(0, sky)
    zl = shift(ab, z_axes, 8, 1)
    zr = shift(ab, z_axes, 8, -1)
    zf = shift(ab, z_axes, 8, 2)
    lo, hi = turn(1, sky)
    cl_lo = shift(lo, z_axes, 8, 1)
    cr_hi = shift(hi, z_axes, 8, -1)
    cl_hi = shift(hi, z_axes, 8, 1)
    cr_lo = shift(lo, z_axes, 8, -1)
    cf_lo = shift(cl_lo, z_axes, 8, 1)
    cf_hi = shift(cr_hi, z_axes, 8, -1)

    mine_a, mine_b = gather3(zl, zr, zf)

    def three(x, axis):
        l = shift(x, axis, 4, 1)
        r = shift(x, axis, 4, -1)
        return r, shift(x, axis, 4, 2), l

    ax, bx = three(mine_a, "x"), three(mine_b, "y")
    a0, b0 = join((mine_a,) + ax, (mine_b,) + bx)
    ar, af, al = three(a0, "y")
    br, bf, bl = three(b0, "x")

    payload = arrange(mine0, got0)

    def place(sl, home):
        return jnp.where((sl >> 6) == zh, ((sl >> 2) & 15) * 8 + 4 * home + (sl & 3), -1)

    zh = lax.axis_index("zh")
    here, there = place(slot, zh), place(got0[16, 0, :16], 1 - zh)
    asked = lax.all_to_all(payload, ("x", "y"), split_axis=0, concat_axis=0, tiled=True)
    asked_b = lax.ppermute(asked, "core", swap)
    other_w = lax.ppermute(plane_w, "core", swap)
    ws = plane_w, other_w
    *e1, tw1, tw2 = tables()
    e1, e2 = e1[:2] + [tw1], e1[2:] + [tw2]
    plans, parts = [], []

    def call(plan, srcs):
        keep, send = along_y(plan, ws, e1, srcs)
        plans.append(plan)
        parts.extend([keep, lax.ppermute(send, "core", swap)])

    def blk(kind, d, rows, row, *src):
        return dict(kind=kind, d=d, rows=rows, row=row, src=src)

    call([blk("own", 0, 128, 0, 0)], [own0])
    call([blk("own", 128, 128, 0, 0, 1), blk("a", 0, 3 * R, 0, 2), blk("b", 0, 3 * R, 0, 3)], [lo, hi, a0, b0])
    call(
        [
            blk("c", 0, CR, 0, 0, 1),
            blk("c", 1, CR, 0, 2, 3),
            blk("a", 3, 3 * R, 0, 4),
            blk("a", 1, 3 * R, 0, 5),
            blk("b", 3, 3 * R, 0, 6),
            blk("b", 1, 3 * R, 0, 7),
        ],
        [cl_lo, cl_hi, cr_lo, cr_hi, al, ar, bl, br],
    )
    call([blk("c", 2, CR, 0, 0, 1), blk("a", 2, 3 * R, 0, 2), blk("b", 2, 3 * R, 0, 3)], [cf_lo, cf_hi, af, bf])

    out_a, out_b = along_x(plans, kernel.T, e2, asked, asked_b, parts)
    from_b = lax.ppermute(out_b, "core", swap)
    merged = out_a + from_b
    answers = lax.all_to_all(merged.reshape(16, 64, 128), ("x", "y"), split_axis=0, concat_axis=0, tiled=True)
    rest, other = pick(here, there, answers.reshape(128, 8, 128), observed.reshape(16, 8, 128))
    got = lax.ppermute(other, "zh", swap)
    return (rest - got).reshape(16, 2, 512)


def solution(mesh):
    fine = Mesh(mesh.devices.reshape(2, 4, 4, 2, 4), ("zh", "x", "y", "core", "wa"))
    ba = ("zh", "x", "y", "core")
    rows = ba + ("wa",)
    return jax.shard_map(
        shards,
        mesh=fine,
        in_specs=(
            P(None, None, "wa"),
            P(ba),
            P(),
            P(rows),
            P(rows, None),
            P(rows, None, None),
            P(rows, None, None),
        ),
        out_specs=P(rows, None, None),
        check_vma=False,
    )
```

```python
import functools

import jax
import jax.numpy as jnp
from jax import lax
from jax.experimental import pallas as pl
from jax.experimental.pallas import tpu as pltpu
from jax.sharding import Mesh
from jax.sharding import PartitionSpec as P


N = 2048
SP = 0.7 / N
R = 16
CR = 128
SMEM = pl.BlockSpec(memory_space=pltpu.SMEM)
VMEM = pl.BlockSpec(memory_space=pltpu.VMEM)
HBM = pl.BlockSpec(memory_space=pltpu.HBM)
F32 = jnp.float32
BF16 = jnp.bfloat16

SIN_C = (4.44288292, -7.3082457, 3.60635441, -0.846112886, 0.109826988)
COS_C = (1.4142135, -6.97885099, 5.73946117, -1.88356299, 0.310698192)
G_C = (0.5, 0.12500105, 0.0624521, 0.03985648, 0.0215331, 0.03890036)
MAGIC = 12582912.0


def place_ids():
    return tuple(lax.axis_index(n) for n in ("core", "wa", "x", "y"))


def horner(z, coefs):
    acc = jnp.full_like(z, coefs[-1])
    for c in coefs[-2::-1]:
        acc = acc * z + c
    return acc


def cis_turns(t):
    r = t - ((t + MAGIC) - MAGIC)
    z = r * r
    s = r * horner(z, SIN_C)
    return 1.0 - s * s, s * horner(z, COS_C)


def split(x):
    hi = x.astype(BF16)
    return hi, (x - hi.astype(F32)).astype(BF16)


def bdot(a, b):
    return jnp.dot(a, b, preferred_element_type=F32)


def cis_of(k):
    return cis_turns((k & (N - 1)).astype(F32) * (1.0 / N))


def put_quarter(h, l, i, r, c, v):
    h[i, 128 * r : 128 * r + 128, 128 * c : 128 * c + 128] = v[0]
    l[i, 128 * r : 128 * r + 128, 128 * c : 128 * c + 128] = v[1]


def square_iotas():
    return [lax.broadcasted_iota(jnp.int32, (128, 128), d) for d in range(2)]


def tables_kernel(e1h, e1l, tw1):
    row, col = square_iotas()
    lane = lax.broadcasted_iota(jnp.int32, (8, 128), 1)
    a = lax.axis_index("wa")

    def matrices(p, carry):
        c, s = cis_of(col * (16 * jnp.where(p > 1, 127 - row, row) + 4 * p))
        ch, sh = split(c), split(s)
        put_quarter(e1h, e1l, p, 0, 0, ch)
        put_quarter(e1h, e1l, p, 1, 1, ch)
        put_quarter(e1h, e1l, p, 0, 1, (-sh[0], -sh[1]))
        put_quarter(e1h, e1l, p, 1, 0, sh)
        return carry

    def factors(k, carry):
        c, s = cis_of((512 * a + 128 * (k & 3) + lane) * (1 + (k >> 2)))
        tw1[2 * k] = c
        tw1[2 * k + 1] = -s
        return carry

    lax.fori_loop(0, 4, matrices, 0)
    lax.fori_loop(0, 12, factors, 0)


def tables():
    sds = jax.ShapeDtypeStruct
    return pl.pallas_call(
        tables_kernel,
        out_shape=[sds((4, 256, 256), BF16)] * 2 + [sds((24, 8, 128), F32)],
        out_specs=[VMEM] * 3,
        cost_estimate=pl.CostEstimate(flops=60 * 16 * 16384, bytes_accessed=1 << 20, transcendentals=0),
        name="tables",
    )()


def turn_kernel(sky, own, lo, hi, ab, xin, t, tmp, sem_in, sem_out):
    core, _, xc, yc = place_ids()
    loads, moves = [], []
    for k in range(4):
        col = pl.multiple_of(256 * core + 128 * (k // 2), 128)
        loads.append(pltpu.make_async_copy(sky.at[k % 2, :, pl.ds(col, 128)], xin.at[k], sem_in.at[k]))
        loads[k].start()

    def move(src, dst):
        moves.append(pltpu.make_async_copy(src, dst, sem_out.at[len(moves)]))
        moves[-1].start()

    rev = 127 - lax.broadcasted_iota(jnp.int32, (128, 128), 1)
    for k in range(4):
        b, c = k // 2, k % 2
        loads[k].wait()
        for y4 in range(4):
            def group(i, carry, y4=y4, b=b, c=c, k=k):
                for e in range(2):
                    y0 = 4 * y4 + 2 * i + e
                    v = xin[k, pl.ds(y0, 128, stride=16), :].T
                    if y4 > 1:
                        v = jnp.take_along_axis(v, rev, axis=1)
                    tmp[e] = v
                    for j0 in range(16):
                        t[b, y0, 8 * j0 : 8 * j0 + 8, 128 * c : 128 * c + 128] = tmp[e, pl.ds(j0, 8, stride=16), :]
                return carry

            lax.fori_loop(0, 2, group, 0)
            if k == 3:
                dst = (lo, hi)[y4 // 2].at[pl.ds(4 * (y4 % 2), 4)]
                move(t.at[1, pl.ds(4 * y4, 4)], dst)
        if k == 1:
            move(t.at[0, pl.ds(4 * xc, 4), pl.ds(pl.multiple_of(R * yc, 8), R), :], ab.at[0])
            move(t.at[0, pl.ds(4 * yc, 4), pl.ds(pl.multiple_of(4 * R + R * xc, 8), R), :], ab.at[1])
            move(t.at[0], own)
    for m in moves:
        m.wait()


def turn(sky):
    sds = lambda *d: jax.ShapeDtypeStruct(d, F32)
    outs = [sds(16, 128, 256), sds(8, 128, 256), sds(8, 128, 256), sds(2, 4, R, 256)]
    return pl.pallas_call(
        turn_kernel,
        in_specs=[HBM],
        out_specs=[HBM] * 4,
        out_shape=outs,
        scratch_shapes=[
            pltpu.VMEM((4, N, 128), F32),
            pltpu.VMEM((2, 16, 128, 256), F32),
            pltpu.VMEM((2, 128, 128), F32),
            pltpu.SemaphoreType.DMA((4,)),
            pltpu.SemaphoreType.DMA((7,)),
        ],
        cost_estimate=pl.CostEstimate(flops=1 << 22, bytes_accessed=8 << 20, transcendentals=0),
        name="turn",
    )(sky)


def gather3_kernel(zl, zr, zf, oa, ob):
    for k, o in enumerate((oa, ob)):
        for i, z in enumerate((zl, zr, zf)):
            o[:, R * i : R * i + R, :] = z[k]


def gather3(*z):
    return pl.pallas_call(
        gather3_kernel,
        out_shape=[jax.ShapeDtypeStruct((4, 3 * R, 256), F32)] * 2,
        in_specs=[VMEM] * 3,
        out_specs=[VMEM] * 2,
        compiler_params=pltpu.CompilerParams(vmem_limit_bytes=8 << 20),
        cost_estimate=pl.CostEstimate(flops=1 << 20, bytes_accessed=1 << 20, transcendentals=0),
        name="gather3",
    )(*z)


def join_kernel(*refs):
    ids = place_ids()
    for k in range(4):
        for base, ref, o in ((ids[2], refs[k], refs[8]), (ids[3], refs[4 + k], refs[9])):
            o[pl.ds(4 * ((base + k) & 3), 4)] = ref[...]


def join(a, b):
    return pl.pallas_call(
        join_kernel,
        out_shape=[jax.ShapeDtypeStruct((16, 3 * R, 256), F32)] * 2,
        in_specs=[VMEM] * 8,
        out_specs=[VMEM] * 2,
        compiler_params=pltpu.CompilerParams(vmem_limit_bytes=16 << 20),
        cost_estimate=pl.CostEstimate(flops=1 << 20, bytes_accessed=3 << 20, transcendentals=0),
        name="join",
    )(*a, *b)


def slab_of(kind, k, ids):
    a = ids[1]
    return (a + (0 if kind == "own" else (3, 1, 2)[k])) & 3


def block_rows(blk, ids):
    kind, d, n = blk["kind"], blk["d"], blk["rows"]
    if kind == "own":
        return [(slab_of(kind, 0, ids), d, n // 8)]
    if kind == "c":
        return [(slab_of(kind, d, ids), 128, n // 8)]
    first = R * ((ids[3] + d) & 3) if kind == "a" else 4 * R + R * ((ids[2] + d) & 3)
    return [(slab_of(kind, k, ids), first, R // 8) for k in range(3)]


def along_y_kernel(plan, n_src, w_own, w_other, e1h, e1l, tw1, *rest):
    ids = place_ids()
    srcs = rest[:n_src]
    keep, send = rest[n_src : n_src + 2]
    eh, el, tw, xin, xh0, xl0, yb0, xh1, xl1, yb1, gb, cs, cy2, tab, where, sem_e, sem_in, sem_out = rest[n_src + 2 :]
    core = ids[0]
    lane = lax.broadcasted_iota(jnp.int32, (8, 128), 1)
    sub = lax.broadcasted_iota(jnp.int32, (8, 128), 0)
    w = [jnp.where(core == pi, w_own[0], w_other[0]) for pi in range(2)]
    n_pairs = sum(blk["rows"] for blk in plan) // 16
    steps = n_pairs // 2

    kinds, k = [], 0
    for blk in plan:
        if blk["src"] not in kinds:
            kinds.append(blk["src"])
        for i in range(blk["rows"] // 16):
            where[2 * k] = kinds.index(blk["src"])
            where[2 * k + 1] = blk["row"] + 16 * i
            k += 1
    k = 0
    for blk in plan:
        for slab, first, n in block_rows(blk, ids):
            for i in range(n):
                row = first + 8 * i
                tab[k] = 512 * slab + 256 * core + 128 * (row >> 7) + ((row >> 3) & 15)
                k += 1

    def load(pair, slot, a):
        kind, row = where[2 * pair], pl.ds(pl.multiple_of(where[2 * pair + 1], 16), 16)
        for i, src in enumerate(kinds):
            @pl.when(kind == i)
            def _(src=src):
                h = 16 // len(src)
                for j, s in enumerate(src):
                    pltpu.make_async_copy(
                        srcs[s].at[:, row, :], xin.at[slot, a, pl.ds(h * j, h)], sem_in.at[slot, a]
                    ).start()

    def stores(k, slot):
        out = []
        for a in range(2):
            dst = pl.ds(4 * k + 2 * a, 2)
            out.append(pltpu.make_async_copy(gb.at[slot, a, core], keep.at[:, :, dst], sem_out.at[slot, a, 0]))
            out.append(pltpu.make_async_copy(gb.at[slot, a, 1 - core], send.at[:, :, dst], sem_out.at[slot, a, 1]))
        return out

    for k in range(min(2, steps)):
        for a in range(2):
            load(2 * k + a, k, a)

    e_copies = [
        pltpu.make_async_copy(src, dst, sem_e.at[i]) for i, (src, dst) in enumerate(((e1h, eh), (e1l, el), (tw1, tw)))
    ]
    for c in e_copies:
        c.start()

    for kap in range(9):
        cy = ((16 * lane + kap).astype(F32) - N / 2) * SP
        cy2[kap] = cy * cy

    def image(pair, slot, s, xh, xl):
        for a in range(2):
            cx = ((tab[2 * pair + a] + 16 * sub).astype(F32) - N / 2) * SP
            cx2 = cx * cx
            for y0 in range(16):
                p, q = y0 // 4, y0 % 4
                kap = min(y0, 16 - y0)
                if y0 <= 8:
                    r2 = cx2 + cy2[kap]
                    t = r2 * horner(r2, G_C)
                    pairs = [cis_turns(t * w[pi]) for pi in range(2)]
                    if 0 < y0 < 8:
                        for pi in range(2):
                            cs[s, a, kap, pi, 0] = pairs[pi][0]
                            cs[s, a, kap, pi, 1] = pairs[pi][1]
                else:
                    pairs = [(cs[s, a, kap, pi, 0], cs[s, a, kap, pi, 1]) for pi in range(2)]
                sr = xin[slot, s, y0, 8 * a : 8 * a + 8, 0:128]
                si = xin[slot, s, y0, 8 * a : 8 * a + 8, 128:256]
                for pi, (c, n) in enumerate(pairs):
                    r0 = 64 * a + 16 * q + 8 * pi
                    h, l = split(jnp.concatenate([sr * c - si * n, sr * n + si * c], axis=1))
                    xh[p, r0 : r0 + 8, :] = h
                    xl[p, r0 : r0 + 8, :] = l

    def long_part(xh, xl, yb):
        for p in range(4):
            x = xh[p]
            yb[p] = bdot(x, eh[p]) + bdot(xl[p], eh[p]) + bdot(x, el[p])

    def short_one(slot, s, yb, a, pi):
        sums = None
        for q in range(4):
            r0 = 64 * a + 16 * q + 8 * pi
            rows = pl.ds(r0 if isinstance(r0, int) else pl.multiple_of(r0, 8), 8)
            v = butterfly4([(yb[p, rows, 0:128], yb[p, rows, 128:256]) for p in range(4)])
            if q:
                out = []
                for j, (r, i) in enumerate(v):
                    k = 8 * (q - 1) + 2 * j
                    out.append((r * tw[k] - i * tw[k + 1], r * tw[k + 1] + i * tw[k]))
                v = out
            sums = v if sums is None else [(x + u, y + z) for (x, y), (u, z) in zip(sums, v)]
        for j, (vr, vi) in enumerate(sums):
            cc = slice(128 * (j % 2), 128 * (j % 2) + 128)
            gb[slot, s, j // 2, pi, 0, a, :, cc] = vr
            gb[slot, s, j // 2, pi, 1, a, :, cc] = vi

    def short_part(slot, s, yb):
        for a in range(2):
            for pi in range(2):
                short_one(slot, s, yb, a, pi)

    def short_tail(i, carry):
        for s, yb in enumerate((yb0, yb1)):
            short_one((steps - 1) % 2, s, yb, i >> 1, i & 1)
        return carry

    def step(k, slot3):
        @pl.when(k >= 2)
        def _():
            for c in stores(k - 2, k & 1):
                c.start()

        @pl.when(k >= 3)
        def _():
            for c in stores(k - 3, 1 - (k & 1)):
                c.wait()

        ahead = jnp.where(slot3 == 0, 2, slot3 - 1)

        @pl.when(k + 2 < steps)
        def _():
            for a in range(2):
                load(2 * k + 4 + a, ahead, a)

        for a in range(2):
            pltpu.make_async_copy(xin.at[slot3, a], xin.at[slot3, a], sem_in.at[slot3, a]).wait()
        done = 1 - (k & 1)
        long_part(xh1, xl1, yb1)
        short_part(done, 0, yb0)
        image(2 * k, slot3, 0, xh0, xl0)
        long_part(xh0, xl0, yb0)
        short_part(done, 1, yb1)
        image(2 * k + 1, slot3, 1, xh1, xl1)
        return jnp.where(slot3 == 2, 0, slot3 + 1)

    def arrived(slot):
        for a in range(2):
            pltpu.make_async_copy(xin.at[slot, a], xin.at[slot, a], sem_in.at[slot, a]).wait()

    if steps > 2:
        for a in range(2):
            load(4 + a, 2, a)
    arrived(0)
    image(0, 0, 0, xh0, xl0)
    for c in e_copies:
        c.wait()
    long_part(xh0, xl0, yb0)
    image(1, 0, 1, xh1, xl1)
    lax.fori_loop(1, steps, step, jnp.int32(1))
    last = (steps - 1) % 2
    if steps >= 2:
        for c in stores(steps - 2, steps % 2):
            c.start()
    if steps >= 3:
        for c in stores(steps - 3, last):
            c.wait()
    long_part(xh1, xl1, yb1)
    lax.fori_loop(0, 4, short_tail, 0)
    for c in stores(steps - 1, last):
        c.start()
    if steps >= 2:
        for c in stores(steps - 2, steps % 2):
            c.wait()
    for c in stores(steps - 1, last):
        c.wait()


def along_y(plan, ws, e1, srcs):
    total = sum(blk["rows"] for blk in plan)
    out = jax.ShapeDtypeStruct((2, 2, total // 8, 8, 256), F32)
    stage = [pltpu.VMEM((4, 128, 256), BF16), pltpu.VMEM((4, 128, 256), BF16), pltpu.VMEM((4, 128, 256), F32)]
    return pl.pallas_call(
        functools.partial(along_y_kernel, plan, len(srcs)),
        out_shape=[out, out],
        in_specs=[SMEM] * 2 + [HBM] * (3 + len(srcs)),
        out_specs=[HBM, HBM],
        scratch_shapes=[
            pltpu.VMEM((4, 256, 256), BF16),
            pltpu.VMEM((4, 256, 256), BF16),
            pltpu.VMEM((24, 8, 128), F32),
            pltpu.VMEM((3, 2, 16, 16, 256), F32),
            *stage,
            *stage,
            pltpu.VMEM((2, 2, 2, 2, 2, 2, 8, 256), F32),
            pltpu.VMEM((2, 2, 8, 2, 2, 8, 128), F32),
            pltpu.VMEM((9, 8, 128), F32),
            pltpu.SMEM((total // 8,), jnp.int32),
            pltpu.SMEM((total // 8,), jnp.int32),
            pltpu.SemaphoreType.DMA((3,)),
            pltpu.SemaphoreType.DMA((3, 2)),
            pltpu.SemaphoreType.DMA((2, 2, 2)),
        ],
        compiler_params=pltpu.CompilerParams(vmem_limit_bytes=67043328),
        cost_estimate=pl.CostEstimate(
            flops=total * 2 * 16 * 3 * 256 * 256 * 2, bytes_accessed=total * 24 * 1024, transcendentals=0
        ),
    )(*ws, *e1, *srcs)


def butterfly4(v):
    (r0, i0), (r1, i1), (r2, i2), (r3, i3) = v
    ar, ai, br, bi = r0 + r2, i0 + i2, r0 - r2, i0 - i2
    cr, ci, dr, di = r1 + r3, i1 + i3, r1 - r3, i1 - i3
    return [(ar + cr, ai + ci), (br + di, bi - dr), (ar - cr, ai - ci), (br - di, bi + dr)]


def dft16(v, tw):
    out = [None] * 16
    inner = [butterfly4([v[4 * p + q] for p in range(4)]) for q in range(4)]
    for t0 in range(4):
        cols = [inner[0][t0]]
        for q in range(1, 4):
            (r, i), (c, s) = inner[q][t0], tw(4 * (q - 1) + t0)
            cols.append((r * c - i * s, r * s + i * c))
        for t1, val in enumerate(butterfly4(cols)):
            out[t0 + 4 * t1] = val
    return out


def along_x_kernel(plans, kt, pos_a, pos_b, *rest):
    ids = place_ids()
    n = len(plans)
    parts = rest[: 2 * n]
    out_a, out_b = rest[2 * n : 2 * n + 2]
    eh, el, tw, pv, d, f0, f1, grid = rest[2 * n + 2 : 2 * n + 10]
    bufs = [rest[2 * n + 10 + 4 * k : 2 * n + 14 + 4 * k] for k in range(4)]
    res, wide, lst, notes, sem, sem_e, sem_o = rest[2 * n + 26 :]
    f = (f0, f1)
    core = ids[0]
    last8 = pl.ds(64, 1)
    notice = [
        pltpu.make_async_copy(src.at[:, last8, :], notes.at[i], sem_o.at[i]) for i, src in enumerate((pos_a, pos_b))
    ]
    for c in notice:
        c.start()
    loads = []
    for i, plan in enumerate(plans):
        off = 0
        for blk in plan:
            for slab, first, cnt in block_rows(blk, ids):
                base = 32 * slab + 8 * (first >> 7)
                for ref, side in ((parts[2 * i], core), (parts[2 * i + 1], 1 - core)):
                    at = pl.ds(pl.multiple_of(base + 16 * side, 8), 8)
                    loads.append((ref, off, cnt, (first >> 3) & 15, at))
                off += cnt
    for pi in range(2):
        for ref, off, cnt, j0, at in loads:
            dst = d.at[pi, :, pl.ds(j0, cnt), at, :]
            pltpu.make_async_copy(ref.at[pi, :, pl.ds(off, cnt)], dst, sem.at[pi]).start()
    small = [(pos_a, pv.at[0]), (pos_b, pv.at[1])]
    small = [pltpu.make_async_copy(s, t, sem_e.at[i]) for i, (s, t) in enumerate(small)]
    for c in small:
        c.start()
    res[...] = jnp.zeros_like(res)
    row, col = square_iotas()

    def matrices(p, carry):
        c, s = cis_of(row * (16 * col + 4 * p))
        ch, sh = split(c * (1.0 / N)), split(s * (1.0 / N))
        put_quarter(eh, el, p, 0, 0, ch)
        put_quarter(eh, el, p, 1, 1, ch)
        put_quarter(eh, el, p, 0, 1, sh)
        put_quarter(eh, el, p, 1, 0, (-sh[0], -sh[1]))
        return carry

    def factors(k, carry):
        c, s = cis_of((128 * (k & 3) + row) * (1 + (k >> 2)))
        tw[0, k] = c
        tw[1, k] = -s
        return carry

    lax.fori_loop(0, 4, matrices, 0)
    lax.fori_loop(0, 12, factors, 0)
    for c in notice:
        c.wait()

    def tile_of(sid):
        return notes[sid >> 7, (sid & 127) >> 3, 0, sid & 7]

    def scan(g, cnt):
        def one(i, cnt):
            lst[cnt] = 8 * g + notes[g >> 4, g & 15, 0, 16 + 8 * core + i]
            return cnt + 1

        return lax.fori_loop(0, notes[g >> 4, g & 15, 0, 8 + core], one, cnt)

    lst[0] = 0
    count = lax.fori_loop(0, 32, scan, jnp.int32(0))
    last = jnp.where(count > 0, lst[jnp.maximum(count - 1, 0)], 0)
    for k in range(8):
        lst[count + k] = last
    pltpu.make_async_copy(d.at[0], d.at[0], sem.at[0]).wait()

    def first(pi, k, qs=range(4)):
        for q in qs:
            x0 = 4 * k + q
            h, l = split(jnp.concatenate([d[pi, 0, x0], d[pi, 1, x0]], axis=0))
            f[pi][x0] = bdot(eh[k], h) + bdot(el[k], h) + bdot(eh[k], l)

    def second(pi, m):
        rr = pl.ds(pl.multiple_of(8 * m, 8), 8)
        ri = pl.ds(pl.multiple_of(128 + 8 * m, 8), 8)
        for jj in range(2):
            cc = slice(128 * jj, 128 * jj + 128)
            v = [(f[pi][x0, rr, cc], f[pi][x0, ri, cc]) for x0 in range(16)]
            v = dft16(v, lambda k: (tw[0, k, rr, :], tw[1, k, rr, :]))
            for t in range(16):
                grid[(pi * 2 + jj) * 16 + t, rr, :] = v[t][0]
                grid[(pi * 2 + jj) * 16 + t, ri, :] = v[t][1]

    def stage0(k, carry):
        first(0, k)
        return carry

    def stage1(k, carry):
        for m in range(4):
            first(1, k, (m,))
            second(0, 4 * k + m)
        return carry

    def stage2(k, carry):
        second(1, k)
        return carry

    lax.fori_loop(0, 4, stage0, 0)
    pltpu.make_async_copy(d.at[1], d.at[1], sem.at[1]).wait()
    lax.fori_loop(0, 4, stage1, 0)
    lax.fori_loop(0, 16, stage2, 0)
    for c in small:
        c.wait()

    sub = lax.broadcasted_iota(jnp.int32, (8, 128), 0)
    lane = lax.broadcasted_iota(jnp.int32, (8, 128), 1)
    wide[...] = jnp.zeros_like(wide)
    wide[:, 0:16] = kt[...]
    spread = jnp.take_along_axis(wide[...], lane >> 3, axis=1)
    table = jnp.broadcast_to(jnp.sum(jnp.where(sub == (lane & 7), spread, 0.0), axis=0, keepdims=True), (8, 128))

    def taps(row):
        row = jnp.broadcast_to(row, (8, 128))
        off = row & 15
        cell = row >> 4
        cl = cell & 7
        idx = off * 8 + ((sub - cl) & 7)
        return jnp.take_along_axis(table, idx, axis=1), (cell >> 3) + (sub < cl).astype(jnp.int32)

    def build(sid, buf):
        ww, wl, ru, hu = buf
        pos = pv[sid >> 7, (sid & 127) >> 3, pl.ds(pl.multiple_of(8 * (sid & 7), 8), 8), :]
        for jp in range(2):
            th = []
            for j in (2 * jp, 2 * jp + 1):
                r, h = taps(pos[4 + j : 5 + j, :])
                rh = r.astype(BF16).astype(F32)
                th.append((rh, r - rh, h))
                ru[j], hu[j] = taps(pos[j : j + 1, :])
            cc = slice(256 * jp, 256 * jp + 256)
            for i in range(16):
                masks = [h == i for _, _, h in th]
                wh = jnp.concatenate([jnp.where(m, v[0], 0.0) for m, v in zip(masks, th)], axis=1).astype(BF16)
                ww[8 * i : 8 * i + 8, cc] = wh
                ww[128 + 8 * i : 136 + 8 * i, cc] = wh
                wl[8 * i : 8 * i + 8, cc] = jnp.concatenate(
                    [jnp.where(m, v[1], 0.0) for m, v in zip(masks, th)], axis=1
                ).astype(BF16)

    def finish(sid, buf):
        ww, wl, ru, hu = buf
        t = jnp.maximum(tile_of(sid) - 1, 0)
        x = grid[(((sid >> 1) & 1) * 2 + (t & 1)) * 16 + (t >> 4)]
        h = x.astype(BF16)
        hf = h.astype(F32)
        part = bdot(jnp.concatenate([hf, x - hf], axis=1).astype(BF16), ww[...]) + bdot(h, wl[...])
        rows = []
        for j in range(4):
            r, h = ru[j], hu[j]
            for c in range(2):
                acc = jnp.zeros((8, 128), F32)
                for i in range(16):
                    acc = jnp.where(h == i, part[128 * c + 8 * i : 128 * c + 8 * i + 8, 128 * j : 128 * j + 128], acc)
                rows.append(jnp.sum(r * acc, axis=0, keepdims=True))
        res[sid] = jnp.concatenate(rows[0::2] + rows[1::2], axis=0)

    build(lst[0], bufs[0])
    build(lst[1], bufs[1])

    def four(i, carry):
        for k in range(4):
            finish(lst[4 * i + k], bufs[k])
            build(lst[4 * i + 2 + k], bufs[(k + 2) % 4])
        return carry

    lax.fori_loop(0, (count + 3) >> 2, four, 0)

    def hand_over(i, carry):
        r8 = pl.ds(pl.multiple_of(8 * i, 8), 8)
        out_a[r8] = res[r8]
        out_b[r8] = res[pl.ds(pl.multiple_of(128 + 8 * i, 8), 8)]
        return carry

    lax.fori_loop(0, 16, hand_over, 0)


def along_x(plans, kt, pos_a, pos_b, parts):
    buf = [
        pltpu.VMEM((256, 512), BF16),
        pltpu.VMEM((128, 512), BF16),
        pltpu.VMEM((4, 8, 128), F32),
        pltpu.VMEM((4, 8, 128), jnp.int32),
    ]
    return pl.pallas_call(
        functools.partial(along_x_kernel, plans),
        out_shape=[jax.ShapeDtypeStruct((128, 8, 128), F32)] * 2,
        in_specs=[VMEM] + [HBM] * (2 + len(parts)),
        out_specs=[VMEM, VMEM],
        scratch_shapes=[
            pltpu.VMEM((4, 256, 256), BF16),
            pltpu.VMEM((4, 256, 256), BF16),
            pltpu.VMEM((2, 12, 128, 128), F32),
            pltpu.VMEM((2, 16, 72, 128), jnp.int32),
            pltpu.VMEM((2, 2, 16, 128, 256), F32),
            pltpu.VMEM((16, 256, 256), F32),
            pltpu.VMEM((16, 256, 256), F32),
            pltpu.VMEM((64, 256, 128), F32),
            *buf,
            *buf,
            *buf,
            *buf,
            pltpu.VMEM((256, 8, 128), F32),
            pltpu.VMEM((8, 128), F32),
            pltpu.SMEM((272,), jnp.int32),
            pltpu.SMEM((2, 16, 1, 128), jnp.int32),
            pltpu.SemaphoreType.DMA((2,)),
            pltpu.SemaphoreType.DMA((2,)),
            pltpu.SemaphoreType.DMA((2,)),
        ],
        compiler_params=pltpu.CompilerParams(vmem_limit_bytes=67043328),
        cost_estimate=pl.CostEstimate(flops=60_000_000_000, bytes_accessed=16 << 20, transcendentals=0),
        name="along_x",
    )(kt, pos_a, pos_b, *parts)


def arrange_kernel(mine, got, payload, blocks, notes, counts, sem):
    zh = lax.axis_index("zh")
    copies = []
    for i, src in enumerate((mine, got)):
        copies.append(pltpu.make_async_copy(src.at[pl.ds(0, 16)], blocks.at[i], sem.at[2 * i]))
        copies.append(pltpu.make_async_copy(src.at[16], notes.at[i], sem.at[2 * i + 1]))
    for c in copies:
        c.start()
    for c in copies:
        c.wait()
    payload[:, 64:72, :] = jnp.zeros((16, 8, 128), jnp.int32)
    for i in range(32):
        counts[i] = 0
    lane = lax.broadcasted_iota(jnp.int32, (8, 128), 1)
    for i, home in enumerate((zh, 1 - zh)):
        def one(b, carry, i=i, home=home):
            slot, tile = notes[i, 0, b], notes[i, 1, b]
            mine = (slot >> 6) == zh
            chip, k = (slot >> 2) & 15, 4 * home + (slot & 3)

            @pl.when(mine)
            def _():
                payload[chip, pl.ds(pl.multiple_of(8 * k, 8), 8), :] = blocks[i, b]
                side = ((tile - 1) >> 1) & 1
                n = counts[2 * chip + side]
                counts[2 * chip + side] = n + 1
                row = jnp.where(lane == k, tile, payload[chip, 64:72, :])
                row = jnp.where(lane == 8 + side, n + 1, row)
                payload[chip, 64:72, :] = jnp.where(lane == 16 + 8 * side + n, k, row)

            return carry

        lax.fori_loop(0, 16, one, 0)


def arrange(mine, got):
    i32 = jnp.int32
    return pl.pallas_call(
        arrange_kernel,
        out_shape=jax.ShapeDtypeStruct((16, 72, 128), i32),
        in_specs=[HBM, HBM],
        out_specs=VMEM,
        scratch_shapes=[
            pltpu.VMEM((2, 16, 8, 128), i32),
            pltpu.SMEM((2, 8, 128), i32),
            pltpu.SMEM((32,), i32),
            pltpu.SemaphoreType.DMA((4,)),
        ],
        compiler_params=pltpu.CompilerParams(vmem_limit_bytes=8 << 20),
        cost_estimate=pl.CostEstimate(flops=1 << 20, bytes_accessed=1 << 20, transcendentals=0),
        name="arrange",
    )(mine, got)


def pick_kernel(here, there, answers, observed, rest, other):
    for b in range(16):
        i, j = here[b], there[b]
        v = answers[jnp.maximum(i, 0)]
        rest[b] = observed[b] - jnp.where(i >= 0, v, 0.0)
        v = answers[jnp.maximum(j, 0)]
        other[b] = jnp.where(j >= 0, v, 0.0)


def pick(here, there, answers, observed):
    return pl.pallas_call(
        pick_kernel,
        out_shape=[jax.ShapeDtypeStruct((16, 8, 128), F32)] * 2,
        in_specs=[SMEM, SMEM, VMEM, VMEM],
        out_specs=[VMEM, VMEM],
        compiler_params=pltpu.CompilerParams(vmem_limit_bytes=8 << 20),
        name="pick",
    )(here, there, answers, observed)


def shift(x, axes, size, by):
    return lax.ppermute(x, axes, [(i, (i + by) % size) for i in range(size)])


def shards(sky, plane_w, kernel, tile_ids, plane_ids, positions, observed):
    i32 = jnp.int32
    z_axes = ("zh", "wa")
    swap = [(0, 1), (1, 0)]

    target = plane_ids[:, 0]
    same = (target[:, None] == target[None, :]).astype(i32)
    slot = target * 2 + jnp.sum(jnp.tril(same, -1), axis=1)
    notes = jnp.pad(jnp.stack([slot, tile_ids + 1]), ((0, 6), (0, 112)))
    mine0 = jnp.concatenate([positions.reshape(16, 8, 128), notes[None]], axis=0)
    got0 = lax.ppermute(mine0, "zh", swap)

    own0, lo, hi, ab = turn(sky)
    zl = shift(ab, z_axes, 8, 1)
    zr = shift(ab, z_axes, 8, -1)
    zf = shift(ab, z_axes, 8, 2)
    cl_lo = shift(lo, z_axes, 8, 1)
    cr_hi = shift(hi, z_axes, 8, -1)
    cl_hi = shift(hi, z_axes, 8, 1)
    cr_lo = shift(lo, z_axes, 8, -1)
    cf_lo = shift(cl_lo, z_axes, 8, 1)
    cf_hi = shift(cr_hi, z_axes, 8, -1)

    mine_a, mine_b = gather3(zl, zr, zf)

    def three(x, axis):
        l = shift(x, axis, 4, 1)
        r = shift(x, axis, 4, -1)
        return r, shift(x, axis, 4, 2), l

    ax, bx = three(mine_a, "x"), three(mine_b, "y")
    a0, b0 = join((mine_a,) + ax, (mine_b,) + bx)
    ar, af, al = three(a0, "y")
    br, bf, bl = three(b0, "x")

    payload = arrange(mine0, got0)

    def place(sl, home):
        return jnp.where((sl >> 6) == zh, ((sl >> 2) & 15) * 8 + 4 * home + (sl & 3), -1)

    zh = lax.axis_index("zh")
    here, there = place(slot, zh), place(got0[16, 0, :16], 1 - zh)
    asked = lax.all_to_all(payload, ("x", "y"), split_axis=0, concat_axis=0, tiled=True)
    asked_b = lax.ppermute(asked, "core", swap)
    other_w = lax.ppermute(plane_w, "core", swap)
    ws = plane_w, other_w
    e1 = tables()
    plans, parts = [], []

    def call(plan, srcs):
        keep, send = along_y(plan, ws, e1, srcs)
        plans.append(plan)
        parts.extend([keep, lax.ppermute(send, "core", swap)])

    def blk(kind, d, rows, row, *src):
        return dict(kind=kind, d=d, rows=rows, row=row, src=src)

    call([blk("own", 0, 128, 0, 0)], [own0])
    call([blk("own", 128, 128, 0, 0, 1), blk("a", 0, 3 * R, 0, 2), blk("b", 0, 3 * R, 0, 3)], [lo, hi, a0, b0])
    call(
        [
            blk("c", 0, CR, 0, 0, 1),
            blk("c", 1, CR, 0, 2, 3),
            blk("a", 3, 3 * R, 0, 4),
            blk("a", 1, 3 * R, 0, 5),
            blk("b", 3, 3 * R, 0, 6),
            blk("b", 1, 3 * R, 0, 7),
        ],
        [cl_lo, cl_hi, cr_lo, cr_hi, al, ar, bl, br],
    )
    call([blk("c", 2, CR, 0, 0, 1), blk("a", 2, 3 * R, 0, 2), blk("b", 2, 3 * R, 0, 3)], [cf_lo, cf_hi, af, bf])

    out_a, out_b = along_x(plans, kernel.T, asked, asked_b, parts)
    from_b = lax.ppermute(out_b, "core", swap)
    merged = out_a + from_b
    answers = lax.all_to_all(merged.reshape(16, 64, 128), ("x", "y"), split_axis=0, concat_axis=0, tiled=True)
    rest, other = pick(here, there, answers.reshape(128, 8, 128), observed.reshape(16, 8, 128))
    got = lax.ppermute(other, "zh", swap)
    return (rest - got).reshape(16, 2, 512)


def solution(mesh):
    fine = Mesh(mesh.devices.reshape(2, 4, 4, 2, 4), ("zh", "x", "y", "core", "wa"))
    ba = ("zh", "x", "y", "core")
    rows = ba + ("wa",)
    return jax.shard_map(
        shards,
        mesh=fine,
        in_specs=(
            P(None, None, "wa"),
            P(ba),
            P(),
            P(rows),
            P(rows, None),
            P(rows, None, None),
            P(rows, None, None),
        ),
        out_specs=P(rows, None, None),
        check_vma=False,
    )
```
